32 devices in a mesh: seq: 4 (over x, core), dp: 8 (over z, y).
Axes of the slice: x: 2, y: 2, z: 4, core: 2. Of those that a mesh axis runs over, the one named last changes fastest.
Arguments:
- hidden_states: bfloat16 [8, 2048, 1024], P('dp', 'seq'), may hold values from -6 to 6
- segment_ids: int32 [8, 2048], P('dp', 'seq'), may hold values from 0 to 3, never falling along the last dimension, each value on 1 to 1024 neighbouring positions
- positions: int32 [8, 2048], P('dp', 'seq'), may hold values from 0 to 2047
- out_grad: bfloat16 [8, 2048, 1024], P('dp', 'seq'), may hold values from -6 to 6
- qkv_weight: bfloat16 [1024, 3072], P(('seq', 'dp')), may hold values from -0.1875 to 0.1875
- qkv_bias: bfloat16 [3072], P(('seq', 'dp')), may hold values from -3 to 3
- dense_weight: bfloat16 [1024, 1024], P(('seq', 'dp')), may hold values from -1.5 to 1.5
- dense_bias: bfloat16 [1024], P(('seq', 'dp')), may hold values from -3 to 3
- up_weight: bfloat16 [1024, 4096], P(('seq', 'dp')), may hold values from -0.1875 to 0.1875
- up_bias: bfloat16 [4096], P(('seq', 'dp')), may hold values from -3 to 3
- down_weight: bfloat16 [4096, 1024], P(('seq', 'dp')), may hold values from -0.09375 to 0.09375
- down_bias: bfloat16 [1024], P(('seq', 'dp')), may hold values from -3 to 3
- attn_gain: bfloat16 [1024], P(('seq', 'dp')), may hold values from 0.5 to 1.5
- attn_shift: bfloat16 [1024], P(('seq', 'dp')), may hold values from -3 to 3
- ffn_gain: bfloat16 [1024], P(('seq', 'dp')), may hold values from 0.5 to 1.5
- ffn_shift: bfloat16 [1024], P(('seq', 'dp')), may hold values from -3 to 3
Outputs:
- output: bfloat16 [8, 2048, 1024], P('dp', 'seq')
- input_grad: bfloat16 [8, 2048, 1024], P('dp', 'seq')
- qkv_weight_grad: float32 [1024, 3072], P(('seq', 'dp'))
- qkv_bias_grad: float32 [3072], P(('seq', 'dp'))
- dense_weight_grad: float32 [1024, 1024], P(('seq', 'dp'))
- dense_bias_grad: float32 [1024], P(('seq', 'dp'))
- up_weight_grad: float32 [1024, 4096], P(('seq', 'dp'))
- up_bias_grad: float32 [4096], P(('seq', 'dp'))
- down_weight_grad: float32 [4096, 1024], P(('seq', 'dp'))
- down_bias_grad: float32 [1024], P(('seq', 'dp'))
- attn_gain_grad: float32 [1024], P(('seq', 'dp'))
- attn_shift_grad: float32 [1024], P(('seq', 'dp'))
- ffn_gain_grad: float32 [1024], P(('seq', 'dp'))
- ffn_shift_grad: float32 [1024], P(('seq', 'dp'))
The draws below stay inside these ranges and needn't reach their ends.
Inputs may be any that keep to these rules, and one draw needn't show every extreme that they name: `segment_ids`: along each sequence the segment numbers never fall, and each of the 4 numbers appears.
All inputs are finite; a program needn't handle non-finite values.
Results may differ from the reference program's by a relative error of at most 0.03.
Values may be sent and summed in bfloat16 or wider, within the bound.
A program may use at most 192 MiB of HBM per device.

```python
import math
import jax
import jax.numpy as jnp
import numpy as np
from jax import lax

D = 1024
HEADS = 16
HEAD = 64
FF = 4096
ROT = 16
MAXPOS = 2048
DOCS = 4
SEQ_LEN = 2048
SEQS = 8


def place_ends(values, key, low, top_value):
    spot = [jax.random.randint(jax.random.fold_in(key, axis), (), 0, length) for axis, length in enumerate(values.shape)]
    main_axis = values.shape.index(max(values.shape))
    beside = spot[:main_axis] + [(spot[main_axis] + 1) % values.shape[main_axis]] + spot[main_axis + 1:]
    return values.at[tuple(spot)].set(low).at[tuple(beside)].set(top_value)


def block_levels(rng, dims, pieces, low, top_value):
    level = 1.0
    for dim, blocks in pieces:
        steps = jax.random.uniform(jax.random.fold_in(jax.random.fold_in(rng, 6), dim), (blocks,), jnp.float32, low / len(pieces), top_value / len(pieces))
        level = level * jnp.repeat(jnp.exp(steps), dims[dim] // blocks).reshape((-1,) + (1,) * (len(dims) - 1 - dim))
    return level


def length_profile(count, total, most, slope):
    weights = [(1 << 20) // math.isqrt(grade ** slope) + 1 for grade in range(2, count + 1)]
    surplus, given = total - most - (count - 1), [1] * (count - 1)
    while surplus > 0:
        movable = [i for i in range(count - 1) if given[i] < most]
        mass, budget = sum([weights[i] for i in movable]), surplus
        for i in movable:
            addition = min(most - given[i], max(1, budget * weights[i] // mass), surplus)
            given[i] = given[i] + addition
            surplus = surplus - addition
    return np.array([most] + given)


def ragged(own_key, amount, total, most, lean):
    if amount == 2:
        one = jax.random.randint(own_key, (), max(1, total - most), min(most, total - 1) + 1)
        return jnp.stack([one, total - one])
    sizes = jnp.asarray(length_profile(amount, total, most, lean), jnp.int32)
    couples = (amount - 1) // 2
    giver, taker = sizes[1:1 + 2 * couples:2], sizes[2:2 + 2 * couples:2]
    margin = jnp.minimum(giver - 1, most - taker)
    moved = jax.random.randint(jax.random.fold_in(own_key, 1), (couples,), 0, 1 << 20) % (margin + 1)
    sizes = sizes.at[1:1 + 2 * couples:2].set(giver - moved).at[2:2 + 2 * couples:2].set(taker + moved)
    return sizes[jax.random.permutation(jax.random.fold_in(own_key, 2), amount)]


def gaussian(key, shape, deviation, reach, split=(), kind=jnp.bfloat16):
    loudness = block_levels(key, shape, split, -0.22, 0.18) if split else 1.0
    values = jax.random.normal(key, shape, jnp.float32) * deviation * loudness
    return jnp.minimum(jnp.maximum(values, -reach), reach).astype(kind)


def setup_inputs(seed: int = 0) -> dict:
    streams_of = jax.random.split(jax.random.key(seed), 17)
    return {
        "hidden_states": gaussian(streams_of[0], (SEQS, SEQ_LEN, D), 1.0, 6.0, ((0, 8), (1, 4))),
        "segment_ids": jax.vmap(lambda own: jnp.searchsorted(jnp.cumsum(ragged(own, DOCS, SEQ_LEN, SEQ_LEN // 2, 1)), jnp.arange(SEQ_LEN), side="right"))(jax.random.split(streams_of[1], SEQS)).reshape((SEQS, SEQ_LEN)).astype(jnp.int32),
        "positions": place_ends(jax.random.randint(streams_of[2], (SEQS, SEQ_LEN), 0, MAXPOS), jax.random.fold_in(streams_of[2], 1), 0, MAXPOS - 1).astype(jnp.int32),
        "out_grad": gaussian(streams_of[3], (SEQS, SEQ_LEN, D), 1.0, 6.0, ((0, 8), (1, 4))),
        "qkv_weight": gaussian(streams_of[4], (D, 3 * D), D ** -0.5, 0.1875, ((0, 32),)),
        "qkv_bias": gaussian(streams_of[5], (3 * D,), 0.5, 3.0, ((0, 32),)),
        "dense_weight": gaussian(streams_of[6], (D, D), (D // 64) ** -0.5, 1.5, ((0, 32),)),
        "dense_bias": gaussian(streams_of[7], (D,), 0.5, 3.0, ((0, 32),)),
        "up_weight": gaussian(streams_of[8], (D, FF), D ** -0.5, 0.1875, ((0, 32),)),
        "up_bias": gaussian(streams_of[9], (FF,), 0.5, 3.0, ((0, 32),)),
        "down_weight": gaussian(streams_of[10], (FF, D), FF ** -0.5, 0.09375, ((0, 32),)),
        "down_bias": gaussian(streams_of[11], (D,), 0.5, 3.0, ((0, 32),)),
        "attn_gain": jnp.clip(1.0 + 0.1 * jax.random.normal(streams_of[12], (D,), jnp.float32), 0.5, 1.5).astype(jnp.bfloat16),
        "attn_shift": gaussian(streams_of[13], (D,), 0.5, 3.0, ((0, 32),)),
        "ffn_gain": jnp.clip(1.0 + 0.1 * jax.random.normal(streams_of[14], (D,), jnp.float32), 0.5, 1.5).astype(jnp.bfloat16),
        "ffn_shift": gaussian(streams_of[15], (D,), 0.5, 3.0, ((0, 32),)),
    }


epsilon = 1e-05
masked_score = -1e+30
rotary_base = 10000.0

@jax.custom_vjp
def low(v):
    return lax.optimization_barrier(v.astype(jnp.bfloat16)).astype(jnp.float32)

@jax.custom_vjp
def low_back(v):
    return v

def low_keep(v):
    return (low(v), None)

def low_pass(kept, grad):
    return (grad,)

def back_keep(v):
    return (v, None)

def back_low(kept, grad):
    return (low(grad),)
low.defvjp(low_keep, low_pass)
low_back.defvjp(back_keep, back_low)

def matmul(left, right):
    return jnp.dot(left, right, precision=lax.Precision.HIGHEST, preferred_element_type=jnp.float32)

def normalize(inputs, gain, shift_vec):
    center = lax.optimization_barrier(jnp.mean(inputs, axis=-1, keepdims=True))
    spread = inputs - center
    variance = lax.optimization_barrier(jnp.mean(spread * spread, axis=-1, keepdims=True))
    return spread * lax.rsqrt(variance + epsilon) * gain + shift_vec

def rotate(tensor, places):
    half_rot = ROT // 2
    freqs = rotary_base ** (-2.0 * jnp.arange(half_rot, dtype=jnp.float32) / ROT)
    angles = places.astype(jnp.float32)[:, None, None] * freqs
    cosine = jnp.cos(angles)
    sine = jnp.sin(angles)
    first = tensor[..., :half_rot]
    second = tensor[..., half_rot:ROT]
    return jnp.concatenate([first * cosine - second * sine, second * cosine + first * sine, tensor[..., ROT:]], axis=-1)

def attend(queries, keys_rot, values, segments):
    length = queries.shape[0]
    row_block = min(512, length)
    block_total = length // row_block
    key_pos = jnp.arange(length, dtype=jnp.int32)
    score_scale = 1.0 / math.sqrt(HEAD)

    def one_block(block_args):
        query_rows, query_segs, row_start = block_args
        scores = jnp.einsum('qhd,khd->hqk', query_rows, keys_rot, precision=lax.Precision.HIGHEST) * score_scale
        scores = low_back(scores)
        query_pos = row_start + jnp.arange(row_block, dtype=jnp.int32)
        allowed = (query_segs[:, None] == segments[None, :]) & (query_pos[:, None] >= key_pos[None, :])
        scores = jnp.where(allowed[None], scores, masked_score)
        probs = jax.nn.softmax(scores, axis=-1)
        mixed = jnp.einsum('hqk,khd->qhd', low(probs), values, precision=lax.Precision.HIGHEST)
        return mixed.reshape(row_block, HEADS * HEAD)
    starts = jnp.arange(block_total, dtype=jnp.int32) * row_block
    blocks = lax.map(jax.checkpoint(one_block), (queries.reshape(block_total, row_block, HEADS, HEAD), segments.reshape(block_total, row_block), starts))
    return blocks.reshape(length, HEADS * HEAD)

def block_layer(params, inputs, segments, places):
    qkv_full, qkv_shift, dense_full, dense_shift, up_full, up_shift, down_full, down_shift, gain_attn, shift_attn, gain_ffn, shift_ffn = params
    length = inputs.shape[0]
    attn_normed = low(normalize(inputs, gain_attn, shift_attn))
    ffn_normed = low(normalize(inputs, gain_ffn, shift_ffn))
    joined = low_back(matmul(attn_normed, qkv_full) + qkv_shift)
    queries = low(rotate(joined[:, :D].reshape(length, HEADS, HEAD), places))
    keys_rot = low(rotate(joined[:, D:2 * D].reshape(length, HEADS, HEAD), places))
    values = low(joined[:, 2 * D:].reshape(length, HEADS, HEAD))
    mixed = low(low_back(attend(queries, keys_rot, values, segments)))
    attn_out = matmul(mixed, dense_full) + dense_shift
    up_pre = low_back(matmul(ffn_normed, up_full) + up_shift)
    activation = low(jax.nn.gelu(up_pre, approximate=False))
    mlp_out = matmul(activation, down_full) + down_shift
    return inputs + attn_out + mlp_out

def reference(hidden_states, segment_ids, positions, out_grad, qkv_weight, qkv_bias, dense_weight, dense_bias, up_weight, up_bias, down_weight, down_bias, attn_gain, attn_shift, ffn_gain, ffn_shift):
    params = tuple((weight.astype(jnp.float32) for weight in (qkv_weight, qkv_bias, dense_weight, dense_bias, up_weight, up_bias, down_weight, down_bias, attn_gain, attn_shift, ffn_gain, ffn_shift)))

    def one_sequence(running_grads, sequence_args):
        tokens, segments, places, cotangent = sequence_args

        def forward(param_tuple, token_rows):
            return block_layer(param_tuple, token_rows, segments, places)
        result, pullback = jax.vjp(forward, params, tokens.astype(jnp.float32))
        param_grads, token_grads = pullback(cotangent.astype(jnp.float32))
        running_grads = jax.tree.map(lambda running, update: running + update, running_grads, param_grads)
        return (running_grads, (result.astype(jnp.bfloat16), token_grads.astype(jnp.bfloat16)))
    zero_grads = jax.tree.map(jnp.zeros_like, params)
    grad_sums, (outputs, input_grads) = lax.scan(one_sequence, zero_grads, (hidden_states, segment_ids, positions, out_grad))
    return (outputs, input_grads, grad_sums[0], grad_sums[1], grad_sums[2], grad_sums[3], grad_sums[4], grad_sums[5], grad_sums[6], grad_sums[7], grad_sums[8], grad_sums[9], grad_sums[10], grad_sums[11])
```

```python
import functools
import math

import jax
import jax.numpy as jnp
import numpy as np
from jax import lax
from jax.experimental import pallas as pl
from jax.experimental.pallas import tpu as pltpu
from jax.sharding import PartitionSpec as P

HEAD = 64
ROT = 16
DOCS = 4
HI = 4

epsilon = 1e-05
masked_score = -1e30
rotary_base = 10000.0

BF = jnp.bfloat16
F32 = jnp.float32
NT = (((1,), (1,)), ((), ()))
TN = (((0,), (0,)), ((), ()))


VMEM_LIMIT = 60 * 1024 * 1024


def xor_swap(value, axis, count, mask):
    return lax.ppermute(value, axis, [(i, i ^ mask) for i in range(count)])


def mm(left, right):
    return jnp.dot(left, right, preferred_element_type=F32)


def mm_nt(left, right):
    return lax.dot_general(left, right, NT, preferred_element_type=F32)


def mm_tn(left, right):
    return lax.dot_general(left, right, TN, preferred_element_type=F32)


def params_of(**more):
    return pltpu.CompilerParams(vmem_limit_bytes=VMEM_LIMIT, **more)


def whole(shape):
    zeros = (0,) * len(shape)
    return pl.BlockSpec(shape, lambda *grid_and_ids: zeros)


class Dims:
    def __init__(self, ns, nd, tokens, width, ff):
        self.ns, self.nd = ns, nd
        self.hi, self.lo = HI, nd // HI
        self.nx = ns // 2
        self.tokens, self.width = tokens, width
        self.seq = ns * tokens
        self.hw = width // ns
        self.ffw = ff // ns
        self.heads = self.hw // HEAD


def piece_copies(dims, kind, ids, pieces, target, sems):
    s, z, y = ids[0], ids[1], ids[2]
    copies = []
    for jz in range(dims.hi):
        for jy in range(dims.lo):
            piece = pieces[jz * dims.lo + jy]
            owner = (z ^ jz) * dims.lo + (y ^ jy)
            if kind == "row":
                rows = piece.shape[0]
                at = pl.multiple_of(owner * rows, rows)
                copies.append(
                    pltpu.make_async_copy(piece, target.at[pl.ds(at, rows)], sems.at[len(copies)])
                )
            else:
                rows = piece.shape[1]
                for js in range(dims.ns):
                    at = pl.multiple_of(((s ^ js) * dims.nd + owner) * rows, rows)
                    copies.append(
                        pltpu.make_async_copy(
                            piece.at[js], target.at[pl.ds(at, rows)], sems.at[len(copies)]
                        )
                    )
    return copies


def token_call(dims, name, ids, body, lhs, weights, extras, outs, tile, flops, scratch=()):
    count = dims.seq // tile
    n_lhs, n_out = len(lhs), len(outs)
    sizes = [len(w[1]) for w in weights]
    sem_counts = [
        len(w[1]) * (dims.ns if w[0] == "col" else 1) for w in weights
    ]

    def kernel(ids_ref, *refs):
        at = 0
        lhs_refs = refs[:n_lhs]
        at = n_lhs
        piece_refs = []
        for size in sizes:
            piece_refs.append(refs[at : at + size])
            at += size
        extra_refs = refs[at : at + len(extras)]
        at += len(extras)
        out_refs = refs[at : at + n_out]
        at += n_out
        weight_refs = refs[at : at + len(weights)]
        at += len(weights)
        sem_refs = refs[at : at + len(weights)]
        at += len(weights)
        scratch_refs = refs[at:]
        step = pl.program_id(0)

        if weights:

            @pl.when(step == 0)
            def _():
                copies = []
                for w, group, target, sems in zip(weights, piece_refs, weight_refs, sem_refs):
                    copies += piece_copies(dims, w[0], ids_ref, group, target, sems)
                for copy in copies:
                    copy.start()
                for copy in copies:
                    copy.wait()

        body(step, count, lhs_refs, weight_refs, extra_refs, out_refs, scratch_refs)

    in_specs = [pl.BlockSpec((tile, a.shape[1]), lambda i, ids_ref: (i, 0)) for a in lhs]
    for size in sizes:
        in_specs += [pl.BlockSpec(memory_space=pl.ANY)] * size
    in_specs += [whole(a.shape) for a in extras]
    bytes_moved = sum(a.size * a.dtype.itemsize for a in lhs) + sum(
        math.prod(o[0].shape) * o[0].dtype.itemsize for o in outs
    )
    return pl.pallas_call(
        kernel,
        out_shape=[o[0] for o in outs],
        grid_spec=pltpu.PrefetchScalarGridSpec(
            num_scalar_prefetch=1,
            grid=(count,),
            in_specs=in_specs,
            out_specs=[o[1] for o in outs],
            scratch_shapes=[pltpu.VMEM(w[2], BF) for w in weights]
            + [pltpu.SemaphoreType.DMA((n,)) for n in sem_counts]
            + list(scratch),
        ),
        compiler_params=params_of(),
        cost_estimate=pl.CostEstimate(flops=flops, bytes_accessed=bytes_moved, transcendentals=0),
        name=name,
    )(ids, *lhs, *[p for w in weights for p in w[1]], *extras)


def tiled_out(rows, cols, tile, dtype=BF):
    return (
        jax.ShapeDtypeStruct((rows, cols), dtype),
        pl.BlockSpec((tile, cols), lambda i, ids_ref: (i, 0)),
    )


def norm_pair(dims, pair, first, second, affine, carried):
    tile = 256
    per = dims.tokens // tile
    base = pair * 2 * per

    def kernel(*refs):
        a_ref, b_ref, affine_ref = refs[:3]
        attn_ref, ffn_ref, hat_ref, rows_ref = refs[-4:]
        block = pl.program_id(0)

        @pl.when(block == 0)
        def _():
            rows_ref[...] = a_ref[...]

        @pl.when(block == 1)
        def _():
            rows_ref[...] = b_ref[...]

        rows = rows_ref[...].astype(F32)
        center = jnp.mean(rows, axis=-1, keepdims=True)
        spread = rows - center
        hat = spread * lax.rsqrt(jnp.mean(spread * spread, axis=-1, keepdims=True) + epsilon)
        attn_ref[...] = (hat * affine_ref[0:1, :] + affine_ref[1:2, :]).astype(BF)
        ffn_ref[...] = (hat * affine_ref[2:3, :] + affine_ref[3:4, :]).astype(BF)
        hat_ref[...] = hat.astype(BF)

    out_spec = pl.BlockSpec((tile, dims.width), lambda b, t: (base + b * per + t, 0))
    shape = jax.ShapeDtypeStruct((dims.seq, dims.width), BF)
    return pl.pallas_call(
        kernel,
        out_shape=[shape] * 3,
        grid=(2, per),
        in_specs=[
            pl.BlockSpec((tile, dims.width), lambda b, t: (jnp.where(b == 0, t, per - 1), 0)),
            pl.BlockSpec((tile, dims.width), lambda b, t: (jnp.where(b == 0, 0, t), 0)),
            pl.BlockSpec((8, dims.width), lambda b, t: (0, 0)),
        ]
        + [pl.BlockSpec(memory_space=pl.ANY)] * len(carried),
        out_specs=[out_spec] * 3,
        scratch_shapes=[pltpu.VMEM((tile, dims.width), BF)],
        input_output_aliases={3 + i: i for i in range(len(carried))},
        compiler_params=params_of(),
        cost_estimate=pl.CostEstimate(
            flops=20 * 2 * dims.tokens * dims.width,
            bytes_accessed=2 * dims.tokens * dims.width * 8,
            transcendentals=0,
        ),
        name="norm_pair",
    )(first, second, affine, *carried)


def up_body(step, count, lhs, weights, extras, outs, scratch):
    pre = mm(lhs[0][...], weights[0][...]) + extras[0][0:1, :]
    total = 0.5 + 0.5 * lax.erf(pre * math.sqrt(0.5))
    density = jnp.exp(-0.5 * pre * pre) * (1.0 / math.sqrt(2.0 * math.pi))
    outs[0][...] = (pre * total).astype(BF)
    outs[1][...] = (total + pre * density).astype(BF)


def turn(values, cosine, sine, sign):
    lane = lax.broadcasted_iota(jnp.int32, (1, values.shape[1]), 1) % HEAD
    width = values.shape[1]
    half = ROT // 2
    other = jnp.where(
        lane < half, pltpu.roll(values, width - half, 1), pltpu.roll(values, half, 1)
    )
    return values * cosine + sign * (other * sine)


def spread_lanes(table, width):
    times = width // table.shape[1]
    return table if times == 1 else jnp.concatenate([table] * times, axis=1)


def qkv_body(dims, step, count, lhs, weights, extras, outs, scratch):
    hw = dims.hw
    joined = mm(lhs[0][...], weights[0][...]) + extras[0][0:1, :]
    cosine = spread_lanes(lhs[1][...], hw)
    sine = spread_lanes(lhs[2][...], hw)
    queries = turn(joined[:, :hw], cosine, sine, 1.0)
    keys = turn(joined[:, hw : 2 * hw], cosine, sine, 1.0)
    values = joined[:, 2 * hw :]
    outs[0][...] = queries.astype(BF) * (1.0 / math.sqrt(HEAD))
    outs[1][...] = keys.astype(BF)
    outs[2][...] = values.astype(BF)
    outs[3][...] = keys.T.astype(BF)
    outs[4][...] = values.T.astype(BF)


def mix_grad_body(step, count, lhs, weights, extras, outs, scratch):
    outs[0][...] = mm_nt(lhs[0][...], weights[0][...]).astype(BF)


def attention(dims, ids, queries, keys, values, keys_t, values_t, grad_mix, cos_table, sin_table):
    tile = 256
    hw, seq, heads = dims.hw, dims.seq, dims.heads
    per = dims.tokens // tile
    count = seq // tile
    scale = 1.0 / math.sqrt(HEAD)

    def place(ids_ref, block):
        return ((block // per) ^ ids_ref[0]) * per + block % per

    def kernel(
        ids_ref, q_ref, k_ref, v_ref, kt_ref, vt_ref, g_ref, cos_ref, sin_ref,
        mix_ref, gq_ref, gk_ref, gv_ref, sum_ref,
        score_ref, prob_ref, gk_acc, gv_acc,
    ):
        block = pl.program_id(0)

        @pl.when(block == 0)
        def _():
            gk_acc[...] = jnp.zeros_like(gk_acc)
            gv_acc[...] = jnp.zeros_like(gv_acc)
            sum_ref[...] = jnp.zeros_like(sum_ref)

        lane = lax.broadcasted_iota(jnp.int32, (1, hw), 1)
        own = [lane // HEAD == h for h in range(heads)]
        queries_here = q_ref[...]
        grads_here = g_ref[...]
        q_heads = [jnp.where(own[h], queries_here, jnp.zeros_like(queries_here)) for h in range(heads)]
        q_pos = block * tile + lax.broadcasted_iota(jnp.int32, (1, tile), 1)
        begin = jnp.zeros((1, tile), jnp.int32)
        low = 0
        for doc in range(1, DOCS):
            edge = ids_ref[doc]
            begin = jnp.where(q_pos >= edge, jnp.maximum(begin, edge), begin)
            low = jnp.where(edge <= block * tile, jnp.maximum(low, edge), low)
        low = low // tile

        def rows_of(key_block):
            return pl.ds(pl.multiple_of(place(ids_ref, key_block) * tile, tile), tile)

        def slot(key_block):
            return pl.ds(pl.multiple_of((key_block - low) * tile, tile), tile)

        def score_pass(key_block, highs):
            rows = k_ref[rows_of(key_block), :]
            key_pos = key_block * tile + lax.broadcasted_iota(jnp.int32, (tile, tile), 0)
            allowed = (key_pos >= begin) & (key_pos <= q_pos)
            result = []
            for h in range(heads):
                scores = jnp.where(allowed, mm_nt(rows, q_heads[h]), masked_score)
                score_ref[h, slot(key_block), :] = scores
                result.append(jnp.maximum(highs[h], jnp.max(scores, axis=0, keepdims=True)))
            return tuple(result)

        highs = lax.fori_loop(
            low, block + 1, score_pass,
            tuple(jnp.full((1, tile), masked_score, F32) for _ in range(heads)),
        )

        def prob_pass(key_block, carry):
            result = []
            rows = rows_of(key_block)
            for h in range(heads):
                total, mixed = carry[2 * h], carry[2 * h + 1]
                probs = jnp.exp(score_ref[h, slot(key_block), :] - highs[h])
                total = total + jnp.sum(probs, axis=0, keepdims=True)
                probs = probs.astype(BF)
                prob_ref[h, slot(key_block), :] = probs
                mixed = mixed + mm(vt_ref[h * HEAD : (h + 1) * HEAD, rows], probs)
                result += [total, mixed]
            return tuple(result)

        start = []
        for h in range(heads):
            start += [jnp.zeros((1, tile), F32), jnp.zeros((HEAD, tile), F32)]
        summed = lax.fori_loop(low, block + 1, prob_pass, tuple(start))

        grads_t = grads_here.astype(F32).T
        mixed_parts, scaled_parts, deltas = [], [], []
        for h in range(heads):
            inverse = 1.0 / summed[2 * h]
            mixed = summed[2 * h + 1] * inverse
            grads = grads_t[h * HEAD : (h + 1) * HEAD, :] * inverse
            deltas.append(jnp.sum(mixed * grads, axis=0, keepdims=True))
            mixed_parts.append(mixed)
            scaled_parts.append(grads)
        mix_ref[...] = jnp.concatenate(mixed_parts, axis=0).T.astype(BF)
        scaled = jnp.concatenate(scaled_parts, axis=0).T.astype(BF)
        g_heads = [jnp.where(own[h], scaled, jnp.zeros_like(scaled)) for h in range(heads)]

        def grad_pass(key_block, grads_q):
            rows = rows_of(key_block)
            value_rows = v_ref[rows, :]
            result = []
            grad_k = gk_acc[rows, :]
            grad_v = gv_acc[rows, :]
            for h in range(heads):
                probs = prob_ref[h, slot(key_block), :]
                grad_probs = mm_nt(value_rows, g_heads[h])
                grad_scores = (probs.astype(F32) * (grad_probs - deltas[h])).astype(BF)
                grad_v = grad_v + mm(probs, g_heads[h])
                grad_k = grad_k + mm(grad_scores, q_heads[h])
                result.append(
                    grads_q[h] + mm(kt_ref[h * HEAD : (h + 1) * HEAD, rows], grad_scores)
                )
            gk_acc[rows, :] = grad_k
            gv_acc[rows, :] = grad_v
            return tuple(result)

        grads_q = lax.fori_loop(
            low, block + 1, grad_pass, tuple(jnp.zeros((HEAD, tile), F32) for _ in range(heads))
        )
        here = rows_of(block)
        rot = (jnp.concatenate(grads_q, axis=0) * scale).T
        grad_q = turn(
            rot, spread_lanes(cos_ref[here, :], hw), spread_lanes(sin_ref[here, :], hw), -1.0
        ).astype(BF)
        gq_ref[...] = grad_q
        sum_ref[0:1, :] += jnp.sum(grad_q.astype(F32), axis=0, keepdims=True)

        @pl.when(block == count - 1)
        def _():
            def finish(t, carry):
                rows = pl.ds(pl.multiple_of(t * tile, tile), tile)
                grad_k = turn(
                    gk_acc[rows, :],
                    spread_lanes(cos_ref[rows, :], hw),
                    spread_lanes(sin_ref[rows, :], hw),
                    -1.0,
                ).astype(BF)
                grad_v = gv_acc[rows, :].astype(BF)
                gk_ref[rows, :] = grad_k
                gv_ref[rows, :] = grad_v
                sum_ref[1:2, :] += jnp.sum(grad_k.astype(F32), axis=0, keepdims=True)
                sum_ref[2:3, :] += jnp.sum(grad_v.astype(F32), axis=0, keepdims=True)
                return carry

            lax.fori_loop(0, count, finish, 0)

    tiled = pl.BlockSpec((tile, hw), lambda i, ids_ref: (place(ids_ref, i), 0))
    shape = jax.ShapeDtypeStruct((seq, hw), BF)
    return pl.pallas_call(
        kernel,
        out_shape=[shape] * 4 + [jax.ShapeDtypeStruct((8, hw), F32)],
        grid_spec=pltpu.PrefetchScalarGridSpec(
            num_scalar_prefetch=1,
            grid=(count,),
            in_specs=[
                tiled,
                whole((seq, hw)),
                whole((seq, hw)),
                whole((hw, seq)),
                whole((hw, seq)),
                tiled,
                whole(cos_table.shape),
                whole(sin_table.shape),
            ],
            out_specs=[tiled, tiled, whole((seq, hw)), whole((seq, hw)), whole((8, hw))],
            scratch_shapes=[
                pltpu.VMEM((heads, seq, tile), F32),
                pltpu.VMEM((heads, seq, tile), BF),
                pltpu.VMEM((seq, hw), F32),
                pltpu.VMEM((seq, hw), F32),
            ],
        ),
        compiler_params=params_of(),
        cost_estimate=pl.CostEstimate(
            flops=12 * seq * seq * hw, bytes_accessed=10 * seq * hw * 2, transcendentals=0
        ),
        name="attention",
    )(ids, queries, keys, values, keys_t, values_t, grad_mix, cos_table, sin_table)


def split_specs(dims, tile):
    per = dims.tokens // tile
    shape = jax.ShapeDtypeStruct((dims.nx, dims.tokens, dims.width), BF)

    def spec(odd):
        def index(i, ids_ref):
            block, t = i // per, i % per
            mine = block % 2 == odd
            row = jnp.where(mine, t, per - 1 if odd == 0 else 0)
            return (block // 2, row, 0)

        return pl.BlockSpec((None, tile, dims.width), index)

    return [(shape, spec(1)), (shape, spec(0))], per


def put_split(step, per, outs, value):
    odd = (step // per) % 2

    @pl.when(odd == 1)
    def _():
        outs[0][...] = value

    @pl.when(odd == 0)
    def _():
        outs[1][...] = value


def out_body(per, step, count, lhs, weights, extras, outs, scratch):
    value = mm(lhs[0][...], weights[0][...]) + mm(lhs[1][...], weights[1][...])
    put_split(step, per, outs, value.astype(BF))


def up_grad_body(step, count, lhs, weights, extras, outs, scratch):
    grads = (mm_nt(lhs[0][...], weights[0][...]) * lhs[1][...].astype(F32)).astype(BF)
    outs[0][...] = grads

    @pl.when(step == 0)
    def _():
        outs[1][...] = jnp.zeros_like(outs[1])

    outs[1][0:1, :] += jnp.sum(grads.astype(F32), axis=0, keepdims=True)


def in_grad_body(per, hw, step, count, lhs, weights, extras, outs, scratch):
    up_grad, gq, gk, gv, hat_ref = lhs
    qkv_ref, up_ref = weights
    affine = extras[0]
    attn = (
        mm_nt(gq[...], qkv_ref[:, :hw])
        + mm_nt(gk[...], qkv_ref[:, hw : 2 * hw])
        + mm_nt(gv[...], qkv_ref[:, 2 * hw :])
    )
    ffn = mm_nt(up_grad[...], up_ref[...])
    hat = hat_ref[...].astype(F32)

    @pl.when(step == 0)
    def _():
        outs[2][...] = jnp.zeros_like(outs[2])

    for row, value in enumerate((attn * hat, attn, ffn * hat, ffn)):
        outs[2][row : row + 1, :] += jnp.sum(value, axis=0, keepdims=True)
    put_split(step, per, outs, (attn * affine[0:1, :] + ffn * affine[2:3, :]).astype(BF))


def weight_grad(dims, name, kind, ids, left, rights):
    tile = 512
    m = left.shape[1]
    widths = [r.shape[1] for r in rights]
    n = sum(widths)
    count = dims.seq // tile
    hi, lo, ns, nd = dims.hi, dims.lo, dims.ns, dims.nd
    if kind == "row":
        rows = m // nd
        shape = (hi, rows, n)
    else:
        rows = m // (nd * ns)
        shape = (hi, ns, rows, n)

    def kernel(ids_ref, left_ref, *refs):
        right_refs = refs[: len(rights)]
        out_refs = refs[len(rights) : len(rights) + lo]
        total = refs[-1]
        step = pl.program_id(0)
        at = 0
        for width, right_ref in zip(widths, right_refs):
            part = mm_tn(left_ref[...], right_ref[...])
            cols = slice(at, at + width)

            @pl.when(step == 0)
            def _():
                total[:, cols] = part

            @pl.when(step > 0)
            def _():
                total[:, cols] += part

            at += width

        @pl.when(step == count - 1)
        def _():
            s, z, y = ids_ref[0], ids_ref[1], ids_ref[2]
            for jy in range(lo):
                for jz in range(hi):
                    owner = (z ^ jz) * lo + (y ^ jy)
                    if kind == "row":
                        at = pl.multiple_of(owner * rows, rows)
                        out_refs[jy][jz] = total[pl.ds(at, rows), :].astype(BF)
                    else:
                        for js in range(ns):
                            at = pl.multiple_of(((s ^ js) * nd + owner) * rows, rows)
                            out_refs[jy][jz, js] = total[pl.ds(at, rows), :].astype(BF)

    return pl.pallas_call(
        kernel,
        out_shape=[jax.ShapeDtypeStruct(shape, BF)] * lo,
        grid_spec=pltpu.PrefetchScalarGridSpec(
            num_scalar_prefetch=1,
            grid=(count,),
            in_specs=[pl.BlockSpec((tile, m), lambda i, ids_ref: (i, 0))]
            + [pl.BlockSpec((tile, w), lambda i, ids_ref: (i, 0)) for w in widths],
            out_specs=[whole(shape)] * lo,
            scratch_shapes=[pltpu.VMEM((m, n), F32)],
        ),
        compiler_params=params_of(),
        cost_estimate=pl.CostEstimate(
            flops=2 * dims.seq * m * n,
            bytes_accessed=2 * (dims.seq * (m + n) + m * n),
            transcendentals=0,
        ),
        name=name,
    )(ids, left, *rights)


def cut_columns(dims, ids, qkv, up):
    ns, hw, ffw = dims.ns, dims.hw, dims.ffw
    rows = qkv.shape[0]

    def kernel(ids_ref, qkv_ref, up_ref, *outs):
        for js in range(ns):
            other = ids_ref[0] ^ js
            for part in range(3):
                at = pl.multiple_of(part * dims.width + other * hw, hw)
                outs[js][:, part * hw : (part + 1) * hw] = qkv_ref[:, pl.ds(at, hw)]
            at = pl.multiple_of(other * ffw, ffw)
            outs[js][:, 3 * hw :] = up_ref[:, pl.ds(at, ffw)]

    shape = (rows, 3 * hw + ffw)
    return pl.pallas_call(
        kernel,
        out_shape=[jax.ShapeDtypeStruct(shape, BF)] * ns,
        grid_spec=pltpu.PrefetchScalarGridSpec(
            num_scalar_prefetch=1,
            grid=(1,),
            in_specs=[whole(qkv.shape), whole(up.shape)],
            out_specs=[whole(shape)] * ns,
        ),
        compiler_params=params_of(),
        name="cut_columns",
    )(ids, qkv, up)


def join_columns(dims, ids, pieces, parts, width):
    ns = dims.ns
    rows, n = pieces[0].shape
    w = n // parts
    total = n * ns

    def kernel(ids_ref, *refs):
        out = refs[-1]
        for js in range(ns):
            other = ids_ref[0] ^ js
            for part in range(parts):
                at = pl.multiple_of(part * width + other * w, w)
                out[:, pl.ds(at, w)] = refs[js][:, part * w : (part + 1) * w].astype(F32)

    return pl.pallas_call(
        kernel,
        out_shape=jax.ShapeDtypeStruct((rows, total), F32),
        grid_spec=pltpu.PrefetchScalarGridSpec(
            num_scalar_prefetch=1,
            grid=(1,),
            in_specs=[whole((rows, n))] * ns,
            out_specs=whole((rows, total)),
        ),
        compiler_params=params_of(),
        name="join_columns",
    )(ids, *pieces)


def per_device(
    hidden_states,
    segment_ids,
    positions,
    out_grad,
    qkv_weight,
    qkv_bias,
    dense_weight,
    dense_bias,
    up_weight,
    up_bias,
    down_weight,
    down_bias,
    attn_gain,
    attn_shift,
    ffn_gain,
    ffn_shift,
):
    ns, nd = lax.axis_size("seq"), lax.axis_size("dp")
    tokens, width = hidden_states.shape[1:]
    dims = Dims(ns, nd, tokens, width, up_weight.shape[1])
    hi, lo, nx = dims.hi, dims.lo, dims.nx
    hw, ffw, seq = dims.hw, dims.ffw, dims.seq
    s, d = lax.axis_index("seq"), lax.axis_index("dp")
    z, y = d // lo, d % lo
    ids = jnp.stack([s, z, y, s]).astype(jnp.int32)

    def by_seq(value, mask):
        return xor_swap(value, "seq", ns, mask)

    def by_dp(value, mask):
        return xor_swap(value, "dp", nd, mask)

    hidden, grad_out = hidden_states[0], out_grad[0]

    fields = (qkv_bias, dense_bias, up_bias, down_bias, attn_gain, attn_shift, ffn_gain, ffn_shift)
    mine = jnp.concatenate(fields)
    index = s * nd + d
    small = jnp.where(jnp.arange(ns * nd)[:, None] == index, mine[None, :], jnp.zeros((), BF))
    mask = 1
    while mask < ns:
        small = small + by_seq(small, mask)
        mask *= 2
    mask = 1
    while mask < nd:
        small = small + by_dp(small, mask)
        mask *= 2
    full, at = [], 0
    for field in fields:
        n = field.shape[0]
        full.append(small[:, at : at + n].reshape(-1).astype(F32))
        at += n
    b_qkv, b_dense, b_up, b_down, g_attn, s_attn, g_ffn, s_ffn = full
    affine = jnp.concatenate(
        [jnp.stack([g_attn, s_attn, g_ffn, s_ffn]), jnp.zeros((4, width), F32)], axis=0
    )
    bias_qkv = lax.dynamic_index_in_dim(
        b_qkv.reshape(3, ns, hw), s, 1, keepdims=False
    ).reshape(1, 3 * hw)
    bias_up = lax.dynamic_slice_in_dim(b_up, s * ffw, ffw).reshape(1, ffw)

    meta = jnp.stack([segment_ids[0], positions[0]])
    metas = [meta] + [by_seq(meta, js) for js in range(1, ns)]
    meta_all = jnp.concatenate(metas, axis=1)
    starts = [jnp.sum((meta_all[0] < v).astype(jnp.int32)) for v in range(1, DOCS)]
    doc_ids = jnp.stack([s.astype(jnp.int32)] + starts)
    half = ROT // 2
    freqs = rotary_base ** (-2.0 * jnp.arange(half, dtype=F32) / ROT)
    angles = meta_all[1].astype(F32)[None, :] * freqs[:, None]
    table = 2 * HEAD
    pick = np.zeros((half, table), np.float32)
    signed = np.zeros((half, table), np.float32)
    rest = np.ones((1, table), np.float32)
    for lane in range(table):
        if lane % HEAD < ROT:
            pick[lane % HEAD % half, lane] = 1.0
            signed[lane % HEAD % half, lane] = -1.0 if lane % HEAD < half else 1.0
            rest[0, lane] = 0.0
    exact = lax.Precision.HIGHEST
    cos_table = lax.dot_general(jnp.cos(angles), jnp.asarray(pick), TN, precision=exact) + rest
    sin_table = lax.dot_general(jnp.sin(angles), jnp.asarray(signed), TN, precision=exact)

    def gather_tokens(value):
        found = [value, by_seq(value, 1)]
        for m in range(1, nx):
            across = by_seq(value, 2 * m)
            found += [across, by_seq(across, 1)]
        return found

    blocks = gather_tokens(hidden)

    cuts = cut_columns(dims, ids, qkv_weight, up_weight)
    got = [cuts[0]] + [by_seq(cuts[js], js) for js in range(1, ns)]
    stacked = jnp.stack(got)

    def gather_dp(shard):
        pieces = []
        for jz in range(hi):
            here = shard if jz == 0 else by_dp(shard, jz * lo)
            pieces += [here] + [by_dp(here, jy) for jy in range(1, lo)]
        return pieces

    up_pieces = gather_dp(stacked[:, :, 3 * hw :])
    qkv_pieces = gather_dp(stacked[:, :, : 3 * hw])
    dense_pieces = gather_dp(dense_weight)
    down_pieces = gather_dp(down_weight)
    qkv_w = ("col", qkv_pieces, (width, 3 * hw))
    up_w = ("col", up_pieces, (width, ffw))
    dense_w = ("row", dense_pieces, (hw, width))
    down_w = ("row", down_pieces, (ffw, width))

    carried = ()
    for m in range(nx):
        carried = norm_pair(dims, m, blocks[2 * m], blocks[2 * m + 1], affine, carried)
    attn_low, ffn_low, hat_low = carried

    tile = 256
    act, slope = token_call(
        dims, "up", ids, up_body, [ffn_low], [up_w], [bias_up],
        [tiled_out(seq, ffw, tile)] * 2, tile, 2 * seq * width * ffw * 2,
    )
    flip = (
        jax.ShapeDtypeStruct((hw, seq), BF),
        pl.BlockSpec((hw, tile), lambda i, ids_ref: (0, i)),
    )
    queries, keys, values, keys_t, values_t = token_call(
        dims, "qkv", ids, functools.partial(qkv_body, dims), [attn_low, cos_table, sin_table],
        [qkv_w], [bias_qkv], [tiled_out(seq, hw, tile)] * 3 + [flip] * 2, tile,
        2 * seq * width * 3 * hw,
    )
    grads_all = jnp.concatenate(gather_tokens(grad_out), axis=0)
    grad_mix = token_call(
        dims, "mix_grad", ids, mix_grad_body, [grads_all], [dense_w], [],
        [tiled_out(seq, hw, tile)], tile, 2 * seq * width * hw,
    )[0]
    mixed, gq, gk, gv, qkv_sums = attention(
        dims, doc_ids, queries, keys, values, keys_t, values_t, grad_mix, cos_table, sin_table
    )

    def reduce_tokens(others, own):
        got = by_seq(others, 1)
        total = own[0].astype(F32) + got[0].astype(F32)
        for m in range(1, nx):
            total = total + by_seq(own[m] + got[m], 2 * m).astype(F32)
        return total

    def reduce_dp(parts):
        got = [by_dp(parts[jy], jy) for jy in range(1, lo)]

        def slab(jz):
            value = parts[0][jz].astype(F32)
            for g in got:
                value = value + g[jz].astype(F32)
            return value

        total = slab(0)
        for jz in range(1, hi):
            total = total + by_dp(slab(jz).astype(BF), jz * lo).astype(F32)
        return total

    def columns_home(total, parts):
        low = total.astype(BF)
        pieces = [low[0]] + [by_seq(low[js], js) for js in range(1, ns)]
        return join_columns(dims, ids, pieces, parts, width)

    down_parts = weight_grad(dims, "down_grad", "row", ids, act, [grads_all])
    grad_down = reduce_dp(down_parts)
    dense_parts = weight_grad(dims, "dense_grad", "row", ids, mixed, [grads_all])
    grad_dense = reduce_dp(dense_parts)
    qkv_parts = weight_grad(dims, "qkv_grad", "col", ids, attn_low, [gq, gk, gv])
    grad_qkv = columns_home(reduce_dp(qkv_parts), 3)

    sums_shape = lambda n: (jax.ShapeDtypeStruct((8, n), F32), whole((8, n)))
    grad_up_low, up_sums = token_call(
        dims, "up_grad", ids, up_grad_body, [grads_all, slope], [down_w], [],
        [tiled_out(seq, ffw, tile), sums_shape(ffw)], tile, 2 * seq * width * ffw,
    )
    up_parts = weight_grad(dims, "up_w_grad", "col", ids, ffn_low, [grad_up_low])
    grad_up = columns_home(reduce_dp(up_parts), 1)

    outs, per = split_specs(dims, tile)
    others, own = token_call(
        dims, "out", ids, functools.partial(out_body, per), [mixed, act], [dense_w, down_w], [],
        outs, tile, 2 * seq * width * (hw + ffw),
    )
    out_total = reduce_tokens(others, own)
    output = (hidden.astype(F32) + out_total + (b_dense + b_down)[None, :]).astype(BF)

    others, own, gain_sums = token_call(
        dims, "in_grad", ids, functools.partial(in_grad_body, per, hw),
        [grad_up_low, gq, gk, gv, hat_low], [qkv_w, up_w], [affine],
        outs + [sums_shape(width)], tile, 2 * seq * width * (3 * hw + ffw),
    )
    gx = reduce_tokens(others, own)
    rows = hidden.astype(F32)
    spread = rows - jnp.mean(rows, axis=-1, keepdims=True)
    inv_std = lax.rsqrt(jnp.mean(spread * spread, axis=-1, keepdims=True) + epsilon)
    hat = spread * inv_std
    back = inv_std * (
        gx
        - jnp.mean(gx, axis=-1, keepdims=True)
        - hat * jnp.mean(gx * hat, axis=-1, keepdims=True)
    )
    grad_out_f = grad_out.astype(F32)
    input_grad = (grad_out_f + back).astype(BF)

    def placed(value, parts, w):
        base = jnp.zeros((parts, ns, w), F32)
        return lax.dynamic_update_slice_in_dim(base, value.reshape(parts, 1, w), s, 1).reshape(-1)

    out_sum = jnp.sum(grad_out_f, axis=0)
    vectors = (
        placed(qkv_sums[:3], 3, hw),
        out_sum,
        placed(up_sums[0], 1, ffw),
        gain_sums[0],
        gain_sums[1],
        gain_sums[2],
        gain_sums[3],
    )
    packed = jnp.concatenate(vectors).reshape(-1, 128)
    mask = 1
    while mask < ns:
        packed = packed + by_seq(packed, mask)
        mask *= 2
    mask = 1
    while mask < nd:
        packed = packed + by_dp(packed, mask)
        mask *= 2
    flat = packed.reshape(-1)
    small_out, at = [], 0
    for vector in vectors:
        n = vector.shape[0]
        share = n // (ns * nd)
        small_out.append(lax.dynamic_slice_in_dim(flat, at + index * share, share))
        at += n
    gb_qkv, gb_out, gb_up, gg_attn, gs_attn, gg_ffn, gs_ffn = small_out
    return (
        output[None],
        input_grad[None],
        grad_qkv,
        gb_qkv,
        grad_dense,
        gb_out,
        grad_up,
        gb_up,
        grad_down,
        gb_out,
        gg_attn,
        gs_attn,
        gg_ffn,
        gs_ffn,
    )


def solution(mesh):
    token = P("dp", "seq", None)
    matrix = P(("seq", "dp"), None)
    vector = P(("seq", "dp"))
    weights = (matrix, vector) * 4 + (vector,) * 4
    return jax.shard_map(
        per_device,
        mesh=mesh,
        in_specs=(token, P("dp", "seq"), P("dp", "seq"), token) + weights,
        out_specs=(token, token) + weights,
        check_vma=False,
    )
```

```python
import functools
import math

import jax
import jax.numpy as jnp
import numpy as np
from jax import lax
from jax.experimental import pallas as pl
from jax.experimental.pallas import tpu as pltpu
from jax.sharding import PartitionSpec as P

HEAD = 64
ROT = 16
DOCS = 4
HI = 4

epsilon = 1e-05
masked_score = -1e30
rotary_base = 10000.0

BF = jnp.bfloat16
F32 = jnp.float32
NT = (((1,), (1,)), ((), ()))
TN = (((0,), (0,)), ((), ()))


VMEM_LIMIT = 60 * 1024 * 1024


def xor_swap(value, axis, count, mask):
    return lax.ppermute(value, axis, [(i, i ^ mask) for i in range(count)])


def mm(left, right):
    return jnp.dot(left, right, preferred_element_type=F32)


def mm_nt(left, right):
    return lax.dot_general(left, right, NT, preferred_element_type=F32)


def mm_tn(left, right):
    return lax.dot_general(left, right, TN, preferred_element_type=F32)


def params_of(**more):
    return pltpu.CompilerParams(vmem_limit_bytes=VMEM_LIMIT, **more)


def whole(shape):
    zeros = (0,) * len(shape)
    return pl.BlockSpec(shape, lambda *grid_and_ids: zeros)


class Dims:
    def __init__(self, ns, nd, tokens, width, ff):
        self.ns, self.nd = ns, nd
        self.hi, self.lo = HI, nd // HI
        self.nx = ns // 2
        self.tokens, self.width = tokens, width
        self.seq = ns * tokens
        self.hw = width // ns
        self.ffw = ff // ns
        self.heads = self.hw // HEAD


def piece_copies(dims, kind, ids, pieces, target, sems):
    s, z, y = ids[0], ids[1], ids[2]
    if kind == "full":
        return [pltpu.make_async_copy(pieces[0], target, sems.at[0])]
    copies = []
    for jz in range(dims.hi):
        for jy in range(dims.lo):
            piece = pieces[jz * dims.lo + jy]
            owner = (z ^ jz) * dims.lo + (y ^ jy)
            if kind == "row":
                rows = piece.shape[0]
                at = pl.multiple_of(owner * rows, rows)
                copies.append(
                    pltpu.make_async_copy(piece, target.at[pl.ds(at, rows)], sems.at[len(copies)])
                )
            else:
                rows = piece.shape[1]
                for js in range(dims.ns):
                    at = pl.multiple_of(((s ^ js) * dims.nd + owner) * rows, rows)
                    copies.append(
                        pltpu.make_async_copy(
                            piece.at[js], target.at[pl.ds(at, rows)], sems.at[len(copies)]
                        )
                    )
    return copies


def token_call(dims, name, ids, body, lhs, weights, extras, outs, tile, flops, scratch=()):
    count = dims.seq // tile
    n_lhs, n_out = len(lhs), len(outs)
    sizes = [len(w[1]) for w in weights]
    sem_counts = [
        len(w[1]) * (dims.ns if w[0] == "col" else 1) for w in weights
    ]

    def kernel(ids_ref, *refs):
        at = 0
        lhs_refs = refs[:n_lhs]
        at = n_lhs
        piece_refs = []
        for size in sizes:
            piece_refs.append(refs[at : at + size])
            at += size
        extra_refs = refs[at : at + len(extras)]
        at += len(extras)
        out_refs = refs[at : at + n_out]
        at += n_out
        weight_refs = refs[at : at + len(weights)]
        at += len(weights)
        sem_refs = refs[at : at + len(weights)]
        at += len(weights)
        scratch_refs = refs[at:]
        step = pl.program_id(0)

        if weights:

            @pl.when(step == 0)
            def _():
                copies = []
                for w, group, target, sems in zip(weights, piece_refs, weight_refs, sem_refs):
                    copies += piece_copies(dims, w[0], ids_ref, group, target, sems)
                for copy in copies:
                    copy.start()
                for copy in copies:
                    copy.wait()

        body(step, count, lhs_refs, weight_refs, extra_refs, out_refs, scratch_refs)

    in_specs = [pl.BlockSpec((tile, a.shape[1]), lambda i, ids_ref: (i, 0)) for a in lhs]
    for size in sizes:
        in_specs += [pl.BlockSpec(memory_space=pl.ANY)] * size
    in_specs += [whole(a.shape) for a in extras]
    bytes_moved = sum(a.size * a.dtype.itemsize for a in lhs) + sum(
        math.prod(o[0].shape) * o[0].dtype.itemsize for o in outs
    )
    return pl.pallas_call(
        kernel,
        out_shape=[o[0] for o in outs],
        grid_spec=pltpu.PrefetchScalarGridSpec(
            num_scalar_prefetch=1,
            grid=(count,),
            in_specs=in_specs,
            out_specs=[o[1] for o in outs],
            scratch_shapes=[pltpu.VMEM(w[2], BF) for w in weights]
            + [pltpu.SemaphoreType.DMA((n,)) for n in sem_counts]
            + list(scratch),
        ),
        compiler_params=params_of(),
        cost_estimate=pl.CostEstimate(flops=flops, bytes_accessed=bytes_moved, transcendentals=0),
        name=name,
    )(ids, *lhs, *[p for w in weights for p in w[1]], *extras)


def tiled_out(rows, cols, tile, dtype=BF):
    return (
        jax.ShapeDtypeStruct((rows, cols), dtype),
        pl.BlockSpec((tile, cols), lambda i, ids_ref: (i, 0)),
    )


def norm_pair(dims, pair, first, second, affine, carried):
    tile = 256
    per = dims.tokens // tile
    base = pair * 2 * per

    def kernel(*refs):
        a_ref, b_ref, affine_ref = refs[:3]
        attn_ref, ffn_ref, hat_ref, rows_ref = refs[-4:]
        block = pl.program_id(0)

        @pl.when(block == 0)
        def _():
            rows_ref[...] = a_ref[...]

        @pl.when(block == 1)
        def _():
            rows_ref[...] = b_ref[...]

        rows = rows_ref[...].astype(F32)
        center = jnp.mean(rows, axis=-1, keepdims=True)
        spread = rows - center
        hat = spread * lax.rsqrt(jnp.mean(spread * spread, axis=-1, keepdims=True) + epsilon)
        attn_ref[...] = (hat * affine_ref[0:1, :] + affine_ref[1:2, :]).astype(BF)
        ffn_ref[...] = (hat * affine_ref[2:3, :] + affine_ref[3:4, :]).astype(BF)
        hat_ref[...] = hat.astype(BF)

    out_spec = pl.BlockSpec((tile, dims.width), lambda b, t: (base + b * per + t, 0))
    shape = jax.ShapeDtypeStruct((dims.seq, dims.width), BF)
    return pl.pallas_call(
        kernel,
        out_shape=[shape] * 3,
        grid=(2, per),
        in_specs=[
            pl.BlockSpec((tile, dims.width), lambda b, t: (jnp.where(b == 0, t, per - 1), 0)),
            pl.BlockSpec((tile, dims.width), lambda b, t: (jnp.where(b == 0, 0, t), 0)),
            pl.BlockSpec((8, dims.width), lambda b, t: (0, 0)),
        ]
        + [pl.BlockSpec(memory_space=pl.ANY)] * len(carried),
        out_specs=[out_spec] * 3,
        scratch_shapes=[pltpu.VMEM((tile, dims.width), BF)],
        input_output_aliases={3 + i: i for i in range(len(carried))},
        compiler_params=params_of(),
        cost_estimate=pl.CostEstimate(
            flops=20 * 2 * dims.tokens * dims.width,
            bytes_accessed=2 * dims.tokens * dims.width * 8,
            transcendentals=0,
        ),
        name="norm_pair",
    )(first, second, affine, *carried)


def up_body(step, count, lhs, weights, extras, outs, scratch):
    pre = mm(lhs[0][...], weights[0][...]) + extras[0][0:1, :]
    total = 0.5 + 0.5 * lax.erf(pre * math.sqrt(0.5))
    density = jnp.exp(-0.5 * pre * pre) * (1.0 / math.sqrt(2.0 * math.pi))
    outs[0][...] = (pre * total).astype(BF)
    outs[1][...] = (total + pre * density).astype(BF)


def turn(values, cosine, sine, sign):
    lane = lax.broadcasted_iota(jnp.int32, (1, values.shape[1]), 1) % HEAD
    width = values.shape[1]
    half = ROT // 2
    other = jnp.where(
        lane < half, pltpu.roll(values, width - half, 1), pltpu.roll(values, half, 1)
    )
    return values * cosine + sign * (other * sine)


def spread_lanes(table, width):
    times = width // table.shape[1]
    return table if times == 1 else jnp.concatenate([table] * times, axis=1)


def qkv_body(dims, step, count, lhs, weights, extras, outs, scratch):
    hw = dims.hw
    joined = mm(lhs[0][...], weights[0][...]) + extras[0][0:1, :]
    cosine = spread_lanes(lhs[1][...], hw)
    sine = spread_lanes(lhs[2][...], hw)
    queries = turn(joined[:, :hw], cosine, sine, 1.0)
    keys = turn(joined[:, hw : 2 * hw], cosine, sine, 1.0)
    values = joined[:, 2 * hw :]
    outs[0][...] = queries.astype(BF) * (1.0 / math.sqrt(HEAD))
    outs[1][...] = keys.astype(BF)
    outs[2][...] = values.astype(BF)
    outs[3][...] = keys.T.astype(BF)
    outs[4][...] = values.T.astype(BF)


def mix_grad_body(step, count, lhs, weights, extras, outs, scratch):
    outs[0][...] = mm_nt(lhs[0][...], weights[0][...]).astype(BF)


def attention(dims, ids, queries, keys, values, keys_t, values_t, grad_mix, cos_table, sin_table):
    tile = 256
    hw, seq, heads = dims.hw, dims.seq, dims.heads
    per = dims.tokens // tile
    count = seq // tile
    scale = 1.0 / math.sqrt(HEAD)

    def place(ids_ref, block):
        return ((block // per) ^ ids_ref[0]) * per + block % per

    def kernel(
        ids_ref, q_ref, k_ref, v_ref, kt_ref, vt_ref, g_ref, cos_ref, sin_ref,
        mix_ref, gq_ref, gk_ref, gv_ref, sum_ref,
        score_ref, prob_ref, gk_acc, gv_acc,
    ):
        block = pl.program_id(0)

        @pl.when(block == 0)
        def _():
            gk_acc[...] = jnp.zeros_like(gk_acc)
            gv_acc[...] = jnp.zeros_like(gv_acc)
            sum_ref[...] = jnp.zeros_like(sum_ref)

        lane = lax.broadcasted_iota(jnp.int32, (1, hw), 1)
        own = [lane // HEAD == h for h in range(heads)]
        queries_here = q_ref[...]
        grads_here = g_ref[...]
        q_heads = [jnp.where(own[h], queries_here, jnp.zeros_like(queries_here)) for h in range(heads)]
        q_pos = block * tile + lax.broadcasted_iota(jnp.int32, (1, tile), 1)
        begin = jnp.zeros((1, tile), jnp.int32)
        low = 0
        for doc in range(1, DOCS):
            edge = ids_ref[doc]
            begin = jnp.where(q_pos >= edge, jnp.maximum(begin, edge), begin)
            low = jnp.where(edge <= block * tile, jnp.maximum(low, edge), low)
        low = low // tile

        def rows_of(key_block):
            return pl.ds(pl.multiple_of(place(ids_ref, key_block) * tile, tile), tile)

        def slot(key_block):
            return pl.ds(pl.multiple_of((key_block - low) * tile, tile), tile)

        def score_pass(key_block, highs):
            rows = k_ref[rows_of(key_block), :]
            key_pos = key_block * tile + lax.broadcasted_iota(jnp.int32, (tile, tile), 0)
            allowed = (key_pos >= begin) & (key_pos <= q_pos)
            result = []
            for h in range(heads):
                scores = jnp.where(allowed, mm_nt(rows, q_heads[h]), masked_score)
                score_ref[h, slot(key_block), :] = scores
                result.append(jnp.maximum(highs[h], jnp.max(scores, axis=0, keepdims=True)))
            return tuple(result)

        highs = lax.fori_loop(
            low, block + 1, score_pass,
            tuple(jnp.full((1, tile), masked_score, F32) for _ in range(heads)),
        )

        def prob_pass(key_block, carry):
            result = []
            rows = rows_of(key_block)
            for h in range(heads):
                total, mixed = carry[2 * h], carry[2 * h + 1]
                probs = jnp.exp(score_ref[h, slot(key_block), :] - highs[h])
                total = total + jnp.sum(probs, axis=0, keepdims=True)
                probs = probs.astype(BF)
                prob_ref[h, slot(key_block), :] = probs
                mixed = mixed + mm(vt_ref[h * HEAD : (h + 1) * HEAD, rows], probs)
                result += [total, mixed]
            return tuple(result)

        start = []
        for h in range(heads):
            start += [jnp.zeros((1, tile), F32), jnp.zeros((HEAD, tile), F32)]
        summed = lax.fori_loop(low, block + 1, prob_pass, tuple(start))

        grads_t = grads_here.astype(F32).T
        mixed_parts, scaled_parts, deltas = [], [], []
        for h in range(heads):
            inverse = 1.0 / summed[2 * h]
            mixed = summed[2 * h + 1] * inverse
            grads = grads_t[h * HEAD : (h + 1) * HEAD, :] * inverse
            deltas.append(jnp.sum(mixed * grads, axis=0, keepdims=True))
            mixed_parts.append(mixed)
            scaled_parts.append(grads)
        mix_ref[...] = jnp.concatenate(mixed_parts, axis=0).T.astype(BF)
        scaled = jnp.concatenate(scaled_parts, axis=0).T.astype(BF)
        g_heads = [jnp.where(own[h], scaled, jnp.zeros_like(scaled)) for h in range(heads)]

        def grad_pass(key_block, grads_q):
            rows = rows_of(key_block)
            value_rows = v_ref[rows, :]
            result = []
            grad_k = gk_acc[rows, :]
            grad_v = gv_acc[rows, :]
            for h in range(heads):
                probs = prob_ref[h, slot(key_block), :]
                grad_probs = mm_nt(value_rows, g_heads[h])
                grad_scores = (probs.astype(F32) * (grad_probs - deltas[h])).astype(BF)
                grad_v = grad_v + mm(probs, g_heads[h])
                grad_k = grad_k + mm(grad_scores, q_heads[h])
                result.append(
                    grads_q[h] + mm(kt_ref[h * HEAD : (h + 1) * HEAD, rows], grad_scores)
                )
            gk_acc[rows, :] = grad_k
            gv_acc[rows, :] = grad_v
            return tuple(result)

        grads_q = lax.fori_loop(
            low, block + 1, grad_pass, tuple(jnp.zeros((HEAD, tile), F32) for _ in range(heads))
        )
        here = rows_of(block)
        rot = (jnp.concatenate(grads_q, axis=0) * scale).T
        grad_q = turn(
            rot, spread_lanes(cos_ref[here, :], hw), spread_lanes(sin_ref[here, :], hw), -1.0
        ).astype(BF)
        gq_ref[...] = grad_q
        sum_ref[0:1, :] += jnp.sum(grad_q.astype(F32), axis=0, keepdims=True)

        @pl.when(block == count - 1)
        def _():
            def finish(t, carry):
                rows = pl.ds(pl.multiple_of(t * tile, tile), tile)
                grad_k = turn(
                    gk_acc[rows, :],
                    spread_lanes(cos_ref[rows, :], hw),
                    spread_lanes(sin_ref[rows, :], hw),
                    -1.0,
                ).astype(BF)
                grad_v = gv_acc[rows, :].astype(BF)
                gk_ref[rows, :] = grad_k
                gv_ref[rows, :] = grad_v
                sum_ref[1:2, :] += jnp.sum(grad_k.astype(F32), axis=0, keepdims=True)
                sum_ref[2:3, :] += jnp.sum(grad_v.astype(F32), axis=0, keepdims=True)
                return carry

            lax.fori_loop(0, count, finish, 0)

    tiled = pl.BlockSpec((tile, hw), lambda i, ids_ref: (place(ids_ref, i), 0))
    shape = jax.ShapeDtypeStruct((seq, hw), BF)
    return pl.pallas_call(
        kernel,
        out_shape=[shape] * 4 + [jax.ShapeDtypeStruct((8, hw), F32)],
        grid_spec=pltpu.PrefetchScalarGridSpec(
            num_scalar_prefetch=1,
            grid=(count,),
            in_specs=[
                tiled,
                whole((seq, hw)),
                whole((seq, hw)),
                whole((hw, seq)),
                whole((hw, seq)),
                tiled,
                whole(cos_table.shape),
                whole(sin_table.shape),
            ],
            out_specs=[tiled, tiled, whole((seq, hw)), whole((seq, hw)), whole((8, hw))],
            scratch_shapes=[
                pltpu.VMEM((heads, seq, tile), F32),
                pltpu.VMEM((heads, seq, tile), BF),
                pltpu.VMEM((seq, hw), F32),
                pltpu.VMEM((seq, hw), F32),
            ],
        ),
        compiler_params=params_of(),
        cost_estimate=pl.CostEstimate(
            flops=12 * seq * seq * hw, bytes_accessed=10 * seq * hw * 2, transcendentals=0
        ),
        name="attention",
    )(ids, queries, keys, values, keys_t, values_t, grad_mix, cos_table, sin_table)


def split_specs(dims, tile):
    per = dims.tokens // tile
    shape = jax.ShapeDtypeStruct((dims.nx, dims.tokens, dims.width), BF)

    def spec(odd):
        def index(i, ids_ref):
            block, t = i // per, i % per
            mine = block % 2 == odd
            row = jnp.where(mine, t, per - 1 if odd == 0 else 0)
            return (block // 2, row, 0)

        return pl.BlockSpec((None, tile, dims.width), index)

    return [(shape, spec(1)), (shape, spec(0))], per


def put_split(step, per, outs, value):
    odd = (step // per) % 2

    @pl.when(odd == 1)
    def _():
        outs[0][...] = value

    @pl.when(odd == 0)
    def _():
        outs[1][...] = value


def out_body(per, step, count, lhs, weights, extras, outs, scratch):
    value = mm(lhs[0][...], weights[0][...]) + mm(lhs[1][...], weights[1][...])
    put_split(step, per, outs, value.astype(BF))


def up_grad_body(step, count, lhs, weights, extras, outs, scratch):
    grads = (mm_nt(lhs[0][...], weights[0][...]) * lhs[1][...].astype(F32)).astype(BF)
    outs[0][...] = grads

    @pl.when(step == 0)
    def _():
        outs[1][...] = jnp.zeros_like(outs[1])

    outs[1][0:1, :] += jnp.sum(grads.astype(F32), axis=0, keepdims=True)


def in_grad_body(per, hw, step, count, lhs, weights, extras, outs, scratch):
    up_grad, gq, gk, gv, hat_ref = lhs
    qkv_ref, up_ref = weights
    affine = extras[0]
    attn = (
        mm_nt(gq[...], qkv_ref[:, :hw])
        + mm_nt(gk[...], qkv_ref[:, hw : 2 * hw])
        + mm_nt(gv[...], qkv_ref[:, 2 * hw :])
    )
    ffn = mm_nt(up_grad[...], up_ref[...])
    hat = hat_ref[...].astype(F32)

    @pl.when(step == 0)
    def _():
        outs[2][...] = jnp.zeros_like(outs[2])

    for row, value in enumerate((attn * hat, attn, ffn * hat, ffn)):
        outs[2][row : row + 1, :] += jnp.sum(value, axis=0, keepdims=True)
    put_split(step, per, outs, (attn * affine[0:1, :] + ffn * affine[2:3, :]).astype(BF))


def weight_grad(dims, name, kind, ids, left, rights):
    tile = 512
    m = left.shape[1]
    widths = [r.shape[1] for r in rights]
    n = sum(widths)
    count = dims.seq // tile
    hi, lo, ns, nd = dims.hi, dims.lo, dims.ns, dims.nd
    if kind == "row":
        rows = m // nd
        shape = (hi, rows, n)
    else:
        rows = m // (nd * ns)
        shape = (hi, ns, rows, n)

    def kernel(ids_ref, left_ref, *refs):
        right_refs = refs[: len(rights)]
        out_refs = refs[len(rights) : len(rights) + lo]
        total = refs[-1]
        step = pl.program_id(0)
        at = 0
        for width, right_ref in zip(widths, right_refs):
            part = mm_tn(left_ref[...], right_ref[...])
            cols = slice(at, at + width)

            @pl.when(step == 0)
            def _():
                total[:, cols] = part

            @pl.when(step > 0)
            def _():
                total[:, cols] += part

            at += width

        @pl.when(step == count - 1)
        def _():
            s, z, y = ids_ref[0], ids_ref[1], ids_ref[2]
            for jy in range(lo):
                for jz in range(hi):
                    owner = (z ^ jz) * lo + (y ^ jy)
                    if kind == "row":
                        at = pl.multiple_of(owner * rows, rows)
                        out_refs[jy][jz] = total[pl.ds(at, rows), :].astype(BF)
                    else:
                        for js in range(ns):
                            at = pl.multiple_of(((s ^ js) * nd + owner) * rows, rows)
                            out_refs[jy][jz, js] = total[pl.ds(at, rows), :].astype(BF)

    return pl.pallas_call(
        kernel,
        out_shape=[jax.ShapeDtypeStruct(shape, BF)] * lo,
        grid_spec=pltpu.PrefetchScalarGridSpec(
            num_scalar_prefetch=1,
            grid=(count,),
            in_specs=[pl.BlockSpec((tile, m), lambda i, ids_ref: (i, 0))]
            + [pl.BlockSpec((tile, w), lambda i, ids_ref: (i, 0)) for w in widths],
            out_specs=[whole(shape)] * lo,
            scratch_shapes=[pltpu.VMEM((m, n), F32)],
        ),
        compiler_params=params_of(),
        cost_estimate=pl.CostEstimate(
            flops=2 * dims.seq * m * n,
            bytes_accessed=2 * (dims.seq * (m + n) + m * n),
            transcendentals=0,
        ),
        name=name,
    )(ids, left, *rights)


def cut_columns(dims, ids, qkv, up):
    ns, hw, ffw = dims.ns, dims.hw, dims.ffw
    rows = qkv.shape[0]

    def kernel(ids_ref, qkv_ref, up_ref, *outs):
        for js in range(ns):
            other = ids_ref[0] ^ js
            for part in range(3):
                at = pl.multiple_of(part * dims.width + other * hw, hw)
                outs[js][:, part * hw : (part + 1) * hw] = qkv_ref[:, pl.ds(at, hw)]
            at = pl.multiple_of(other * ffw, ffw)
            outs[js][:, 3 * hw :] = up_ref[:, pl.ds(at, ffw)]

    shape = (rows, 3 * hw + ffw)
    return pl.pallas_call(
        kernel,
        out_shape=[jax.ShapeDtypeStruct(shape, BF)] * ns,
        grid_spec=pltpu.PrefetchScalarGridSpec(
            num_scalar_prefetch=1,
            grid=(1,),
            in_specs=[whole(qkv.shape), whole(up.shape)],
            out_specs=[whole(shape)] * ns,
        ),
        compiler_params=params_of(),
        name="cut_columns",
    )(ids, qkv, up)


def join_columns(dims, ids, pieces, parts, width):
    ns = dims.ns
    rows, n = pieces[0].shape
    w = n // parts
    total = n * ns

    def kernel(ids_ref, *refs):
        out = refs[-1]
        for js in range(ns):
            other = ids_ref[0] ^ js
            for part in range(parts):
                at = pl.multiple_of(part * width + other * w, w)
                out[:, pl.ds(at, w)] = refs[js][:, part * w : (part + 1) * w].astype(F32)

    return pl.pallas_call(
        kernel,
        out_shape=jax.ShapeDtypeStruct((rows, total), F32),
        grid_spec=pltpu.PrefetchScalarGridSpec(
            num_scalar_prefetch=1,
            grid=(1,),
            in_specs=[whole((rows, n))] * ns,
            out_specs=whole((rows, total)),
        ),
        compiler_params=params_of(),
        name="join_columns",
    )(ids, *pieces)


class Net:
    def __init__(self, send, recv):
        self.send_sems, self.recv_sems, self.copies = send, recv, []

    def send(self, source, target, **peer):
        at = len(self.copies)
        copy = pltpu.make_async_remote_copy(
            src_ref=source,
            dst_ref=target,
            send_sem=self.send_sems.at[at],
            recv_sem=self.recv_sems.at[at],
            device_id=peer,
            device_id_type=pl.DeviceIdType.MESH,
        )
        copy.start()
        self.copies.append(copy)
        return copy

    def finish(self):
        for copy in self.copies:
            copy.wait_send()


class Local:
    def __init__(self, sems):
        self.sems, self.copies = sems, []

    def copy(self, source, target):
        done = pltpu.make_async_copy(source, target, self.sems.at[len(self.copies)])
        done.start()
        self.copies.append(done)
        return done


def greet(peers):
    barrier = pltpu.get_barrier_semaphore()
    for peer in peers:
        pl.semaphore_signal(
            barrier, inc=1, device_id=peer, device_id_type=pl.DeviceIdType.MESH
        )
    pl.semaphore_wait(barrier, len(peers))


def lane_row(ref, start, count):
    parts = [ref[pl.ds(start + k, 1), :] for k in range(count)]
    return parts[0] if count == 1 else jnp.concatenate(parts, axis=1)


def table_constants():
    half = ROT // 2
    table = 2 * HEAD
    constants = np.zeros((24, table), np.float32)
    for lane in range(table):
        if lane % HEAD < ROT:
            constants[lane % HEAD % half, lane] = 1.0
            constants[half + lane % HEAD % half, lane] = -1.0 if lane % HEAD < half else 1.0
        else:
            constants[2 * half, lane] = 1.0
    return constants


def gather_kernel(dims, rows_at, hidden, grad_out, meta, small, qkv, up, dense, down):
    ns, nd, hi, lo, nx = dims.ns, dims.nd, dims.hi, dims.lo, dims.nx
    tokens, width, hw, ffw, seq = dims.tokens, dims.width, dims.hw, dims.ffw, dims.seq
    share = qkv.shape[0]
    down_share = down.shape[0]
    dense_share = dense.shape[0]
    small_rows = small.shape[0]
    stages = []
    mask = 2
    while mask < ns:
        stages.append(("seq", mask))
        mask *= 2
    stages.append(("seq", 1))
    mask = 1
    while mask < nd:
        stages.append(("dp", mask))
        mask *= 2
    n_net = 160
    n_local = 64

    def kernel(
        hid, gout, meta_ref, small_ref, qkv_ref, up_ref, dense_ref, down_ref, const_ref,
        attn_out, ffn_out, hat_out, g_out, act_out, slope_out, q_out, k_out, v_out, kt_out,
        vt_out, mix_out, qkv_out, up_out, dense_out, down_out, cos_out, sin_out, meta_out,
        small_out,
        h_buf, g_buf, attn_buf, ffn_buf, hat_buf, act_buf, slope_buf, q_buf, k_buf, v_buf,
        kt_buf, vt_buf, mix_buf, w_qkv, w_up, w_dense, w_down, cos_buf, sin_buf, meta_buf,
        small_send, small_recv, small_full, affine,
        send_sems, recv_sems, local_sems,
    ):
        s, d = lax.axis_index("seq"), lax.axis_index("dp")
        z, y = d // lo, d % lo
        net, local = Net(send_sems, recv_sems), Local(local_sems)

        greet(
            [{"seq": s ^ js} for js in range(1, ns)]
            + [{"dp": d ^ (jz * lo)} for jz in range(1, hi)]
            + [{"dp": d ^ jy} for jy in range(1, lo)]
        )

        def block(ref, j):
            return ref.at[j * tokens : (j + 1) * tokens]

        def stage(k, source):
            axis, by = stages[k]
            where = {axis: (s if axis == "seq" else d) ^ by}
            return net.send(source, small_recv.at[k], **where)

        flight = stage(0, small_ref)
        metas = [net.send(meta_ref, meta_buf.at[js], seq=s ^ js) for js in range(1, ns)]
        meta_own = local.copy(meta_ref, meta_buf.at[0])
        h_own = local.copy(hid, block(h_buf, 0))
        g_own = local.copy(gout, block(g_buf, 0))
        h_core = net.send(hid, block(h_buf, 1), seq=s ^ 1)

        def to_columns(js):
            other = s ^ js
            pairs = []
            for part in range(3):
                at = pl.multiple_of(part * width + other * hw, hw)
                pairs.append(
                    (
                        qkv_ref.at[:, pl.ds(at, hw)],
                        w_qkv.at[s, d, :, part * hw : (part + 1) * hw],
                    )
                )
            at = pl.multiple_of(other * ffw, ffw)
            pairs.append((up_ref.at[:, pl.ds(at, ffw)], w_up.at[s, d]))
            if js == 0:
                return [local.copy(a, b) for a, b in pairs]
            return [net.send(a, b, seq=other) for a, b in pairs]

        cut_own = to_columns(0)
        cut_core = to_columns(1)
        dense_own = local.copy(dense_ref, w_dense.at[d])
        down_own = local.copy(down_ref, w_down.at[d])
        held = small_ref[...]
        cuts = []
        h_cross, g_cross = [], []
        for k in range(len(stages)):
            flight.wait_recv()
            held = held + small_recv[k]
            if k + 1 < len(stages):
                small_send[k] = held
                flight = stage(k + 1, small_send.at[k])
            if k == 0:
                for js in range(2, ns):
                    cuts += to_columns(js)
                for m in range(1, nx):
                    h_cross.append(net.send(hid, block(h_buf, 2 * m), seq=s ^ (2 * m)))
                g_core = net.send(gout, block(g_buf, 1), seq=s ^ 1)
                for m in range(1, nx):
                    g_cross.append(net.send(gout, block(g_buf, 2 * m), seq=s ^ (2 * m)))
        small_full[...] = held.astype(F32)
        for row, name in enumerate(("attn_gain", "attn_shift", "ffn_gain", "ffn_shift")):
            affine[row : row + 1, :] = lane_row(small_full, rows_at[name], width // 128)
        small_done = local.copy(small_full, small_out)

        def along_z(weight):
            return [
                net.send(weight(d), weight(d), dp=d ^ (jz * lo)) for jz in range(1, hi)
            ]

        def along_y(weight, jz):
            at = (z ^ jz) * lo + y
            return [net.send(weight(at), weight(at), dp=d ^ jy) for jy in range(1, lo)]

        part_qkv = lambda at: w_qkv.at[:, at]
        part_up = lambda at: w_up.at[:, at]
        part_dense = lambda at: w_dense.at[at]
        part_down = lambda at: w_down.at[at]
        for done in cut_own:
            done.wait()
        for done in cut_core + cuts:
            done.wait_recv()
        z_qkv = along_z(part_qkv)
        y_qkv = along_y(part_qkv, 0)
        dense_own.wait()
        z_dense = along_z(part_dense)
        y_dense = along_y(part_dense, 0)
        z_up = along_z(part_up)
        y_up = along_y(part_up, 0)
        down_own.wait()
        z_down = along_z(part_down)
        y_down = along_y(part_down, 0)

        tile = 256

        def norm(first, last):
            def body(t, carry):
                rows = pl.ds(pl.multiple_of(t * tile, tile), tile)
                x = h_buf[rows, :].astype(F32)
                spread = x - jnp.mean(x, axis=-1, keepdims=True)
                hat = spread * lax.rsqrt(
                    jnp.mean(spread * spread, axis=-1, keepdims=True) + epsilon
                )
                attn_buf[rows, :] = (hat * affine[0:1, :] + affine[1:2, :]).astype(BF)
                ffn_buf[rows, :] = (hat * affine[2:3, :] + affine[3:4, :]).astype(BF)
                hat_buf[rows, :] = hat.astype(BF)
                return carry

            per = tokens // tile
            lax.fori_loop(first * per, last * per, body, 0)
            here = slice(first * tokens, last * tokens)
            for source, target in ((attn_buf, attn_out), (ffn_buf, ffn_out), (hat_buf, hat_out)):
                local.copy(source.at[here], target.at[here])

        h_own.wait()
        h_core.wait_recv()
        norm(0, 2)

        def forward_y(arrivals, weight):
            sent = []
            for jz, done in enumerate(arrivals, 1):
                done.wait_recv()
                sent += along_y(weight, jz)
            return sent

        y_qkv += forward_y(z_qkv, part_qkv)
        h_far = []
        for m, done in enumerate(h_cross, 1):
            done.wait_recv()
            here = block(h_buf, 2 * m)
            h_far.append(net.send(here, block(h_buf, 2 * m + 1), seq=s ^ 1))
        y_dense += forward_y(z_dense, part_dense)
        for done in h_far:
            done.wait_recv()
        norm(2, ns)

        for done in y_qkv:
            done.wait_recv()
        meta_own.wait()
        for done in metas:
            done.wait_recv()
        half = ROT // 2
        parts = hw // 128
        bias_qkv = jnp.concatenate(
            [
                lane_row(small_full, rows_at["qkv_bias"] + part * (width // 128) + s * parts, parts)
                for part in range(3)
            ],
            axis=1,
        )

        def qkv_block(j, carry):
            rows = pl.ds(pl.multiple_of(j * tokens, tokens), tokens)
            exact = lax.Precision.HIGHEST
            cosine = lax.dot_general(
                meta_buf[j, 0:half, :], const_ref[0:half, :], TN, precision=exact,
                preferred_element_type=F32,
            ) + const_ref[2 * half : 2 * half + 1, :]
            sine = lax.dot_general(
                meta_buf[j, half : 2 * half, :], const_ref[half : 2 * half, :], TN,
                precision=exact, preferred_element_type=F32,
            )
            cos_buf[rows, :] = cosine
            sin_buf[rows, :] = sine
            cosine, sine = spread_lanes(cosine, hw), spread_lanes(sine, hw)
            joined = mm(attn_buf[rows, :], w_qkv[...].reshape(width, 3 * hw)) + bias_qkv
            queries = turn(joined[:, :hw], cosine, sine, 1.0)
            keys = turn(joined[:, hw : 2 * hw], cosine, sine, 1.0)
            values = joined[:, 2 * hw :]
            q_buf[rows, :] = queries.astype(BF) * (1.0 / math.sqrt(HEAD))
            k_buf[rows, :] = keys.astype(BF)
            v_buf[rows, :] = values.astype(BF)
            kt_buf[:, rows] = keys.T.astype(BF)
            vt_buf[:, rows] = values.T.astype(BF)
            return carry

        lax.fori_loop(0, ns, qkv_block, 0)
        for source, target in (
            (q_buf, q_out), (k_buf, k_out), (v_buf, v_out), (kt_buf, kt_out), (vt_buf, vt_out),
            (cos_buf, cos_out), (sin_buf, sin_out), (w_qkv, qkv_out), (meta_buf, meta_out),
        ):
            local.copy(source, target)

        y_up += forward_y(z_up, part_up)
        g_far = []
        for m, done in enumerate(g_cross, 1):
            done.wait_recv()
            here = block(g_buf, 2 * m)
            g_far.append(net.send(here, block(g_buf, 2 * m + 1), seq=s ^ 1))
        for done in y_dense + g_far + [g_core]:
            done.wait_recv()
        g_own.wait()

        def mix_block(j, carry):
            rows = pl.ds(pl.multiple_of(j * tokens, tokens), tokens)
            mix_buf[rows, :] = mm_nt(g_buf[rows, :], w_dense[...].reshape(hw, width)).astype(BF)
            return carry

        lax.fori_loop(0, ns, mix_block, 0)
        for source, target in ((mix_buf, mix_out), (g_buf, g_out), (w_dense, dense_out)):
            local.copy(source, target)

        for done in y_up:
            done.wait_recv()
        bias_up = lane_row(small_full, rows_at["up_bias"] + s * (ffw // 128), ffw // 128)

        def up_block(t, carry):
            rows = pl.ds(pl.multiple_of(t * tile, tile), tile)
            pre = mm(ffn_buf[rows, :], w_up[...].reshape(width, ffw)) + bias_up
            total = 0.5 + 0.5 * lax.erf(pre * math.sqrt(0.5))
            density = jnp.exp(-0.5 * pre * pre) * (1.0 / math.sqrt(2.0 * math.pi))
            act_buf[rows, :] = (pre * total).astype(BF)
            slope_buf[rows, :] = (total + pre * density).astype(BF)
            return carry

        lax.fori_loop(0, seq // tile, up_block, 0)
        for source, target in ((act_buf, act_out), (slope_buf, slope_out), (w_up, up_out)):
            local.copy(source, target)

        for done in forward_y(z_down, part_down) + y_down:
            done.wait_recv()
        down_last = local.copy(w_down, down_out)
        waited = [meta_own, h_own, g_own, dense_own, down_own] + cut_own
        for done in local.copies:
            if not any(done is w for w in waited):
                done.wait()
        net.finish()

    sds = jax.ShapeDtypeStruct
    any_spec = pl.BlockSpec(memory_space=pl.ANY)
    const = jnp.asarray(table_constants())
    out_shapes = (
        [sds((seq, width), BF)] * 4
        + [sds((seq, ffw), BF)] * 2
        + [sds((seq, hw), BF)] * 3
        + [sds((hw, seq), BF)] * 2
        + [sds((seq, hw), BF)]
        + [
            sds((ns, nd, share, 3 * hw), BF),
            sds((ns, nd, share, ffw), BF),
            sds((nd, dense_share, width), BF),
            sds((nd, down_share, width), BF),
            sds((seq, 2 * HEAD), F32),
            sds((seq, 2 * HEAD), F32),
            sds((ns,) + meta.shape, F32),
            sds(small.shape, F32),
        ]
    )
    scratch = [pltpu.VMEM(x.shape, x.dtype) for x in (
        [sds((seq, width), BF)] * 2 + [sds((seq, width), BF)] * 3 + out_shapes[4:19]
    )] + [
        pltpu.VMEM((len(stages), small_rows, 128), BF),
        pltpu.VMEM((len(stages), small_rows, 128), BF),
        pltpu.VMEM((small_rows, 128), F32),
        pltpu.VMEM((8, width), F32),
        pltpu.SemaphoreType.DMA((n_net,)),
        pltpu.SemaphoreType.DMA((n_net,)),
        pltpu.SemaphoreType.DMA((n_local,)),
    ]
    return pl.pallas_call(
        kernel,
        out_shape=out_shapes,
        in_specs=[any_spec, any_spec, pl.BlockSpec(memory_space=pltpu.VMEM),
                  pl.BlockSpec(memory_space=pltpu.VMEM), any_spec, any_spec, any_spec, any_spec,
                  pl.BlockSpec(memory_space=pltpu.VMEM)],
        out_specs=[any_spec] * len(out_shapes),
        scratch_shapes=scratch,
        compiler_params=pltpu.CompilerParams(
            vmem_limit_bytes=VMEM_LIMIT, collective_id=1, has_side_effects=True
        ),
        name="gather",
    )(hidden, grad_out, meta, small, qkv, up, dense, down, const)


def permute_plan(
    hidden_states,
    segment_ids,
    positions,
    out_grad,
    qkv_weight,
    qkv_bias,
    dense_weight,
    dense_bias,
    up_weight,
    up_bias,
    down_weight,
    down_bias,
    attn_gain,
    attn_shift,
    ffn_gain,
    ffn_shift,
):
    ns, nd = lax.axis_size("seq"), lax.axis_size("dp")
    tokens, width = hidden_states.shape[1:]
    dims = Dims(ns, nd, tokens, width, up_weight.shape[1])
    hi, lo, nx = dims.hi, dims.lo, dims.nx
    hw, ffw, seq = dims.hw, dims.ffw, dims.seq
    s, d = lax.axis_index("seq"), lax.axis_index("dp")
    z, y = d // lo, d % lo
    ids = jnp.stack([s, z, y, s]).astype(jnp.int32)

    def by_seq(value, mask):
        return xor_swap(value, "seq", ns, mask)

    def by_dp(value, mask):
        return xor_swap(value, "dp", nd, mask)

    hidden, grad_out = hidden_states[0], out_grad[0]

    fields = (qkv_bias, dense_bias, up_bias, down_bias, attn_gain, attn_shift, ffn_gain, ffn_shift)
    mine = jnp.concatenate(fields)
    index = s * nd + d
    small = jnp.where(jnp.arange(ns * nd)[:, None] == index, mine[None, :], jnp.zeros((), BF))
    mask = 1
    while mask < ns:
        small = small + by_seq(small, mask)
        mask *= 2
    mask = 1
    while mask < nd:
        small = small + by_dp(small, mask)
        mask *= 2
    full, at = [], 0
    for field in fields:
        n = field.shape[0]
        full.append(small[:, at : at + n].reshape(-1).astype(F32))
        at += n
    b_qkv, b_dense, b_up, b_down, g_attn, s_attn, g_ffn, s_ffn = full
    affine = jnp.concatenate(
        [jnp.stack([g_attn, s_attn, g_ffn, s_ffn]), jnp.zeros((4, width), F32)], axis=0
    )
    bias_qkv = lax.dynamic_index_in_dim(
        b_qkv.reshape(3, ns, hw), s, 1, keepdims=False
    ).reshape(1, 3 * hw)
    bias_up = lax.dynamic_slice_in_dim(b_up, s * ffw, ffw).reshape(1, ffw)

    meta = jnp.stack([segment_ids[0], positions[0]])
    metas = [meta] + [by_seq(meta, js) for js in range(1, ns)]
    meta_all = jnp.concatenate(metas, axis=1)
    starts = [jnp.sum((meta_all[0] < v).astype(jnp.int32)) for v in range(1, DOCS)]
    doc_ids = jnp.stack([s.astype(jnp.int32)] + starts)
    half = ROT // 2
    freqs = rotary_base ** (-2.0 * jnp.arange(half, dtype=F32) / ROT)
    angles = meta_all[1].astype(F32)[None, :] * freqs[:, None]
    table = 2 * HEAD
    pick = np.zeros((half, table), np.float32)
    signed = np.zeros((half, table), np.float32)
    rest = np.ones((1, table), np.float32)
    for lane in range(table):
        if lane % HEAD < ROT:
            pick[lane % HEAD % half, lane] = 1.0
            signed[lane % HEAD % half, lane] = -1.0 if lane % HEAD < half else 1.0
            rest[0, lane] = 0.0
    exact = lax.Precision.HIGHEST
    cos_table = lax.dot_general(jnp.cos(angles), jnp.asarray(pick), TN, precision=exact) + rest
    sin_table = lax.dot_general(jnp.sin(angles), jnp.asarray(signed), TN, precision=exact)

    def gather_tokens(value):
        found = [value, by_seq(value, 1)]
        for m in range(1, nx):
            across = by_seq(value, 2 * m)
            found += [across, by_seq(across, 1)]
        return found

    blocks = gather_tokens(hidden)

    cuts = cut_columns(dims, ids, qkv_weight, up_weight)
    got = [cuts[0]] + [by_seq(cuts[js], js) for js in range(1, ns)]
    stacked = jnp.stack(got)

    def gather_dp(shard):
        pieces = []
        for jz in range(hi):
            here = shard if jz == 0 else by_dp(shard, jz * lo)
            pieces += [here] + [by_dp(here, jy) for jy in range(1, lo)]
        return pieces

    up_pieces = gather_dp(stacked[:, :, 3 * hw :])
    qkv_pieces = gather_dp(stacked[:, :, : 3 * hw])
    dense_pieces = gather_dp(dense_weight)
    down_pieces = gather_dp(down_weight)
    qkv_w = ("col", qkv_pieces, (width, 3 * hw))
    up_w = ("col", up_pieces, (width, ffw))
    dense_w = ("row", dense_pieces, (hw, width))
    down_w = ("row", down_pieces, (ffw, width))

    carried = ()
    for m in range(nx):
        carried = norm_pair(dims, m, blocks[2 * m], blocks[2 * m + 1], affine, carried)
    attn_low, ffn_low, hat_low = carried

    tile = 256
    act, slope = token_call(
        dims, "up", ids, up_body, [ffn_low], [up_w], [bias_up],
        [tiled_out(seq, ffw, tile)] * 2, tile, 2 * seq * width * ffw * 2,
    )
    flip = (
        jax.ShapeDtypeStruct((hw, seq), BF),
        pl.BlockSpec((hw, tile), lambda i, ids_ref: (0, i)),
    )
    queries, keys, values, keys_t, values_t = token_call(
        dims, "qkv", ids, functools.partial(qkv_body, dims), [attn_low, cos_table, sin_table],
        [qkv_w], [bias_qkv], [tiled_out(seq, hw, tile)] * 3 + [flip] * 2, tile,
        2 * seq * width * 3 * hw,
    )
    grads_all = jnp.concatenate(gather_tokens(grad_out), axis=0)
    grad_mix = token_call(
        dims, "mix_grad", ids, mix_grad_body, [grads_all], [dense_w], [],
        [tiled_out(seq, hw, tile)], tile, 2 * seq * width * hw,
    )[0]
    mixed, gq, gk, gv, qkv_sums = attention(
        dims, doc_ids, queries, keys, values, keys_t, values_t, grad_mix, cos_table, sin_table
    )

    def reduce_tokens(others, own):
        got = by_seq(others, 1)
        total = own[0].astype(F32) + got[0].astype(F32)
        for m in range(1, nx):
            total = total + by_seq(own[m] + got[m], 2 * m).astype(F32)
        return total

    def reduce_dp(parts):
        got = [by_dp(parts[jy], jy) for jy in range(1, lo)]

        def slab(jz):
            value = parts[0][jz].astype(F32)
            for g in got:
                value = value + g[jz].astype(F32)
            return value

        total = slab(0)
        for jz in range(1, hi):
            total = total + by_dp(slab(jz).astype(BF), jz * lo).astype(F32)
        return total

    def columns_home(total, parts):
        low = total.astype(BF)
        pieces = [low[0]] + [by_seq(low[js], js) for js in range(1, ns)]
        return join_columns(dims, ids, pieces, parts, width)

    down_parts = weight_grad(dims, "down_grad", "row", ids, act, [grads_all])
    grad_down = reduce_dp(down_parts)
    dense_parts = weight_grad(dims, "dense_grad", "row", ids, mixed, [grads_all])
    grad_dense = reduce_dp(dense_parts)
    qkv_parts = weight_grad(dims, "qkv_grad", "col", ids, attn_low, [gq, gk, gv])
    grad_qkv = columns_home(reduce_dp(qkv_parts), 3)

    sums_shape = lambda n: (jax.ShapeDtypeStruct((8, n), F32), whole((8, n)))
    grad_up_low, up_sums = token_call(
        dims, "up_grad", ids, up_grad_body, [grads_all, slope], [down_w], [],
        [tiled_out(seq, ffw, tile), sums_shape(ffw)], tile, 2 * seq * width * ffw,
    )
    up_parts = weight_grad(dims, "up_w_grad", "col", ids, ffn_low, [grad_up_low])
    grad_up = columns_home(reduce_dp(up_parts), 1)

    outs, per = split_specs(dims, tile)
    others, own = token_call(
        dims, "out", ids, functools.partial(out_body, per), [mixed, act], [dense_w, down_w], [],
        outs, tile, 2 * seq * width * (hw + ffw),
    )
    out_total = reduce_tokens(others, own)
    output = (hidden.astype(F32) + out_total + (b_dense + b_down)[None, :]).astype(BF)

    others, own, gain_sums = token_call(
        dims, "in_grad", ids, functools.partial(in_grad_body, per, hw),
        [grad_up_low, gq, gk, gv, hat_low], [qkv_w, up_w], [affine],
        outs + [sums_shape(width)], tile, 2 * seq * width * (3 * hw + ffw),
    )
    gx = reduce_tokens(others, own)
    rows = hidden.astype(F32)
    spread = rows - jnp.mean(rows, axis=-1, keepdims=True)
    inv_std = lax.rsqrt(jnp.mean(spread * spread, axis=-1, keepdims=True) + epsilon)
    hat = spread * inv_std
    back = inv_std * (
        gx
        - jnp.mean(gx, axis=-1, keepdims=True)
        - hat * jnp.mean(gx * hat, axis=-1, keepdims=True)
    )
    grad_out_f = grad_out.astype(F32)
    input_grad = (grad_out_f + back).astype(BF)

    def placed(value, parts, w):
        base = jnp.zeros((parts, ns, w), F32)
        return lax.dynamic_update_slice_in_dim(base, value.reshape(parts, 1, w), s, 1).reshape(-1)

    out_sum = jnp.sum(grad_out_f, axis=0)
    vectors = (
        placed(qkv_sums[:3], 3, hw),
        out_sum,
        placed(up_sums[0], 1, ffw),
        gain_sums[0],
        gain_sums[1],
        gain_sums[2],
        gain_sums[3],
    )
    packed = jnp.concatenate(vectors).reshape(-1, 128)
    mask = 1
    while mask < ns:
        packed = packed + by_seq(packed, mask)
        mask *= 2
    mask = 1
    while mask < nd:
        packed = packed + by_dp(packed, mask)
        mask *= 2
    flat = packed.reshape(-1)
    small_out, at = [], 0
    for vector in vectors:
        n = vector.shape[0]
        share = n // (ns * nd)
        small_out.append(lax.dynamic_slice_in_dim(flat, at + index * share, share))
        at += n
    gb_qkv, gb_out, gb_up, gg_attn, gs_attn, gg_ffn, gs_ffn = small_out
    return (
        output[None],
        input_grad[None],
        grad_qkv,
        gb_qkv,
        grad_dense,
        gb_out,
        grad_up,
        gb_up,
        grad_down,
        gb_out,
        gg_attn,
        gs_attn,
        gg_ffn,
        gs_ffn,
    )


def fused_plan(
    hidden_states,
    segment_ids,
    positions,
    out_grad,
    qkv_weight,
    qkv_bias,
    dense_weight,
    dense_bias,
    up_weight,
    up_bias,
    down_weight,
    down_bias,
    attn_gain,
    attn_shift,
    ffn_gain,
    ffn_shift,
):
    ns, nd = lax.axis_size("seq"), lax.axis_size("dp")
    tokens, width = hidden_states.shape[1:]
    dims = Dims(ns, nd, tokens, width, up_weight.shape[1])
    hi, lo, nx = dims.hi, dims.lo, dims.nx
    hw, ffw, seq = dims.hw, dims.ffw, dims.seq
    s, d = lax.axis_index("seq"), lax.axis_index("dp")
    index = s * nd + d
    ids = jnp.stack([s, d // lo, d % lo, s]).astype(jnp.int32)

    def by_seq(value, mask):
        return xor_swap(value, "seq", ns, mask)

    def by_dp(value, mask):
        return xor_swap(value, "dp", nd, mask)

    hidden, grad_out = hidden_states[0], out_grad[0]
    fields = {
        "qkv_bias": qkv_bias,
        "dense_bias": dense_bias,
        "up_bias": up_bias,
        "down_bias": down_bias,
        "attn_gain": attn_gain,
        "attn_shift": attn_shift,
        "ffn_gain": ffn_gain,
        "ffn_shift": ffn_shift,
    }
    rows_at, row = {}, 0
    for name, field in fields.items():
        rows_at[name] = row
        row += field.shape[0] * ns * nd // 128
    small_rows = -(-row // 16) * 16
    small = jnp.zeros((small_rows * 128,), BF)
    for name, field in fields.items():
        at = rows_at[name] * 128 + index * field.shape[0]
        small = lax.dynamic_update_slice_in_dim(small, field, at, 0)
    small = small.reshape(small_rows, 128)
    half = ROT // 2
    freqs = rotary_base ** (-2.0 * jnp.arange(half, dtype=F32) / ROT)
    angles = positions[0].astype(F32)[None, :] * freqs[:, None]
    meta = jnp.concatenate(
        [
            jnp.cos(angles),
            jnp.sin(angles),
            jnp.broadcast_to(segment_ids[0].astype(F32)[None, :], (half, tokens)),
        ],
        axis=0,
    )
    (
        attn_low, ffn_low, hat_low, grads_all, act, slope, queries, keys, values, keys_t, values_t,
        grad_mix, qkv_full, up_full, dense_full, down_full, cos_table, sin_table, meta_all,
        small_all,
    ) = gather_kernel(
        dims, rows_at, hidden, grad_out, meta, small, qkv_weight, up_weight, dense_weight,
        down_weight,
    )
    segments = meta_all[:, 2 * half]
    starts = [jnp.sum((segments < v).astype(jnp.int32)) for v in range(1, DOCS)]
    doc_ids = jnp.stack([s.astype(jnp.int32)] + starts)
    qkv_w = ("full", [qkv_full.reshape(width, 3 * hw)], (width, 3 * hw))
    up_w = ("full", [up_full.reshape(width, ffw)], (width, ffw))
    dense_w = ("full", [dense_full.reshape(hw, width)], (hw, width))
    down_w = ("full", [down_full.reshape(ffw, width)], (ffw, width))
    take = lambda name: small_all[rows_at[name] : rows_at[name] + width // 128].reshape(-1)
    affine = jnp.concatenate(
        [
            jnp.stack([take(n) for n in ("attn_gain", "attn_shift", "ffn_gain", "ffn_shift")]),
            jnp.zeros((4, width), F32),
        ],
        axis=0,
    )
    b_dense, b_down = take("dense_bias"), take("down_bias")
    tile = 256
    mixed, gq, gk, gv, qkv_sums = attention(
        dims, doc_ids, queries, keys, values, keys_t, values_t, grad_mix, cos_table, sin_table
    )

    def reduce_tokens(others, own):
        got = by_seq(others, 1)
        total = own[0].astype(F32) + got[0].astype(F32)
        for m in range(1, nx):
            total = total + by_seq(own[m] + got[m], 2 * m).astype(F32)
        return total

    def reduce_dp(parts):
        got = [by_dp(parts[jy], jy) for jy in range(1, lo)]

        def slab(jz):
            value = parts[0][jz].astype(F32)
            for g in got:
                value = value + g[jz].astype(F32)
            return value

        total = slab(0)
        for jz in range(1, hi):
            total = total + by_dp(slab(jz).astype(BF), jz * lo).astype(F32)
        return total

    def columns_home(total, parts):
        low = total.astype(BF)
        pieces = [low[0]] + [by_seq(low[js], js) for js in range(1, ns)]
        return join_columns(dims, ids, pieces, parts, width)

    down_parts = weight_grad(dims, "down_grad", "row", ids, act, [grads_all])
    grad_down = reduce_dp(down_parts)
    dense_parts = weight_grad(dims, "dense_grad", "row", ids, mixed, [grads_all])
    grad_dense = reduce_dp(dense_parts)
    qkv_parts = weight_grad(dims, "qkv_grad", "col", ids, attn_low, [gq, gk, gv])
    grad_qkv = columns_home(reduce_dp(qkv_parts), 3)

    sums_shape = lambda n: (jax.ShapeDtypeStruct((8, n), F32), whole((8, n)))
    grad_up_low, up_sums = token_call(
        dims, "up_grad", ids, up_grad_body, [grads_all, slope], [down_w], [],
        [tiled_out(seq, ffw, tile), sums_shape(ffw)], tile, 2 * seq * width * ffw,
    )
    up_parts = weight_grad(dims, "up_w_grad", "col", ids, ffn_low, [grad_up_low])
    grad_up = columns_home(reduce_dp(up_parts), 1)

    outs, per = split_specs(dims, tile)
    others, own = token_call(
        dims, "out", ids, functools.partial(out_body, per), [mixed, act], [dense_w, down_w], [],
        outs, tile, 2 * seq * width * (hw + ffw),
    )
    out_total = reduce_tokens(others, own)
    output = (hidden.astype(F32) + out_total + (b_dense + b_down)[None, :]).astype(BF)

    others, own, gain_sums = token_call(
        dims, "in_grad", ids, functools.partial(in_grad_body, per, hw),
        [grad_up_low, gq, gk, gv, hat_low], [qkv_w, up_w], [affine],
        outs + [sums_shape(width)], tile, 2 * seq * width * (3 * hw + ffw),
    )
    gx = reduce_tokens(others, own)
    rows = hidden.astype(F32)
    spread = rows - jnp.mean(rows, axis=-1, keepdims=True)
    inv_std = lax.rsqrt(jnp.mean(spread * spread, axis=-1, keepdims=True) + epsilon)
    hat = spread * inv_std
    back = inv_std * (
        gx
        - jnp.mean(gx, axis=-1, keepdims=True)
        - hat * jnp.mean(gx * hat, axis=-1, keepdims=True)
    )
    grad_out_f = grad_out.astype(F32)
    input_grad = (grad_out_f + back).astype(BF)

    def placed(value, parts, w):
        base = jnp.zeros((parts, ns, w), F32)
        return lax.dynamic_update_slice_in_dim(base, value.reshape(parts, 1, w), s, 1).reshape(-1)

    out_sum = jnp.sum(grad_out_f, axis=0)
    vectors = (
        placed(qkv_sums[:3], 3, hw),
        out_sum,
        placed(up_sums[0], 1, ffw),
        gain_sums[0],
        gain_sums[1],
        gain_sums[2],
        gain_sums[3],
    )
    packed = jnp.concatenate(vectors).reshape(-1, 128)
    mask = 1
    while mask < ns:
        packed = packed + by_seq(packed, mask)
        mask *= 2
    mask = 1
    while mask < nd:
        packed = packed + by_dp(packed, mask)
        mask *= 2
    flat = packed.reshape(-1)
    small_out, at = [], 0
    for vector in vectors:
        n = vector.shape[0]
        share = n // (ns * nd)
        small_out.append(lax.dynamic_slice_in_dim(flat, at + index * share, share))
        at += n
    gb_qkv, gb_out, gb_up, gg_attn, gs_attn, gg_ffn, gs_ffn = small_out
    return (
        output[None],
        input_grad[None],
        grad_qkv,
        gb_qkv,
        grad_dense,
        gb_out,
        grad_up,
        gb_up,
        grad_down,
        gb_out,
        gg_attn,
        gs_attn,
        gg_ffn,
        gs_ffn,
    )


def per_device(*args):
    tokens, width = args[0].shape[1:]
    ns, nd = lax.axis_size("seq"), lax.axis_size("dp")
    fits = ns * tokens * width <= 2048 * 1024 and width // (ns * nd) % 16 == 0
    return fused_plan(*args) if fits else permute_plan(*args)


def solution(mesh):
    token = P("dp", "seq", None)
    matrix = P(("seq", "dp"), None)
    vector = P(("seq", "dp"))
    weights = (matrix, vector) * 4 + (vector,) * 4
    return jax.shard_map(
        per_device,
        mesh=mesh,
        in_specs=(token, P("dp", "seq"), P("dp", "seq"), token) + weights,
        out_specs=(token, token) + weights,
        check_vma=False,
    )
```

```python
import functools
import math

import jax
import jax.numpy as jnp
import numpy as np
from jax import lax
from jax.experimental import pallas as pl
from jax.experimental.pallas import tpu as pltpu
from jax.sharding import PartitionSpec as P

HEAD = 64
ROT = 16
DOCS = 4
HI = 4

epsilon = 1e-05
masked_score = -1e30
rotary_base = 10000.0

BF = jnp.bfloat16
F32 = jnp.float32
NT = (((1,), (1,)), ((), ()))
TN = (((0,), (0,)), ((), ()))


VMEM_LIMIT = 60 * 1024 * 1024
MAIN_LIMIT = 61 * 1024 * 1024


def xor_swap(value, axis, count, mask):
    return lax.ppermute(value, axis, [(i, i ^ mask) for i in range(count)])


def mm(left, right):
    return jnp.dot(left, right, preferred_element_type=F32)


def mm_nt(left, right):
    return lax.dot_general(left, right, NT, preferred_element_type=F32)


def mm_tn(left, right):
    return lax.dot_general(left, right, TN, preferred_element_type=F32)


def params_of(**more):
    return pltpu.CompilerParams(vmem_limit_bytes=VMEM_LIMIT, **more)


def whole(shape):
    zeros = (0,) * len(shape)
    return pl.BlockSpec(shape, lambda *grid_and_ids: zeros)


class Dims:
    def __init__(self, ns, nd, tokens, width, ff):
        self.ns, self.nd = ns, nd
        self.hi, self.lo = HI, nd // HI
        self.nx = ns // 2
        self.tokens, self.width = tokens, width
        self.seq = ns * tokens
        self.hw = width // ns
        self.ffw = ff // ns
        self.heads = self.hw // HEAD


def piece_copies(dims, kind, ids, pieces, target, sems):
    s, z, y = ids[0], ids[1], ids[2]
    copies = []
    for jz in range(dims.hi):
        for jy in range(dims.lo):
            piece = pieces[jz * dims.lo + jy]
            owner = (z ^ jz) * dims.lo + (y ^ jy)
            if kind == "row":
                rows = piece.shape[0]
                at = pl.multiple_of(owner * rows, rows)
                copies.append(
                    pltpu.make_async_copy(piece, target.at[pl.ds(at, rows)], sems.at[len(copies)])
                )
            else:
                rows = piece.shape[1]
                for js in range(dims.ns):
                    at = pl.multiple_of(((s ^ js) * dims.nd + owner) * rows, rows)
                    copies.append(
                        pltpu.make_async_copy(
                            piece.at[js], target.at[pl.ds(at, rows)], sems.at[len(copies)]
                        )
                    )
    return copies


def token_call(dims, name, ids, body, lhs, weights, extras, outs, tile, flops, scratch=()):
    count = dims.seq // tile
    n_lhs, n_out = len(lhs), len(outs)
    sizes = [len(w[1]) for w in weights]
    sem_counts = [
        len(w[1]) * (dims.ns if w[0] == "col" else 1) for w in weights
    ]

    def kernel(ids_ref, *refs):
        at = 0
        lhs_refs = refs[:n_lhs]
        at = n_lhs
        piece_refs = []
        for size in sizes:
            piece_refs.append(refs[at : at + size])
            at += size
        extra_refs = refs[at : at + len(extras)]
        at += len(extras)
        out_refs = refs[at : at + n_out]
        at += n_out
        weight_refs = refs[at : at + len(weights)]
        at += len(weights)
        sem_refs = refs[at : at + len(weights)]
        at += len(weights)
        scratch_refs = refs[at:]
        step = pl.program_id(0)

        if weights:

            @pl.when(step == 0)
            def _():
                copies = []
                for w, group, target, sems in zip(weights, piece_refs, weight_refs, sem_refs):
                    copies += piece_copies(dims, w[0], ids_ref, group, target, sems)
                for copy in copies:
                    copy.start()
                for copy in copies:
                    copy.wait()

        body(step, count, lhs_refs, weight_refs, extra_refs, out_refs, scratch_refs)

    in_specs = [pl.BlockSpec((tile, a.shape[1]), lambda i, ids_ref: (i, 0)) for a in lhs]
    for size in sizes:
        in_specs += [pl.BlockSpec(memory_space=pl.ANY)] * size
    in_specs += [whole(a.shape) for a in extras]
    bytes_moved = sum(a.size * a.dtype.itemsize for a in lhs) + sum(
        math.prod(o[0].shape) * o[0].dtype.itemsize for o in outs
    )
    return pl.pallas_call(
        kernel,
        out_shape=[o[0] for o in outs],
        grid_spec=pltpu.PrefetchScalarGridSpec(
            num_scalar_prefetch=1,
            grid=(count,),
            in_specs=in_specs,
            out_specs=[o[1] for o in outs],
            scratch_shapes=[pltpu.VMEM(w[2], BF) for w in weights]
            + [pltpu.SemaphoreType.DMA((n,)) for n in sem_counts]
            + list(scratch),
        ),
        compiler_params=params_of(),
        cost_estimate=pl.CostEstimate(flops=flops, bytes_accessed=bytes_moved, transcendentals=0),
        name=name,
    )(ids, *lhs, *[p for w in weights for p in w[1]], *extras)


def tiled_out(rows, cols, tile, dtype=BF):
    return (
        jax.ShapeDtypeStruct((rows, cols), dtype),
        pl.BlockSpec((tile, cols), lambda i, ids_ref: (i, 0)),
    )


def norm_pair(dims, pair, first, second, affine, carried):
    tile = 256
    per = dims.tokens // tile
    base = pair * 2 * per

    def kernel(*refs):
        a_ref, b_ref, affine_ref = refs[:3]
        attn_ref, ffn_ref, hat_ref, rows_ref = refs[-4:]
        block = pl.program_id(0)

        @pl.when(block == 0)
        def _():
            rows_ref[...] = a_ref[...]

        @pl.when(block == 1)
        def _():
            rows_ref[...] = b_ref[...]

        rows = rows_ref[...].astype(F32)
        center = jnp.mean(rows, axis=-1, keepdims=True)
        spread = rows - center
        hat = spread * lax.rsqrt(jnp.mean(spread * spread, axis=-1, keepdims=True) + epsilon)
        attn_ref[...] = (hat * affine_ref[0:1, :] + affine_ref[1:2, :]).astype(BF)
        ffn_ref[...] = (hat * affine_ref[2:3, :] + affine_ref[3:4, :]).astype(BF)
        hat_ref[...] = hat.astype(BF)

    out_spec = pl.BlockSpec((tile, dims.width), lambda b, t: (base + b * per + t, 0))
    shape = jax.ShapeDtypeStruct((dims.seq, dims.width), BF)
    return pl.pallas_call(
        kernel,
        out_shape=[shape] * 3,
        grid=(2, per),
        in_specs=[
            pl.BlockSpec((tile, dims.width), lambda b, t: (jnp.where(b == 0, t, per - 1), 0)),
            pl.BlockSpec((tile, dims.width), lambda b, t: (jnp.where(b == 0, 0, t), 0)),
            pl.BlockSpec((8, dims.width), lambda b, t: (0, 0)),
        ]
        + [pl.BlockSpec(memory_space=pl.ANY)] * len(carried),
        out_specs=[out_spec] * 3,
        scratch_shapes=[pltpu.VMEM((tile, dims.width), BF)],
        input_output_aliases={3 + i: i for i in range(len(carried))},
        compiler_params=params_of(),
        cost_estimate=pl.CostEstimate(
            flops=20 * 2 * dims.tokens * dims.width,
            bytes_accessed=2 * dims.tokens * dims.width * 8,
            transcendentals=0,
        ),
        name="norm_pair",
    )(first, second, affine, *carried)


def up_body(step, count, lhs, weights, extras, outs, scratch):
    pre = mm(lhs[0][...], weights[0][...]) + extras[0][0:1, :]
    total = 0.5 + 0.5 * lax.erf(pre * math.sqrt(0.5))
    density = jnp.exp(-0.5 * pre * pre) * (1.0 / math.sqrt(2.0 * math.pi))
    outs[0][...] = (pre * total).astype(BF)
    outs[1][...] = (total + pre * density).astype(BF)


def turn(values, cosine, sine, sign):
    lane = lax.broadcasted_iota(jnp.int32, (1, values.shape[1]), 1) % HEAD
    width = values.shape[1]
    half = ROT // 2
    other = jnp.where(
        lane < half, pltpu.roll(values, width - half, 1), pltpu.roll(values, half, 1)
    )
    return values * cosine + sign * (other * sine)


def spread_lanes(table, width):
    times = width // table.shape[1]
    return table if times == 1 else jnp.concatenate([table] * times, axis=1)


def qkv_body(dims, step, count, lhs, weights, extras, outs, scratch):
    hw = dims.hw
    joined = mm(lhs[0][...], weights[0][...]) + extras[0][0:1, :]
    cosine = spread_lanes(lhs[1][...], hw)
    sine = spread_lanes(lhs[2][...], hw)
    queries = turn(joined[:, :hw], cosine, sine, 1.0)
    keys = turn(joined[:, hw : 2 * hw], cosine, sine, 1.0)
    values = joined[:, 2 * hw :]
    outs[0][...] = queries.astype(BF) * (1.0 / math.sqrt(HEAD))
    outs[1][...] = keys.astype(BF)
    outs[2][...] = values.astype(BF)
    outs[3][...] = keys.T.astype(BF)
    outs[4][...] = values.T.astype(BF)


def mix_grad_body(step, count, lhs, weights, extras, outs, scratch):
    outs[0][...] = mm_nt(lhs[0][...], weights[0][...]).astype(BF)


def attention(dims, ids, queries, keys, values, keys_t, values_t, grad_mix, cos_table, sin_table):
    tile = 256
    hw, seq, heads = dims.hw, dims.seq, dims.heads
    per = dims.tokens // tile
    count = seq // tile
    scale = 1.0 / math.sqrt(HEAD)

    def place(ids_ref, block):
        return ((block // per) ^ ids_ref[0]) * per + block % per

    def kernel(
        ids_ref, q_ref, k_ref, v_ref, kt_ref, vt_ref, g_ref, cos_ref, sin_ref,
        mix_ref, gq_ref, gk_ref, gv_ref, sum_ref,
        score_ref, prob_ref, gk_acc, gv_acc,
    ):
        block = pl.program_id(0)

        @pl.when(block == 0)
        def _():
            gk_acc[...] = jnp.zeros_like(gk_acc)
            gv_acc[...] = jnp.zeros_like(gv_acc)
            sum_ref[...] = jnp.zeros_like(sum_ref)

        lane = lax.broadcasted_iota(jnp.int32, (1, hw), 1)
        own = [lane // HEAD == h for h in range(heads)]
        queries_here = q_ref[...]
        grads_here = g_ref[...]
        q_heads = [jnp.where(own[h], queries_here, jnp.zeros_like(queries_here)) for h in range(heads)]
        q_pos = block * tile + lax.broadcasted_iota(jnp.int32, (1, tile), 1)
        begin = jnp.zeros((1, tile), jnp.int32)
        low = 0
        for doc in range(1, DOCS):
            edge = ids_ref[doc]
            begin = jnp.where(q_pos >= edge, jnp.maximum(begin, edge), begin)
            low = jnp.where(edge <= block * tile, jnp.maximum(low, edge), low)
        low = low // tile

        def rows_of(key_block):
            return pl.ds(pl.multiple_of(place(ids_ref, key_block) * tile, tile), tile)

        def slot(key_block):
            return pl.ds(pl.multiple_of((key_block - low) * tile, tile), tile)

        def score_pass(key_block, highs):
            rows = k_ref[rows_of(key_block), :]
            key_pos = key_block * tile + lax.broadcasted_iota(jnp.int32, (tile, tile), 0)
            allowed = (key_pos >= begin) & (key_pos <= q_pos)
            result = []
            for h in range(heads):
                scores = jnp.where(allowed, mm_nt(rows, q_heads[h]), masked_score)
                score_ref[h, slot(key_block), :] = scores
                result.append(jnp.maximum(highs[h], jnp.max(scores, axis=0, keepdims=True)))
            return tuple(result)

        highs = lax.fori_loop(
            low, block + 1, score_pass,
            tuple(jnp.full((1, tile), masked_score, F32) for _ in range(heads)),
        )

        def prob_pass(key_block, carry):
            result = []
            rows = rows_of(key_block)
            for h in range(heads):
                total, mixed = carry[2 * h], carry[2 * h + 1]
                probs = jnp.exp(score_ref[h, slot(key_block), :] - highs[h])
                total = total + jnp.sum(probs, axis=0, keepdims=True)
                probs = probs.astype(BF)
                prob_ref[h, slot(key_block), :] = probs
                mixed = mixed + mm(vt_ref[h * HEAD : (h + 1) * HEAD, rows], probs)
                result += [total, mixed]
            return tuple(result)

        start = []
        for h in range(heads):
            start += [jnp.zeros((1, tile), F32), jnp.zeros((HEAD, tile), F32)]
        summed = lax.fori_loop(low, block + 1, prob_pass, tuple(start))

        grads_t = grads_here.astype(F32).T
        mixed_parts, scaled_parts, deltas = [], [], []
        for h in range(heads):
            inverse = 1.0 / summed[2 * h]
            mixed = summed[2 * h + 1] * inverse
            grads = grads_t[h * HEAD : (h + 1) * HEAD, :] * inverse
            deltas.append(jnp.sum(mixed * grads, axis=0, keepdims=True))
            mixed_parts.append(mixed)
            scaled_parts.append(grads)
        mix_ref[...] = jnp.concatenate(mixed_parts, axis=0).T.astype(BF)
        scaled = jnp.concatenate(scaled_parts, axis=0).T.astype(BF)
        g_heads = [jnp.where(own[h], scaled, jnp.zeros_like(scaled)) for h in range(heads)]

        def grad_pass(key_block, grads_q):
            rows = rows_of(key_block)
            value_rows = v_ref[rows, :]
            result = []
            grad_k = gk_acc[rows, :]
            grad_v = gv_acc[rows, :]
            for h in range(heads):
                probs = prob_ref[h, slot(key_block), :]
                grad_probs = mm_nt(value_rows, g_heads[h])
                grad_scores = (probs.astype(F32) * (grad_probs - deltas[h])).astype(BF)
                grad_v = grad_v + mm(probs, g_heads[h])
                grad_k = grad_k + mm(grad_scores, q_heads[h])
                result.append(
                    grads_q[h] + mm(kt_ref[h * HEAD : (h + 1) * HEAD, rows], grad_scores)
                )
            gk_acc[rows, :] = grad_k
            gv_acc[rows, :] = grad_v
            return tuple(result)

        grads_q = lax.fori_loop(
            low, block + 1, grad_pass, tuple(jnp.zeros((HEAD, tile), F32) for _ in range(heads))
        )
        here = rows_of(block)
        rot = (jnp.concatenate(grads_q, axis=0) * scale).T
        grad_q = turn(
            rot, spread_lanes(cos_ref[here, :], hw), spread_lanes(sin_ref[here, :], hw), -1.0
        ).astype(BF)
        gq_ref[...] = grad_q
        sum_ref[0:1, :] += jnp.sum(grad_q.astype(F32), axis=0, keepdims=True)

        @pl.when(block == count - 1)
        def _():
            def finish(t, carry):
                rows = pl.ds(pl.multiple_of(t * tile, tile), tile)
                grad_k = turn(
                    gk_acc[rows, :],
                    spread_lanes(cos_ref[rows, :], hw),
                    spread_lanes(sin_ref[rows, :], hw),
                    -1.0,
                ).astype(BF)
                grad_v = gv_acc[rows, :].astype(BF)
                gk_ref[rows, :] = grad_k
                gv_ref[rows, :] = grad_v
                sum_ref[1:2, :] += jnp.sum(grad_k.astype(F32), axis=0, keepdims=True)
                sum_ref[2:3, :] += jnp.sum(grad_v.astype(F32), axis=0, keepdims=True)
                return carry

            lax.fori_loop(0, count, finish, 0)

    tiled = pl.BlockSpec((tile, hw), lambda i, ids_ref: (place(ids_ref, i), 0))
    shape = jax.ShapeDtypeStruct((seq, hw), BF)
    return pl.pallas_call(
        kernel,
        out_shape=[shape] * 4 + [jax.ShapeDtypeStruct((8, hw), F32)],
        grid_spec=pltpu.PrefetchScalarGridSpec(
            num_scalar_prefetch=1,
            grid=(count,),
            in_specs=[
                tiled,
                whole((seq, hw)),
                whole((seq, hw)),
                whole((hw, seq)),
                whole((hw, seq)),
                tiled,
                whole(cos_table.shape),
                whole(sin_table.shape),
            ],
            out_specs=[tiled, tiled, whole((seq, hw)), whole((seq, hw)), whole((8, hw))],
            scratch_shapes=[
                pltpu.VMEM((heads, seq, tile), F32),
                pltpu.VMEM((heads, seq, tile), BF),
                pltpu.VMEM((seq, hw), F32),
                pltpu.VMEM((seq, hw), F32),
            ],
        ),
        compiler_params=params_of(),
        cost_estimate=pl.CostEstimate(
            flops=12 * seq * seq * hw, bytes_accessed=10 * seq * hw * 2, transcendentals=0
        ),
        name="attention",
    )(ids, queries, keys, values, keys_t, values_t, grad_mix, cos_table, sin_table)


def split_specs(dims, tile):
    per = dims.tokens // tile
    shape = jax.ShapeDtypeStruct((dims.nx, dims.tokens, dims.width), BF)

    def spec(odd):
        def index(i, ids_ref):
            block, t = i // per, i % per
            mine = block % 2 == odd
            row = jnp.where(mine, t, per - 1 if odd == 0 else 0)
            return (block // 2, row, 0)

        return pl.BlockSpec((None, tile, dims.width), index)

    return [(shape, spec(1)), (shape, spec(0))], per


def put_split(step, per, outs, value):
    odd = (step // per) % 2

    @pl.when(odd == 1)
    def _():
        outs[0][...] = value

    @pl.when(odd == 0)
    def _():
        outs[1][...] = value


def out_body(per, step, count, lhs, weights, extras, outs, scratch):
    value = mm(lhs[0][...], weights[0][...]) + mm(lhs[1][...], weights[1][...])
    put_split(step, per, outs, value.astype(BF))


def up_grad_body(step, count, lhs, weights, extras, outs, scratch):
    grads = (mm_nt(lhs[0][...], weights[0][...]) * lhs[1][...].astype(F32)).astype(BF)
    outs[0][...] = grads

    @pl.when(step == 0)
    def _():
        outs[1][...] = jnp.zeros_like(outs[1])

    outs[1][0:1, :] += jnp.sum(grads.astype(F32), axis=0, keepdims=True)


def in_grad_body(per, hw, step, count, lhs, weights, extras, outs, scratch):
    up_grad, gq, gk, gv, hat_ref = lhs
    qkv_ref, up_ref = weights
    affine = extras[0]
    attn = (
        mm_nt(gq[...], qkv_ref[:, :hw])
        + mm_nt(gk[...], qkv_ref[:, hw : 2 * hw])
        + mm_nt(gv[...], qkv_ref[:, 2 * hw :])
    )
    ffn = mm_nt(up_grad[...], up_ref[...])
    hat = hat_ref[...].astype(F32)

    @pl.when(step == 0)
    def _():
        outs[2][...] = jnp.zeros_like(outs[2])

    for row, value in enumerate((attn * hat, attn, ffn * hat, ffn)):
        outs[2][row : row + 1, :] += jnp.sum(value, axis=0, keepdims=True)
    put_split(step, per, outs, (attn * affine[0:1, :] + ffn * affine[2:3, :]).astype(BF))


def weight_grad(dims, name, kind, ids, left, rights):
    tile = 512
    m = left.shape[1]
    widths = [r.shape[1] for r in rights]
    n = sum(widths)
    count = dims.seq // tile
    hi, lo, ns, nd = dims.hi, dims.lo, dims.ns, dims.nd
    if kind == "row":
        rows = m // nd
        shape = (hi, rows, n)
    else:
        rows = m // (nd * ns)
        shape = (hi, ns, rows, n)

    def kernel(ids_ref, left_ref, *refs):
        right_refs = refs[: len(rights)]
        out_refs = refs[len(rights) : len(rights) + lo]
        total = refs[-1]
        step = pl.program_id(0)
        at = 0
        for width, right_ref in zip(widths, right_refs):
            part = mm_tn(left_ref[...], right_ref[...])
            cols = slice(at, at + width)

            @pl.when(step == 0)
            def _():
                total[:, cols] = part

            @pl.when(step > 0)
            def _():
                total[:, cols] += part

            at += width

        @pl.when(step == count - 1)
        def _():
            s, z, y = ids_ref[0], ids_ref[1], ids_ref[2]
            for jy in range(lo):
                for jz in range(hi):
                    owner = (z ^ jz) * lo + (y ^ jy)
                    if kind == "row":
                        at = pl.multiple_of(owner * rows, rows)
                        out_refs[jy][jz] = total[pl.ds(at, rows), :].astype(BF)
                    else:
                        for js in range(ns):
                            at = pl.multiple_of(((s ^ js) * nd + owner) * rows, rows)
                            out_refs[jy][jz, js] = total[pl.ds(at, rows), :].astype(BF)

    return pl.pallas_call(
        kernel,
        out_shape=[jax.ShapeDtypeStruct(shape, BF)] * lo,
        grid_spec=pltpu.PrefetchScalarGridSpec(
            num_scalar_prefetch=1,
            grid=(count,),
            in_specs=[pl.BlockSpec((tile, m), lambda i, ids_ref: (i, 0))]
            + [pl.BlockSpec((tile, w), lambda i, ids_ref: (i, 0)) for w in widths],
            out_specs=[whole(shape)] * lo,
            scratch_shapes=[pltpu.VMEM((m, n), F32)],
        ),
        compiler_params=params_of(),
        cost_estimate=pl.CostEstimate(
            flops=2 * dims.seq * m * n,
            bytes_accessed=2 * (dims.seq * (m + n) + m * n),
            transcendentals=0,
        ),
        name=name,
    )(ids, left, *rights)


def cut_columns(dims, ids, qkv, up):
    ns, hw, ffw = dims.ns, dims.hw, dims.ffw
    rows = qkv.shape[0]

    def kernel(ids_ref, qkv_ref, up_ref, *outs):
        for js in range(ns):
            other = ids_ref[0] ^ js
            for part in range(3):
                at = pl.multiple_of(part * dims.width + other * hw, hw)
                outs[js][:, part * hw : (part + 1) * hw] = qkv_ref[:, pl.ds(at, hw)]
            at = pl.multiple_of(other * ffw, ffw)
            outs[js][:, 3 * hw :] = up_ref[:, pl.ds(at, ffw)]

    shape = (rows, 3 * hw + ffw)
    return pl.pallas_call(
        kernel,
        out_shape=[jax.ShapeDtypeStruct(shape, BF)] * ns,
        grid_spec=pltpu.PrefetchScalarGridSpec(
            num_scalar_prefetch=1,
            grid=(1,),
            in_specs=[whole(qkv.shape), whole(up.shape)],
            out_specs=[whole(shape)] * ns,
        ),
        compiler_params=params_of(),
        name="cut_columns",
    )(ids, qkv, up)


def join_columns(dims, ids, pieces, parts, width):
    ns = dims.ns
    rows, n = pieces[0].shape
    w = n // parts
    total = n * ns

    def kernel(ids_ref, *refs):
        out = refs[-1]
        for js in range(ns):
            other = ids_ref[0] ^ js
            for part in range(parts):
                at = pl.multiple_of(part * width + other * w, w)
                out[:, pl.ds(at, w)] = refs[js][:, part * w : (part + 1) * w].astype(F32)

    return pl.pallas_call(
        kernel,
        out_shape=jax.ShapeDtypeStruct((rows, total), F32),
        grid_spec=pltpu.PrefetchScalarGridSpec(
            num_scalar_prefetch=1,
            grid=(1,),
            in_specs=[whole((rows, n))] * ns,
            out_specs=whole((rows, total)),
        ),
        compiler_params=params_of(),
        name="join_columns",
    )(ids, *pieces)


def permute_plan(
    hidden_states,
    segment_ids,
    positions,
    out_grad,
    qkv_weight,
    qkv_bias,
    dense_weight,
    dense_bias,
    up_weight,
    up_bias,
    down_weight,
    down_bias,
    attn_gain,
    attn_shift,
    ffn_gain,
    ffn_shift,
):
    ns, nd = lax.axis_size("seq"), lax.axis_size("dp")
    tokens, width = hidden_states.shape[1:]
    dims = Dims(ns, nd, tokens, width, up_weight.shape[1])
    hi, lo, nx = dims.hi, dims.lo, dims.nx
    hw, ffw, seq = dims.hw, dims.ffw, dims.seq
    s, d = lax.axis_index("seq"), lax.axis_index("dp")
    z, y = d // lo, d % lo
    ids = jnp.stack([s, z, y, s]).astype(jnp.int32)

    def by_seq(value, mask):
        return xor_swap(value, "seq", ns, mask)

    def by_dp(value, mask):
        return xor_swap(value, "dp", nd, mask)

    hidden, grad_out = hidden_states[0], out_grad[0]

    fields = (qkv_bias, dense_bias, up_bias, down_bias, attn_gain, attn_shift, ffn_gain, ffn_shift)
    mine = jnp.concatenate(fields)
    index = s * nd + d
    small = jnp.where(jnp.arange(ns * nd)[:, None] == index, mine[None, :], jnp.zeros((), BF))
    mask = 1
    while mask < ns:
        small = small + by_seq(small, mask)
        mask *= 2
    mask = 1
    while mask < nd:
        small = small + by_dp(small, mask)
        mask *= 2
    full, at = [], 0
    for field in fields:
        n = field.shape[0]
        full.append(small[:, at : at + n].reshape(-1).astype(F32))
        at += n
    b_qkv, b_dense, b_up, b_down, g_attn, s_attn, g_ffn, s_ffn = full
    affine = jnp.concatenate(
        [jnp.stack([g_attn, s_attn, g_ffn, s_ffn]), jnp.zeros((4, width), F32)], axis=0
    )
    bias_qkv = lax.dynamic_index_in_dim(
        b_qkv.reshape(3, ns, hw), s, 1, keepdims=False
    ).reshape(1, 3 * hw)
    bias_up = lax.dynamic_slice_in_dim(b_up, s * ffw, ffw).reshape(1, ffw)

    meta = jnp.stack([segment_ids[0], positions[0]])
    metas = [meta] + [by_seq(meta, js) for js in range(1, ns)]
    meta_all = jnp.concatenate(metas, axis=1)
    starts = [jnp.sum((meta_all[0] < v).astype(jnp.int32)) for v in range(1, DOCS)]
    doc_ids = jnp.stack([s.astype(jnp.int32)] + starts)
    half = ROT // 2
    freqs = rotary_base ** (-2.0 * jnp.arange(half, dtype=F32) / ROT)
    angles = meta_all[1].astype(F32)[None, :] * freqs[:, None]
    table = 2 * HEAD
    pick = np.zeros((half, table), np.float32)
    signed = np.zeros((half, table), np.float32)
    rest = np.ones((1, table), np.float32)
    for lane in range(table):
        if lane % HEAD < ROT:
            pick[lane % HEAD % half, lane] = 1.0
            signed[lane % HEAD % half, lane] = -1.0 if lane % HEAD < half else 1.0
            rest[0, lane] = 0.0
    exact = lax.Precision.HIGHEST
    cos_table = lax.dot_general(jnp.cos(angles), jnp.asarray(pick), TN, precision=exact) + rest
    sin_table = lax.dot_general(jnp.sin(angles), jnp.asarray(signed), TN, precision=exact)

    def gather_tokens(value):
        found = [value, by_seq(value, 1)]
        for m in range(1, nx):
            across = by_seq(value, 2 * m)
            found += [across, by_seq(across, 1)]
        return found

    blocks = gather_tokens(hidden)

    cuts = cut_columns(dims, ids, qkv_weight, up_weight)
    got = [cuts[0]] + [by_seq(cuts[js], js) for js in range(1, ns)]
    stacked = jnp.stack(got)

    def gather_dp(shard):
        pieces = []
        for jz in range(hi):
            here = shard if jz == 0 else by_dp(shard, jz * lo)
            pieces += [here] + [by_dp(here, jy) for jy in range(1, lo)]
        return pieces

    up_pieces = gather_dp(stacked[:, :, 3 * hw :])
    qkv_pieces = gather_dp(stacked[:, :, : 3 * hw])
    dense_pieces = gather_dp(dense_weight)
    down_pieces = gather_dp(down_weight)
    qkv_w = ("col", qkv_pieces, (width, 3 * hw))
    up_w = ("col", up_pieces, (width, ffw))
    dense_w = ("row", dense_pieces, (hw, width))
    down_w = ("row", down_pieces, (ffw, width))

    carried = ()
    for m in range(nx):
        carried = norm_pair(dims, m, blocks[2 * m], blocks[2 * m + 1], affine, carried)
    attn_low, ffn_low, hat_low = carried

    tile = 256
    act, slope = token_call(
        dims, "up", ids, up_body, [ffn_low], [up_w], [bias_up],
        [tiled_out(seq, ffw, tile)] * 2, tile, 2 * seq * width * ffw * 2,
    )
    flip = (
        jax.ShapeDtypeStruct((hw, seq), BF),
        pl.BlockSpec((hw, tile), lambda i, ids_ref: (0, i)),
    )
    queries, keys, values, keys_t, values_t = token_call(
        dims, "qkv", ids, functools.partial(qkv_body, dims), [attn_low, cos_table, sin_table],
        [qkv_w], [bias_qkv], [tiled_out(seq, hw, tile)] * 3 + [flip] * 2, tile,
        2 * seq * width * 3 * hw,
    )
    grads_all = jnp.concatenate(gather_tokens(grad_out), axis=0)
    grad_mix = token_call(
        dims, "mix_grad", ids, mix_grad_body, [grads_all], [dense_w], [],
        [tiled_out(seq, hw, tile)], tile, 2 * seq * width * hw,
    )[0]
    mixed, gq, gk, gv, qkv_sums = attention(
        dims, doc_ids, queries, keys, values, keys_t, values_t, grad_mix, cos_table, sin_table
    )

    def reduce_tokens(others, own):
        got = by_seq(others, 1)
        total = own[0].astype(F32) + got[0].astype(F32)
        for m in range(1, nx):
            total = total + by_seq(own[m] + got[m], 2 * m).astype(F32)
        return total

    def reduce_dp(parts):
        got = [by_dp(parts[jy], jy) for jy in range(1, lo)]

        def slab(jz):
            value = parts[0][jz].astype(F32)
            for g in got:
                value = value + g[jz].astype(F32)
            return value

        total = slab(0)
        for jz in range(1, hi):
            total = total + by_dp(slab(jz).astype(BF), jz * lo).astype(F32)
        return total

    def columns_home(total, parts):
        low = total.astype(BF)
        pieces = [low[0]] + [by_seq(low[js], js) for js in range(1, ns)]
        return join_columns(dims, ids, pieces, parts, width)

    down_parts = weight_grad(dims, "down_grad", "row", ids, act, [grads_all])
    grad_down = reduce_dp(down_parts)
    dense_parts = weight_grad(dims, "dense_grad", "row", ids, mixed, [grads_all])
    grad_dense = reduce_dp(dense_parts)
    qkv_parts = weight_grad(dims, "qkv_grad", "col", ids, attn_low, [gq, gk, gv])
    grad_qkv = columns_home(reduce_dp(qkv_parts), 3)

    sums_shape = lambda n: (jax.ShapeDtypeStruct((8, n), F32), whole((8, n)))
    grad_up_low, up_sums = token_call(
        dims, "up_grad", ids, up_grad_body, [grads_all, slope], [down_w], [],
        [tiled_out(seq, ffw, tile), sums_shape(ffw)], tile, 2 * seq * width * ffw,
    )
    up_parts = weight_grad(dims, "up_w_grad", "col", ids, ffn_low, [grad_up_low])
    grad_up = columns_home(reduce_dp(up_parts), 1)

    outs, per = split_specs(dims, tile)
    others, own = token_call(
        dims, "out", ids, functools.partial(out_body, per), [mixed, act], [dense_w, down_w], [],
        outs, tile, 2 * seq * width * (hw + ffw),
    )
    out_total = reduce_tokens(others, own)
    output = (hidden.astype(F32) + out_total + (b_dense + b_down)[None, :]).astype(BF)

    others, own, gain_sums = token_call(
        dims, "in_grad", ids, functools.partial(in_grad_body, per, hw),
        [grad_up_low, gq, gk, gv, hat_low], [qkv_w, up_w], [affine],
        outs + [sums_shape(width)], tile, 2 * seq * width * (3 * hw + ffw),
    )
    gx = reduce_tokens(others, own)
    rows = hidden.astype(F32)
    spread = rows - jnp.mean(rows, axis=-1, keepdims=True)
    inv_std = lax.rsqrt(jnp.mean(spread * spread, axis=-1, keepdims=True) + epsilon)
    hat = spread * inv_std
    back = inv_std * (
        gx
        - jnp.mean(gx, axis=-1, keepdims=True)
        - hat * jnp.mean(gx * hat, axis=-1, keepdims=True)
    )
    grad_out_f = grad_out.astype(F32)
    input_grad = (grad_out_f + back).astype(BF)

    def placed(value, parts, w):
        base = jnp.zeros((parts, ns, w), F32)
        return lax.dynamic_update_slice_in_dim(base, value.reshape(parts, 1, w), s, 1).reshape(-1)

    out_sum = jnp.sum(grad_out_f, axis=0)
    vectors = (
        placed(qkv_sums[:3], 3, hw),
        out_sum,
        placed(up_sums[0], 1, ffw),
        gain_sums[0],
        gain_sums[1],
        gain_sums[2],
        gain_sums[3],
    )
    packed = jnp.concatenate(vectors).reshape(-1, 128)
    mask = 1
    while mask < ns:
        packed = packed + by_seq(packed, mask)
        mask *= 2
    mask = 1
    while mask < nd:
        packed = packed + by_dp(packed, mask)
        mask *= 2
    flat = packed.reshape(-1)
    small_out, at = [], 0
    for vector in vectors:
        n = vector.shape[0]
        share = n // (ns * nd)
        small_out.append(lax.dynamic_slice_in_dim(flat, at + index * share, share))
        at += n
    gb_qkv, gb_out, gb_up, gg_attn, gs_attn, gg_ffn, gs_ffn = small_out
    return (
        output[None],
        input_grad[None],
        grad_qkv,
        gb_qkv,
        grad_dense,
        gb_out,
        grad_up,
        gb_up,
        grad_down,
        gb_out,
        gg_attn,
        gs_attn,
        gg_ffn,
        gs_ffn,
    )


class Bag(dict):
    __getattr__ = dict.__getitem__


class Net:
    def __init__(self, send, recv):
        self.send_sems, self.recv_sems, self.copies = send, recv, []

    def make(self, source, target, **peer):
        at = len(self.copies)
        copy = pltpu.make_async_remote_copy(
            src_ref=source,
            dst_ref=target,
            send_sem=self.send_sems.at[at],
            recv_sem=self.recv_sems.at[at],
            device_id=peer,
            device_id_type=pl.DeviceIdType.MESH,
        )
        self.copies.append(copy)
        return copy

    def send(self, source, target, **peer):
        copy = self.make(source, target, **peer)
        copy.start()
        return copy

    def finish(self):
        for copy in self.copies:
            copy.wait_send()


class Local:
    def __init__(self, sems):
        self.sems, self.copies, self.done = sems, [], 0

    def make(self, source, target):
        copy = pltpu.make_async_copy(source, target, self.sems.at[self.done + len(self.copies)])
        self.copies.append(copy)
        return copy

    def copy(self, source, target):
        copy = self.make(source, target)
        copy.start()
        return copy

    def load(self, source, target):
        copy = pltpu.make_async_copy(source, target, self.sems.at[self.done + len(self.copies)])
        copy.start()
        self.done += 1
        return copy

    def finish(self):
        for copy in self.copies:
            copy.wait()


def greet(peers):
    barrier = pltpu.get_barrier_semaphore()
    for peer in peers:
        pl.semaphore_signal(
            barrier, inc=1, device_id=peer, device_id_type=pl.DeviceIdType.MESH
        )
    pl.semaphore_wait(barrier, len(peers))


def neighbours(dims, s, d):
    return (
        [{"seq": s ^ js} for js in range(1, dims.ns)]
        + [{"dp": d ^ (jz * dims.lo)} for jz in range(1, dims.hi)]
        + [{"dp": d ^ jy} for jy in range(1, dims.lo)]
    )


def table_constants():
    half = ROT // 2
    table = 2 * HEAD
    constants = np.zeros((24, table), np.float32)
    for lane in range(table):
        if lane % HEAD < ROT:
            constants[lane % HEAD % half, lane] = 1.0
            constants[half + lane % HEAD % half, lane] = -1.0 if lane % HEAD < half else 1.0
        else:
            constants[2 * half, lane] = 1.0
    return constants


def rotary_tables(rows, const_ref, width):
    half = ROT // 2
    exact = lax.Precision.HIGHEST
    cosine = lax.dot_general(
        rows[0:half, :], const_ref[0:half, :], TN, precision=exact, preferred_element_type=F32
    ) + const_ref[2 * half : 2 * half + 1, :]
    sine = lax.dot_general(
        rows[half : 2 * half, :], const_ref[half : 2 * half, :], TN, precision=exact,
        preferred_element_type=F32,
    )
    return spread_lanes(cosine, width), spread_lanes(sine, width)


def gather_kernel(dims, hidden, grad_out, meta, small, qkv, up, dense):
    ns, nd, hi, lo, nx = dims.ns, dims.nd, dims.hi, dims.lo, dims.nx
    tokens, width, hw, ffw, seq = dims.tokens, dims.width, dims.hw, dims.ffw, dims.seq
    share, dense_share = qkv.shape[0], dense.shape[0]
    n_net, n_local = 128, 64

    def kernel(
        hid, gout, meta_ref, small_ref, qkv_ref, up_ref, dense_ref, const_ref,
        attn_out, ffn_out, hat_out, g_out, act_out, slope_out, q_out, k_out, v_out, kt_out,
        vt_out, mix_out, qkv_out, up_out, dense_out, meta_out, affine_out,
        h_buf, g_buf, attn_buf, ffn_buf, hat_buf, act_buf, slope_buf, q_buf, k_buf, v_buf,
        kt_buf, vt_buf, mix_buf, w_qkv, w_up, w_dense, meta_buf, affine, vectors, bias_rows,
        send_sems, recv_sems, local_sems,
    ):
        s, d = lax.axis_index("seq"), lax.axis_index("dp")
        z, y = d // lo, d % lo
        net, local = Net(send_sems, recv_sems), Local(local_sems)
        h_own = local.load(hid, h_buf.at[0:tokens])
        greet(neighbours(dims, s, d))

        def block(ref, j):
            return ref.at[j * tokens : (j + 1) * tokens]

        def along_z(weight):
            return [net.send(weight(d), weight(d), dp=d ^ (jz * lo)) for jz in range(1, hi)]

        def along_y(weight, jz):
            at = (z ^ jz) * lo + y
            return [net.send(weight(at), weight(at), dp=d ^ jy) for jy in range(1, lo)]

        def forward_y(arrivals, weight):
            sent = []
            for jz, done in enumerate(arrivals, 1):
                done.wait_recv()
                sent += along_y(weight, jz)
            return sent

        def to_columns(js, name):
            other = s ^ js
            if name == "up":
                at = pl.multiple_of(other * ffw, ffw)
                pairs = [(up_ref.at[:, pl.ds(at, ffw)], w_up.at[s, d])]
            else:
                pairs = []
                for part in range(3):
                    at = pl.multiple_of(part * width + other * hw, hw)
                    pairs.append(
                        (
                            qkv_ref.at[:, pl.ds(at, hw)],
                            w_qkv.at[s, d, :, part * hw : (part + 1) * hw],
                        )
                    )
            if js == 0:
                return [local.load(a, b) for a, b in pairs]
            return [net.send(a, b, seq=other) for a, b in pairs]

        tiny = [net.send(small_ref, vectors.at[s, d], seq=s ^ js) for js in range(1, ns)]
        vectors[s, d] = small_ref[...]
        cuts = Bag()
        for name in ("up", "qkv"):
            cuts[name] = [to_columns(js, name) for js in range(ns)]
        metas = [net.send(meta_ref, meta_buf.at[js], seq=s ^ js) for js in range(1, ns)]
        meta_buf[0] = meta_ref[...]
        h_core = net.send(hid, block(h_buf, 1), seq=s ^ 1)
        h_cross = [net.send(hid, block(h_buf, 2 * m), seq=s ^ (2 * m)) for m in range(1, nx)]
        g_core = net.send(gout, block(g_buf, 1), seq=s ^ 1)
        g_cross = [net.send(gout, block(g_buf, 2 * m), seq=s ^ (2 * m)) for m in range(1, nx)]
        g_own = local.load(gout, block(g_buf, 0))
        dense_own = local.load(dense_ref, w_dense.at[d])

        part_qkv = lambda at: w_qkv.at[:, at]
        part_up = lambda at: w_up.at[:, at]
        part_dense = lambda at: w_dense.at[at]
        part_tiny = lambda at: vectors.at[:, at]

        for done in tiny:
            done.wait_recv()
        z_tiny = along_z(part_tiny)
        y_tiny = along_y(part_tiny, 0)

        def spread_weight(name, weight):
            for done in cuts[name][0]:
                done.wait()
            for group in cuts[name][1:]:
                for done in group:
                    done.wait_recv()
            return along_z(weight), along_y(weight, 0)

        z_up, y_up = spread_weight("up", part_up)
        y_tiny += forward_y(z_tiny, part_tiny)
        z_qkv, y_qkv = spread_weight("qkv", part_qkv)
        dense_own.wait()
        z_dense, y_dense = along_z(part_dense), along_y(part_dense, 0)

        for done in y_tiny:
            done.wait_recv()
        n = width // (ns * nd)
        per_row = 128 // n
        for row in range(width // 128):
            total = None
            for q in range(per_row):
                owner = row * per_row + q
                tile = vectors[owner // nd, owner % nd]
                tile = pltpu.roll(tile, q * n, 1) if q else tile
                total = tile if total is None else total + tile
            lanes = slice(row * 128, (row + 1) * 128)
            affine[0:4, lanes] = total[4:8, :]
            affine[4:5, lanes] = total[1:2, :] + total[3:4, :]
        lane = lax.broadcasted_iota(jnp.int32, (1, 128), 1)
        n = 3 * n
        bias_rows[...] = jnp.zeros_like(bias_rows)
        for owner in range(ns * nd):
            start, row = owner * n % 128, owner * n // 128
            tile = vectors[owner // nd, owner % nd]
            tile = (pltpu.roll(tile, start, 1) if start else tile)[0:1, :]
            bias_rows[row : row + 1, :] += jnp.where(lane >= start, tile, 0.0)
            if start + n > 128:
                bias_rows[row + 1 : row + 2, :] += jnp.where(lane < start, tile, 0.0)
        local.copy(affine, affine_out)
        tile = 256

        def norm(first, last):
            def body(t, carry):
                rows = pl.ds(pl.multiple_of(t * tile, tile), tile)
                x = h_buf[rows, :].astype(F32)
                spread = x - jnp.mean(x, axis=-1, keepdims=True)
                hat = spread * lax.rsqrt(
                    jnp.mean(spread * spread, axis=-1, keepdims=True) + epsilon
                )
                attn_buf[rows, :] = (hat * affine[0:1, :] + affine[1:2, :]).astype(BF)
                ffn_buf[rows, :] = (hat * affine[2:3, :] + affine[3:4, :]).astype(BF)
                hat_buf[rows, :] = hat.astype(BF)
                return carry

            per = tokens // tile
            lax.fori_loop(first * per, last * per, body, 0)
            here = slice(first * tokens, last * tokens)
            for source, target in ((attn_buf, attn_out), (ffn_buf, ffn_out), (hat_buf, hat_out)):
                local.copy(source.at[here], target.at[here])

        h_own.wait()
        h_core.wait_recv()
        norm(0, 2)
        y_up += forward_y(z_up, part_up)
        h_far = []
        for m, done in enumerate(h_cross, 1):
            done.wait_recv()
            h_far.append(
                net.send(block(h_buf, 2 * m), block(h_buf, 2 * m + 1), seq=s ^ 1)
            )
        for done in h_far:
            done.wait_recv()
        norm(2, ns)

        for done in y_up:
            done.wait_recv()
        bias_up = jnp.concatenate(
            [
                vectors[(s * (ffw // 128) + c) // nd, (s * (ffw // 128) + c) % nd, 2:3, :]
                for c in range(ffw // 128)
            ],
            axis=1,
        )

        def up_rows(first, last):
            def body(t, carry):
                rows = pl.ds(pl.multiple_of(t * tile, tile), tile)
                pre = mm(ffn_buf[rows, :], w_up[...].reshape(width, ffw)) + bias_up
                total = 0.5 + 0.5 * lax.erf(pre * math.sqrt(0.5))
                density = jnp.exp(-0.5 * pre * pre) * (1.0 / math.sqrt(2.0 * math.pi))
                act_buf[rows, :] = (pre * total).astype(BF)
                slope_buf[rows, :] = (total + pre * density).astype(BF)
                return carry

            per = tokens // tile
            lax.fori_loop(first * per, last * per, body, 0)
            here = slice(first * tokens, last * tokens)
            for source, target in ((act_buf, act_out), (slope_buf, slope_out)):
                local.copy(source.at[here], target.at[here])

        up_rows(0, ns // 2)
        y_qkv += forward_y(z_qkv, part_qkv)
        up_rows(ns // 2, ns)
        local.copy(w_up, up_out)
        y_dense += forward_y(z_dense, part_dense)

        for done in y_qkv:
            done.wait_recv()
        for done in metas:
            done.wait_recv()
        parts = hw // 128
        bias_qkv = jnp.concatenate(
            [
                bias_rows[pl.ds(part * (width // 128) + s * parts + k, 1), :]
                for part in range(3)
                for k in range(parts)
            ],
            axis=1,
        )

        def qkv_block(j, carry):
            rows = pl.ds(pl.multiple_of(j * tokens, tokens), tokens)
            cosine, sine = rotary_tables(meta_buf[j], const_ref, hw)
            joined = mm(attn_buf[rows, :], w_qkv[...].reshape(width, 3 * hw)) + bias_qkv
            queries = turn(joined[:, :hw], cosine, sine, 1.0)
            keys = turn(joined[:, hw : 2 * hw], cosine, sine, 1.0)
            values = joined[:, 2 * hw :]
            q_buf[rows, :] = queries.astype(BF) * (1.0 / math.sqrt(HEAD))
            k_buf[rows, :] = keys.astype(BF)
            v_buf[rows, :] = values.astype(BF)
            kt_buf[:, rows] = keys.T.astype(BF)
            vt_buf[:, rows] = values.T.astype(BF)
            return carry

        lax.fori_loop(0, ns, qkv_block, 0)
        for source, target in (
            (q_buf, q_out), (k_buf, k_out), (v_buf, v_out), (kt_buf, kt_out), (vt_buf, vt_out),
            (w_qkv, qkv_out), (meta_buf, meta_out),
        ):
            local.copy(source, target)

        g_far = []
        for m, done in enumerate(g_cross, 1):
            done.wait_recv()
            g_far.append(
                net.send(block(g_buf, 2 * m), block(g_buf, 2 * m + 1), seq=s ^ 1)
            )
        for done in y_dense + [g_core]:
            done.wait_recv()
        g_own.wait()

        def mix_block(j, carry):
            rows = pl.ds(pl.multiple_of(j * tokens, tokens), tokens)
            mix_buf[rows, :] = mm_nt(g_buf[rows, :], w_dense[...].reshape(hw, width)).astype(BF)
            return carry

        lax.fori_loop(0, ns - 1, mix_block, 0)
        for done in g_far:
            done.wait_recv()
        lax.fori_loop(ns - 1, ns, mix_block, 0)
        for source, target in ((mix_buf, mix_out), (g_buf, g_out), (w_dense, dense_out)):
            local.copy(source, target)
        local.finish()
        net.finish()

    sds = jax.ShapeDtypeStruct
    any_spec = pl.BlockSpec(memory_space=pl.ANY)
    vmem_spec = pl.BlockSpec(memory_space=pltpu.VMEM)
    const = jnp.asarray(table_constants())
    out_shapes = (
        [sds((seq, width), BF)] * 4
        + [sds((seq, ffw), BF)] * 2
        + [sds((seq, hw), BF)] * 3
        + [sds((hw, seq), BF)] * 2
        + [sds((seq, hw), BF)]
        + [
            sds((ns, nd, share, 3 * hw), BF),
            sds((ns, nd, share, ffw), BF),
            sds((nd, dense_share, width), BF),
            sds((ns,) + meta.shape, F32),
            sds((8, width), F32),
        ]
    )
    scratch = [
        pltpu.VMEM(x.shape, x.dtype)
        for x in [sds((seq, width), BF)] * 5 + out_shapes[4:]
    ] + [
        pltpu.VMEM((ns, nd) + small.shape, F32),
        pltpu.VMEM((3 * width // 128 + 8, 128), F32),
        pltpu.SemaphoreType.DMA((n_net,)),
        pltpu.SemaphoreType.DMA((n_net,)),
        pltpu.SemaphoreType.DMA((n_local,)),
    ]
    return pl.pallas_call(
        kernel,
        out_shape=out_shapes,
        in_specs=[any_spec] * 2 + [vmem_spec] * 2 + [any_spec] * 3 + [vmem_spec],
        out_specs=[any_spec] * len(out_shapes),
        scratch_shapes=scratch,
        compiler_params=pltpu.CompilerParams(
            vmem_limit_bytes=VMEM_LIMIT, collective_id=1, has_side_effects=True
        ),
        name="gather",
    )(hidden, grad_out, meta, small, qkv, up, dense, const)


class Spread:
    def __init__(self, dims, net, where, groups, rows, total, base, cols, bufs):
        self.dims, self.net, self.where, self.groups, self.rows = dims, net, where, groups, rows
        self.total, self.base, self.cols = total, base, cols
        self.send_y, self.recv_y, self.send_z, self.recv_z = bufs

    def part(self, group, owner):
        at = pl.multiple_of(self.base + (group * self.dims.nd + owner) * self.rows, self.rows)
        return self.total[pl.ds(at, self.rows), self.cols]

    def start(self):
        s, d, z, y = self.where
        dims = self.dims
        self.along_y = []
        for jy in range(1, dims.lo):
            for zz in range(dims.hi):
                for g in range(self.groups):
                    self.send_y[jy - 1, zz, g] = self.part(g, zz * dims.lo + (y ^ jy)).astype(BF)
            self.along_y.append(
                self.net.send(self.send_y.at[jy - 1], self.recv_y.at[jy - 1], dp=d ^ jy)
            )

    def summed(self, zz, g):
        s, d, z, y = self.where
        value = self.part(g, zz * self.dims.lo + y)
        for jy in range(1, self.dims.lo):
            value = value + self.recv_y[jy - 1, zz, g].astype(F32)
        return value

    def middle(self):
        s, d, z, y = self.where
        for copy in self.along_y:
            copy.wait_recv()
        self.along_z = []
        for jz in range(1, self.dims.hi):
            for g in range(self.groups):
                self.send_z[jz - 1, g] = self.summed(z ^ jz, g).astype(BF)
            self.along_z.append(
                self.net.send(
                    self.send_z.at[jz - 1], self.recv_z.at[jz - 1], dp=d ^ (jz * self.dims.lo)
                )
            )

    def own(self, g):
        s, d, z, y = self.where
        return self.summed(z, g)

    def arrive(self):
        for copy in self.along_z:
            copy.wait_recv()

    def final(self, g):
        value = self.own(g)
        for jz in range(1, self.dims.hi):
            value = value + self.recv_z[jz - 1, g].astype(F32)
        return value


def main_kernel(dims, arrays, down):
    ns, nd, hi, lo, nx = dims.ns, dims.nd, dims.hi, dims.lo, dims.nx
    tokens, width, hw, ffw, seq = dims.tokens, dims.width, dims.hw, dims.ffw, dims.seq
    heads = dims.heads
    tile = 256
    per = tokens // tile
    blocks = seq // tile
    window = seq // 2 // tile
    wide = heads * tile
    r_col, r_dense, r_down = width // (ns * nd), hw // nd, ffw // nd
    half_d, half_f = width // 2, ffw // 2
    plans = Bag(
        down0=(1, r_down, half_d, True), down1=(1, r_down, half_d, True),
        up0=(ns, r_col, half_f, False), up1=(ns, r_col, half_f, False),
        q=(ns, r_col, hw, False), k=(ns, r_col, hw, False), v=(ns, r_col, hw, False),
        dense=(1, r_dense, width, True),
    )
    columns = [n for n in plans if not plans[n][3]]
    rows_kind = [n for n in plans if plans[n][3]]
    n_net, n_local = 128, 48
    in_names = (
        "queries", "keys", "values", "keys_t", "values_t", "grad_mix", "attn", "ffn", "hat",
        "act", "slope", "grads", "w_qkv", "w_up", "w_dense",
    )
    sds = jax.ShapeDtypeStruct
    cut = (ns, tokens, hw)
    outs = Bag(
        home_out=sds(cut, BF), home_in=sds(cut, BF),
        far_out=sds((nx - 1,) + cut, BF), far_in=sds((nx - 1,) + cut, BF),
        grad_up_low=sds((seq, ffw), BF),
        own_sums=sds((8, 128), F32), swap_sums=sds((ns - 1, 8, 128), F32),
    )
    for name in rows_kind:
        groups, rows, n, _ = plans[name]
        outs["own_" + name] = sds((rows, n), F32)
        outs["z_" + name] = sds((hi - 1, 1, rows, n), BF)
    for name in columns:
        groups, rows, n, _ = plans[name]
        outs["own_" + name] = sds((rows, n), F32)
        outs["swap_" + name] = sds((ns - 1, rows, n), BF)
    scratch = Bag(
        w_qkv=sds((width, 3 * hw), BF), w_up=sds((width, ffw), BF),
        w_dense=sds((hw, width), BF), w_down=sds((nd, r_down, width), BF),
        acc=sds((ffw, width), F32), acc_k=sds((seq, hw), F32), acc_v=sds((seq, hw), F32),
        pool=sds((4, seq, hw), BF),
        keys_t=sds((hw, seq), BF), values_t=sds((hw, seq), BF),
        scores=sds(((window + 1) * tile, wide), F32),
        probs=sds(((window + 1) * tile, wide), BF),
        mixed=sds((seq, hw), BF), gq=sds((seq, hw), BF), gk=sds((seq, hw), BF),
        gv=sds((seq, hw), BF),
        got_out=sds((nx, seq, hw), BF), got_in=sds((nx, seq, hw), BF),
        out_parts=sds((2 * nx, seq, hw), BF),
        qkv_sum=sds((8, hw), F32), up_sum=sds((8, ffw), F32), gain_sum=sds((8, width), F32),
        sum_rows=sds((3 * width // 128 + 8, 128), F32),
        tiles=sds((ns, hi, lo, 8, 128), F32),
        tiles_y=sds((lo - 1, ns, hi, 8, 128), F32), tiles_z=sds((ns, hi, 8, 128), F32),
        tiles_zr=sds((hi - 1, ns, 8, 128), F32), tiles_s=sds((ns, 8, 128), F32),
    )
    for name, (groups, rows, n, landed) in plans.items():
        scratch["sy_" + name] = sds((lo - 1, hi, groups, rows, n), BF)
        scratch["ry_" + name] = sds((lo - 1, hi, groups, rows, n), BF)
        scratch["sz_" + name] = sds((hi - 1, groups, rows, n), BF)
        if not landed:
            scratch["rz_" + name] = sds((hi - 1, groups, rows, n), BF)
            scratch["sw_" + name] = sds((ns - 1, rows, n), BF)
        scratch["ob_" + name] = sds((rows, n), F32)

    def kernel(*all_refs):
        refs = list(all_refs)
        take = lambda names: Bag((name, refs.pop(0)) for name in names)
        hbm = take(in_names)
        down_ref, gout_ref, meta_ref, affine, const_ref = [refs.pop(0) for _ in range(5)]
        out = take(outs)
        vm = take(scratch)
        send_sems, recv_sems, local_sems = refs
        s, d = lax.axis_index("seq"), lax.axis_index("dp")
        z, y = d // lo, d % lo
        where = (s, d, z, y)
        net, local = Net(send_sems, recv_sems), Local(local_sems)
        loads = Bag()
        for at, name in enumerate(("queries", "keys", "values", "grad_mix")):
            loads[name] = local.load(hbm[name], vm.pool.at[at])
        for name in ("keys_t", "values_t", "w_dense", "w_qkv", "w_up"):
            loads[name] = local.load(hbm[name], vm[name])
        q_ref, k_ref, v_ref, g_ref = [vm.pool.at[at] for at in range(4)]
        greet(neighbours(dims, s, d))

        part_down = lambda at: vm.w_down.at[at]
        down_own = local.load(down_ref, part_down(d))
        z_down = [
            net.send(down_ref, part_down(d), dp=d ^ (jz * lo)) for jz in range(1, hi)
        ]
        y_down = [net.send(down_ref, part_down(d), dp=d ^ jy) for jy in range(1, lo)]

        totals = Bag(
            down0=("acc", 0, slice(0, half_d)), down1=("acc", 0, slice(half_d, width)),
            up0=("acc", 0, slice(0, half_f)), up1=("acc", 0, slice(half_f, ffw)),
            q=("scores", 0, slice(0, hw)), k=("scores", 0, slice(hw, 2 * hw)),
            v=("scores", 0, slice(2 * hw, 3 * hw)), dense=("scores", width, slice(0, width)),
        )
        sets = Bag()
        for name, (groups, rows, n, landed) in plans.items():
            total, base, cols = totals[name]
            bufs = (
                vm["sy_" + name], vm["ry_" + name], vm["sz_" + name],
                out["z_" + name] if landed else vm["rz_" + name],
            )
            sets[name] = Spread(dims, net, where, groups, rows, vm[total], base, cols, bufs)

        def tiles(body, names, size):
            pltpu.emit_pipeline(
                body,
                grid=(seq // size,),
                in_specs=[
                    pl.BlockSpec((size, hbm[n].shape[1]), lambda t: (t, 0)) for n in names
                ],
                out_specs=[],
            )(*[hbm[n] for n in names])

        def rows_of_step(size):
            return pl.ds(pl.multiple_of(pl.program_id(0) * size, size), size)

        def finish_rows(name):
            vm["ob_" + name][...] = sets[name].own(0)
            local.copy(vm["ob_" + name], out["own_" + name])

        def add_products(left, right):
            vm.acc[...] += mm_tn(left[...], right[...])

        vm.acc[...] = jnp.zeros_like(vm.acc)
        tiles(add_products, ("act", "grads"), tokens)
        sets.down0.start()

        lane = lax.broadcasted_iota(jnp.int32, (1, hw), 1)
        segments = jnp.concatenate([meta_ref[j, 16:24, :] for j in range(ns)], axis=1)
        edges = [
            jnp.sum((segments[0:1, :] < float(v)).astype(F32), axis=1, keepdims=True).astype(
                jnp.int32
            )
            for v in range(1, DOCS)
        ]

        def by_head(value):
            zero = jnp.zeros_like(value)
            return jnp.concatenate(
                [jnp.where(lane // HEAD == h, value, zero) for h in range(heads)], axis=0
            )

        def rows_at(block):
            at = ((block // per) ^ s) * per + block % per
            return pl.ds(pl.multiple_of(at * tile, tile), tile)

        for name in ("queries", "keys", "values", "grad_mix", "keys_t", "values_t"):
            loads[name].wait()
        vm.acc_k[...] = jnp.zeros_like(vm.acc_k)
        vm.acc_v[...] = jnp.zeros_like(vm.acc_v)
        vm.qkv_sum[...] = jnp.zeros_like(vm.qkv_sum)
        cols = [slice(h * tile, (h + 1) * tile) for h in range(heads)]
        lanes_of = [slice(h * HEAD, (h + 1) * HEAD) for h in range(heads)]
        scale = 1.0 / math.sqrt(HEAD)

        def attend(block, carry_in):
            here = rows_at(block)
            q_stack = by_head(q_ref[here, :])
            q_pos = block * tile + lax.broadcasted_iota(jnp.int32, (1, wide), 1) % tile
            begin = jnp.zeros((1, wide), jnp.int32)
            for edge in edges:
                begin = jnp.where(q_pos >= edge, jnp.maximum(begin, edge), begin)
            low = jnp.maximum(block - window, 0)
            key_row = lax.broadcasted_iota(jnp.int32, (tile, wide), 0)

            def slot(key_block):
                return pl.ds(pl.multiple_of((key_block - low) * tile, tile), tile)

            def score_pass(key_block, high):
                allowed = key_row >= begin - key_block * tile
                scores = jnp.where(
                    allowed, mm_nt(k_ref[rows_at(key_block), :], q_stack), masked_score
                )
                vm.scores[slot(key_block), :] = scores
                return jnp.maximum(high, jnp.max(scores, axis=0, keepdims=True))

            high = lax.fori_loop(low, block, score_pass, jnp.full((1, wide), masked_score, F32))
            allowed = (key_row >= begin - block * tile) & (key_row <= q_pos - block * tile)
            scores = jnp.where(allowed, mm_nt(k_ref[here, :], q_stack), masked_score)
            vm.scores[slot(block), :] = scores
            high = jnp.maximum(high, jnp.max(scores, axis=0, keepdims=True))

            def prob_pass(key_block, carry):
                total, mixed = carry
                rows = rows_at(key_block)
                probs = jnp.exp(vm.scores[slot(key_block), :] - high)
                total = total + jnp.sum(probs, axis=0, keepdims=True)
                probs = probs.astype(BF)
                vm.probs[slot(key_block), :] = probs
                mixed = tuple(
                    mixed[h] + mm(vm.values_t[lanes_of[h], rows], probs[:, cols[h]])
                    for h in range(heads)
                )
                return total, mixed

            zeros = tuple(jnp.zeros((HEAD, tile), F32) for _ in range(heads))
            total, mixed = lax.fori_loop(
                low, block + 1, prob_pass, (jnp.zeros((1, wide), F32), zeros)
            )
            inverse = 1.0 / total
            grads_t = g_ref[here, :].astype(F32).T
            mixed = [mixed[h] * inverse[:, cols[h]] for h in range(heads)]
            scaled = [grads_t[lanes_of[h], :] * inverse[:, cols[h]] for h in range(heads)]
            delta = jnp.concatenate(
                [jnp.sum(mixed[h] * scaled[h], axis=0, keepdims=True) for h in range(heads)],
                axis=1,
            )
            vm.mixed[here, :] = jnp.concatenate(mixed, axis=0).T.astype(BF)
            g_stack = by_head(jnp.concatenate(scaled, axis=0).T.astype(BF))

            def grad_pass(key_block, grads_q):
                rows = rows_at(key_block)
                probs = vm.probs[slot(key_block), :]
                grad_probs = mm_nt(v_ref[rows, :], g_stack)
                grad_scores = (probs.astype(F32) * (grad_probs - delta)).astype(BF)
                vm.acc_v[rows, :] += mm(probs, g_stack)
                vm.acc_k[rows, :] += mm(grad_scores, q_stack)
                return tuple(
                    grads_q[h] + mm(vm.keys_t[lanes_of[h], rows], grad_scores[:, cols[h]])
                    for h in range(heads)
                )

            grads_q = lax.fori_loop(low, block + 1, grad_pass, zeros)
            finish_grad("gq", 0, here, (jnp.concatenate(grads_q, axis=0) * scale).T)
            return carry_in

        def finish_grad(name, row, rows, value):
            if row < 2:
                start = rows.start
                cosine, sine = rotary_tables(
                    meta_ref[start // tokens, :, pl.ds(pl.multiple_of(start % tokens, tile), tile)],
                    const_ref, hw,
                )
                value = turn(value, cosine, sine, -1.0)
            value = value.astype(BF)
            vm[name][rows, :] = value
            vm.qkv_sum[row : row + 1, :] += jnp.sum(value.astype(F32), axis=0, keepdims=True)

        def attend_blocks(first, last):
            none = s // 64
            lax.fori_loop(first + none, last + none, attend, 0)

        def forward_down():
            sent = []
            for jz, done in enumerate(z_down, 1):
                done.wait_recv()
                at = (z ^ jz) * lo + y
                sent += [net.send(part_down(at), part_down(at), dp=d ^ jy) for jy in range(1, lo)]
            return sent

        parity, across = s % 2, s // 2

        def put(parts, j, start, value):
            size = value.shape[0]
            slot = (1 - j % 2) * nx + j // 2
            for c in range(ns):
                at = pl.ds(pl.multiple_of(c * tokens + start, size), size)
                parts[slot, at, :] = value[:, c * hw : (c + 1) * hw]

        def add_got(keep, got, m):
            keep[m] = (keep[m].astype(F32) + got[m].astype(F32)).astype(BF)

        def as_cut(ref):
            return ref.reshape(ns, tokens, hw)

        give_out, keep_out = vm.out_parts.at[0:nx], vm.out_parts.at[nx : 2 * nx]
        core_out = [
            net.make(give_out.at[chip ^ across], vm.got_out.at[chip ^ across], seq=s ^ 1)
            for chip in range(nx)
        ]
        far_out = net.make(as_cut(keep_out.at[1]), out.far_out.at[0], seq=s ^ 2)
        home_out = local.make(as_cut(keep_out.at[0]), out.home_out)

        def out_blocks(first, last):
            def body(act_tile):
                j = (pl.program_id(0) + first) ^ s
                rows = pl.ds(pl.multiple_of(j * tokens, tokens), tokens)
                value = mm(vm.mixed[rows, :], vm.w_dense[...]) + mm(act_tile[...], w_down())
                put(vm.out_parts, j, 0, value.astype(BF))

            pltpu.emit_pipeline(
                body,
                grid=(last - first,),
                in_specs=[pl.BlockSpec((tokens, ffw), lambda t: ((t + first) ^ s, 0))],
                out_specs=[],
            )(hbm.act)

        def cross_out(chip):
            core_out[chip].wait_recv()
            add_got(keep_out, vm.got_out, chip ^ across)

            @pl.when(across == chip)
            def _():
                home_out.start()

            @pl.when(across != chip)
            def _():
                far_out.start()

        attend_blocks(0, blocks // 2)
        y_down += forward_down()
        sets.down1.start()
        attend_blocks(blocks // 2, 3 * blocks // 4)
        sets.down0.middle()
        for done in y_down:
            done.wait_recv()
        down_own.wait()
        vm.up_sum[...] = jnp.zeros_like(vm.up_sum)
        w_down = lambda: vm.w_down[...].reshape(ffw, width)

        def up_tile(g_tile, slope_tile, gu_tile):
            grads = (mm_nt(g_tile[...], w_down()) * slope_tile[...].astype(F32)).astype(BF)
            gu_tile[...] = grads
            vm.up_sum[0:1, :] += jnp.sum(grads.astype(F32), axis=0, keepdims=True)

        pltpu.emit_pipeline(
            up_tile,
            grid=(blocks,),
            in_specs=[
                pl.BlockSpec((tile, width), lambda t: (t, 0)),
                pl.BlockSpec((tile, ffw), lambda t: (t, 0)),
            ],
            out_specs=[pl.BlockSpec((tile, ffw), lambda t: (t, 0))],
        )(hbm.grads, hbm.slope, out.grad_up_low)
        hbm["gu"] = out.grad_up_low
        sets.down1.middle()
        finish_rows("down0")
        finish_rows("down1")
        vm.acc[...] = jnp.zeros_like(vm.acc)
        tiles(add_products, ("ffn", "gu"), tokens)
        sets.up0.start()
        sets.up1.start()
        loads.w_dense.wait()
        out_blocks(0, ns - 1)
        core_out[0].start()

        @pl.when(parity == 1)
        def _():
            core_out[1].start()

        attend_blocks(blocks - 2, blocks - 1)
        cross_out(0)

        @pl.when(parity == 0)
        def _():
            cross_out(1)

        sets.up0.middle()
        attend_blocks(blocks - 1, blocks)
        out_blocks(ns - 1, ns)

        @pl.when(parity == 0)
        def _():
            core_out[1].start()

        sets.up1.middle()

        def finish_kv(t, carry):
            rows = pl.ds(pl.multiple_of(t * tile, tile), tile)
            finish_grad("gk", 1, rows, vm.acc_k[rows, :])
            finish_grad("gv", 2, rows, vm.acc_v[rows, :])
            return carry

        lax.fori_loop(0, blocks, finish_kv, 0)

        @pl.when(parity == 1)
        def _():
            cross_out(1)

        def qkv_tile(left):
            rows = rows_of_step(tokens)
            right = jnp.concatenate([vm[n][rows, :] for n in ("gq", "gk", "gv")], axis=1)
            vm.scores[0:width, 0 : 3 * hw] += mm_tn(left[...], right)

        vm.scores[...] = jnp.zeros_like(vm.scores)
        tiles(qkv_tile, ("attn",), tokens)
        for name in ("q", "k", "v"):
            sets[name].start()

        loads.w_qkv.wait()
        loads.w_up.wait()
        vm.gain_sum[...] = jnp.zeros_like(vm.gain_sum)
        give_in, keep_in = vm.pool.at[0:nx], vm.pool.at[nx : 2 * nx]
        core_in = [net.make(give_in.at[m], vm.got_in.at[m], seq=s ^ 1) for m in range(nx)]
        far_in = net.make(as_cut(keep_in.at[1]), out.far_in.at[0], seq=s ^ 2)
        home_in = local.make(as_cut(keep_in.at[0]), out.home_in)

        def in_blocks(m):
            first = 2 * m * per

            def body(gu_tile, hat_tile):
                t = pl.program_id(0) + first
                rows = pl.ds(pl.multiple_of(t * tile, tile), tile)
                joined = jnp.concatenate([vm[n][rows, :] for n in ("gq", "gk", "gv")], axis=1)
                attn = mm_nt(joined, vm.w_qkv[...])
                ffn = mm_nt(gu_tile[...], vm.w_up[...])
                hat = hat_tile[...].astype(F32)
                for row, value in ((1, attn), (3, ffn), (0, attn * hat), (2, ffn * hat)):
                    vm.gain_sum[row : row + 1, :] += jnp.sum(value, axis=0, keepdims=True)
                value = attn * affine[0:1, :] + ffn * affine[2:3, :]
                put(vm.pool, t // per, (t % per) * tile, value.astype(BF))

            pltpu.emit_pipeline(
                body,
                grid=(2 * per,),
                in_specs=[
                    pl.BlockSpec((tile, ffw), lambda t: (t + first, 0)),
                    pl.BlockSpec((tile, width), lambda t: (t + first, 0)),
                ],
                out_specs=[],
            )(hbm.gu, hbm.hat)
            core_in[m].start()

        in_blocks(1)
        sets.q.middle()

        def dense_tile(g_tile):
            left = vm.mixed[rows_of_step(tokens), :]
            vm.scores[width : width + hw, :] += mm_tn(left, g_tile[...])

        tiles(dense_tile, ("grads",), tokens)
        sets.dense.start()
        core_in[1].wait_recv()
        add_got(keep_in, vm.got_in, 1)
        far_in.start()
        sets.k.middle()
        in_blocks(0)
        sets.v.middle()

        rows = vm.sum_rows
        rows[...] = jnp.zeros_like(rows)
        parts = hw // 128
        for part in range(3):
            for k in range(parts):
                rows[pl.ds(part * (width // 128) + s * parts + k, 1), :] = vm.qkv_sum[
                    part : part + 1, k * 128 : (k + 1) * 128
                ]

        def own_sum(t, total):
            return total + jnp.sum(
                gout_ref[pl.ds(pl.multiple_of(t * 128, 128), 128), :].astype(F32), axis=0,
                keepdims=True,
            )

        out_sum = lax.fori_loop(0, tokens // 128, own_sum, jnp.zeros((1, width), F32))
        lane_row = lax.broadcasted_iota(jnp.int32, (1, 128), 1)
        n = width // (ns * nd)
        per_row = 128 // n
        split = lambda owner: (owner // nd, owner % nd // lo, owner % lo)
        for row in range(width // 128):
            at = slice(row * 128, (row + 1) * 128)
            stack = jnp.concatenate(
                [jnp.zeros((1, 128), F32), out_sum[:, at], jnp.zeros((1, 128), F32)]
                + [vm.gain_sum[k : k + 1, at] for k in range(4)]
                + [jnp.zeros((1, 128), F32)],
                axis=0,
            )
            for q in range(per_row):
                a, b, c = split(row * per_row + q)
                vm.tiles[a, b, c] = pltpu.roll(stack, 128 - q * n, 1) if q else stack
        n = 3 * n
        for owner in range(ns * nd):
            start, row = owner * n % 128, owner * n // 128
            value = rows[row : row + 1, :]
            if start + n > 128:
                value = jnp.where(lane_row >= start, value, rows[row + 1 : row + 2, :])
            a, b, c = split(owner)
            vm.tiles[a, b, c, 0:1, :] = pltpu.roll(value, 128 - start, 1) if start else value
        for c in range(ffw // 128):
            vm.tiles[s, c // lo, c % lo, 2:3, :] = vm.up_sum[0:1, c * 128 : (c + 1) * 128]
        tiles_y = [
            net.send(vm.tiles.at[:, :, y ^ jy], vm.tiles_y.at[jy - 1], dp=d ^ jy)
            for jy in range(1, lo)
        ]

        def column_home(name):
            sets[name].arrive()
            vm["ob_" + name][...] = sets[name].final(s)
            local.copy(vm["ob_" + name], out["own_" + name])
            sent = []
            for js in range(1, ns):
                vm["sw_" + name][js - 1] = sets[name].final(s ^ js).astype(BF)
                sent.append(
                    net.send(
                        vm["sw_" + name].at[js - 1], out["swap_" + name].at[js - 1], seq=s ^ js
                    )
                )
            return sent

        core_in[0].wait_recv()
        add_got(keep_in, vm.got_in, 0)
        home_in.start()
        sent = column_home("up0")
        sets.dense.middle()
        finish_rows("dense")
        for done in tiles_y:
            done.wait_recv()
        total = vm.tiles[:, :, y]
        for jy in range(1, lo):
            total = total + vm.tiles_y[jy - 1]
        vm.tiles_z[...] = total
        tiles_z = [
            net.send(vm.tiles_z.at[:, z ^ jz], vm.tiles_zr.at[jz - 1], dp=d ^ (jz * lo))
            for jz in range(1, hi)
        ]
        for name in ("up1", "q", "k", "v"):
            sent += column_home(name)
        for done in tiles_z:
            done.wait_recv()
        total = vm.tiles_z[:, z]
        for jz in range(1, hi):
            total = total + vm.tiles_zr[jz - 1]
        vm.tiles_s[...] = total
        sent += [
            net.send(vm.tiles_s.at[s ^ js], out.swap_sums.at[js - 1], seq=s ^ js)
            for js in range(1, ns)
        ]
        local.copy(vm.tiles_s.at[s], out.own_sums)
        for name in rows_kind:
            sets[name].arrive()
        far_out.wait_recv()
        far_in.wait_recv()
        for done in sent:
            done.wait_recv()
        local.finish()
        net.finish()

    any_spec = pl.BlockSpec(memory_space=pl.ANY)
    vmem_spec = pl.BlockSpec(memory_space=pltpu.VMEM)
    results = pl.pallas_call(
        kernel,
        out_shape=list(outs.values()),
        in_specs=[any_spec] * (len(in_names) + 1) + [vmem_spec] * 4,
        out_specs=[any_spec] * len(outs),
        scratch_shapes=[pltpu.VMEM(x.shape, x.dtype) for x in scratch.values()]
        + [
            pltpu.SemaphoreType.DMA((n_net,)), pltpu.SemaphoreType.DMA((n_net,)),
            pltpu.SemaphoreType.DMA((n_local,)),
        ],
        compiler_params=pltpu.CompilerParams(
            vmem_limit_bytes=MAIN_LIMIT, collective_id=2, has_side_effects=True
        ),
        name="main",
    )(
        *[arrays[n] for n in in_names], down, arrays.grad_out, arrays.meta,
        arrays.affine, jnp.asarray(table_constants()),
    )
    return dict(zip(outs, results))


def finish_kernel(dims, s, hidden, grad_out, affine, parts):
    ns, nd, hi, nx = dims.ns, dims.nd, dims.hi, dims.nx
    tokens, width, hw, ffw = dims.tokens, dims.width, dims.hw, dims.ffw
    r_col, r_dense, r_down = width // (ns * nd), hw // nd, ffw // nd
    tile = 128
    names = [n for n in parts if n != "grad_up_low"]
    token_names = [n for n in names if n.startswith(("home", "far"))]
    sds = jax.ShapeDtypeStruct

    def kernel(s_ref, hid, gout, affine_ref, *refs):
        part = dict(zip(names, refs[: len(names)]))
        out_ref, in_ref, qkv_out, dense_out, up_out, down_out, sums_out = refs[len(names) :]
        step = pl.program_id(0)
        here = s_ref[0]

        def whole_sum(name):
            columns = []
            for c in range(ns):
                value = part["home_" + name][c].astype(F32)
                for m in range(nx - 1):
                    value = value + part["far_" + name][m, c].astype(F32)
                columns.append(value)
            return jnp.concatenate(columns, axis=1)

        x = hid[...].astype(F32)
        out_ref[...] = (x + whole_sum("out") + affine_ref[4:5, :]).astype(BF)
        gx = whole_sum("in")
        spread = x - jnp.mean(x, axis=-1, keepdims=True)
        inv_std = lax.rsqrt(jnp.mean(spread * spread, axis=-1, keepdims=True) + epsilon)
        hat = spread * inv_std
        back = inv_std * (
            gx
            - jnp.mean(gx, axis=-1, keepdims=True)
            - hat * jnp.mean(gx * hat, axis=-1, keepdims=True)
        )
        in_ref[...] = (gout[...].astype(F32) + back).astype(BF)

        def rows_sum(name):
            value = part["own_" + name][...]
            for jz in range(hi - 1):
                value = value + part["z_" + name][jz, 0].astype(F32)
            return value

        @pl.when(step == 0)
        def _():
            down_out[:, : width // 2] = rows_sum("down0")
            down_out[:, width // 2 :] = rows_sum("down1")
            dense_out[...] = rows_sum("dense")

        def place(target, name, base):
            w = part["own_" + name].shape[1]
            block = width // 1 if target is qkv_out else ffw
            for js in range(ns):
                owner = here ^ js
                at = base(owner)
                value = (
                    part["own_" + name][...]
                    if js == 0
                    else part["swap_" + name][js - 1].astype(F32)
                )
                target[:, pl.ds(pl.multiple_of(at, 128), w)] = value

        @pl.when(step == 1)
        def _():
            for k, name in enumerate(("q", "k", "v")):
                place(qkv_out, name, lambda owner, k=k: k * width + owner * hw)

        @pl.when(step == 2)
        def _():
            for k, name in enumerate(("up0", "up1")):
                place(up_out, name, lambda owner, k=k: owner * ffw + k * (ffw // 2))
            total = part["own_sums"][...]
            for js in range(ns - 1):
                total = total + part["swap_sums"][js]
            sums_out[...] = total

    def spec(name):
        shape = parts[name].shape
        if name in token_names:
            lead = shape[:-2]
            zeros = (0,) * len(lead)
            return pl.BlockSpec(lead + (tile, hw), lambda t, s_ref: zeros + (t, 0))
        return whole(shape)

    token_spec = pl.BlockSpec((tile, width), lambda t, s_ref: (t, 0))
    finals = [
        (r_col, 3 * width), (r_dense, width), (r_col, ffw * ns), (r_down, width), (8, 128)
    ]
    return pl.pallas_call(
        kernel,
        out_shape=[sds((tokens, width), BF)] * 2 + [sds(f, F32) for f in finals],
        grid_spec=pltpu.PrefetchScalarGridSpec(
            num_scalar_prefetch=1,
            grid=(tokens // tile,),
            in_specs=[token_spec, token_spec, whole(affine.shape)] + [spec(n) for n in names],
            out_specs=[token_spec, token_spec] + [whole(f) for f in finals],
        ),
        compiler_params=params_of(),
        name="finish",
    )(s, hidden, grad_out, affine, *[parts[n] for n in names])


def fused_plan(
    hidden_states,
    segment_ids,
    positions,
    out_grad,
    qkv_weight,
    qkv_bias,
    dense_weight,
    dense_bias,
    up_weight,
    up_bias,
    down_weight,
    down_bias,
    attn_gain,
    attn_shift,
    ffn_gain,
    ffn_shift,
):
    ns, nd = lax.axis_size("seq"), lax.axis_size("dp")
    tokens, width = hidden_states.shape[1:]
    dims = Dims(ns, nd, tokens, width, up_weight.shape[1])
    s = lax.axis_index("seq").astype(jnp.int32).reshape(1)
    hidden, grad_out = hidden_states[0], out_grad[0]
    fields = (
        qkv_bias, dense_bias, up_bias, down_bias, attn_gain, attn_shift, ffn_gain, ffn_shift
    )
    small = jnp.stack([jnp.pad(f, (0, 128 - f.shape[0])) for f in fields]).astype(F32)
    half = ROT // 2
    freqs = rotary_base ** (-2.0 * jnp.arange(half, dtype=F32) / ROT)
    angles = positions[0].astype(F32)[None, :] * freqs[:, None]
    meta = jnp.concatenate(
        [
            jnp.cos(angles),
            jnp.sin(angles),
            jnp.broadcast_to(segment_ids[0].astype(F32)[None, :], (half, tokens)),
        ],
        axis=0,
    )
    names = (
        "attn", "ffn", "hat", "grads", "act", "slope", "queries", "keys", "values", "keys_t",
        "values_t", "grad_mix", "w_qkv", "w_up", "w_dense", "meta", "affine",
    )
    arrays = Bag(
        zip(
            names,
            gather_kernel(
                dims, hidden, grad_out, meta, small, qkv_weight, up_weight, dense_weight
            ),
        )
    )
    arrays["w_qkv"] = arrays.w_qkv.reshape(width, -1)
    arrays["w_up"] = arrays.w_up.reshape(width, -1)
    arrays["w_dense"] = arrays.w_dense.reshape(-1, width)
    arrays["grad_out"] = grad_out
    parts = main_kernel(dims, arrays, down_weight)
    output, input_grad, grad_qkv, grad_dense, grad_up, grad_down, sums = finish_kernel(
        dims, s, hidden, grad_out, arrays.affine, parts
    )
    share = width // (ns * nd)
    gb_out = sums[1, :share]
    return (
        output[None],
        input_grad[None],
        grad_qkv,
        sums[0, : qkv_bias.shape[0]],
        grad_dense,
        gb_out,
        grad_up,
        sums[2, : up_bias.shape[0]],
        grad_down,
        gb_out,
        sums[3, :share],
        sums[4, :share],
        sums[5, :share],
        sums[6, :share],
    )


def per_device(*args):
    tokens, width = args[0].shape[1:]
    ns, nd = lax.axis_size("seq"), lax.axis_size("dp")
    fits = ns == 4 and ns * tokens * width <= 2048 * 1024 and width // (ns * nd) % 16 == 0
    return fused_plan(*args) if fits else permute_plan(*args)


def solution(mesh):
    token = P("dp", "seq", None)
    matrix = P(("seq", "dp"), None)
    vector = P(("seq", "dp"))
    weights = (matrix, vector) * 4 + (vector,) * 4
    return jax.shard_map(
        per_device,
        mesh=mesh,
        in_specs=(token, P("dp", "seq"), P("dp", "seq"), token) + weights,
        out_specs=(token, token) + weights,
        check_vma=False,
    )
```

```python
import functools
import math

import jax
import jax.numpy as jnp
import numpy as np
from jax import lax
from jax.experimental import pallas as pl
from jax.experimental.pallas import tpu as pltpu
from jax.sharding import PartitionSpec as P

HEAD = 64
ROT = 16
DOCS = 4
HI = 4

epsilon = 1e-05
masked_score = -1e30
rotary_base = 10000.0

BF = jnp.bfloat16
F32 = jnp.float32
NT = (((1,), (1,)), ((), ()))
TN = (((0,), (0,)), ((), ()))


VMEM_LIMIT = 60 * 1024 * 1024
MAIN_LIMIT = 61 * 1024 * 1024


def xor_swap(value, axis, count, mask):
    return lax.ppermute(value, axis, [(i, i ^ mask) for i in range(count)])


def mm(left, right):
    return jnp.dot(left, right, preferred_element_type=F32)


def mm_nt(left, right):
    return lax.dot_general(left, right, NT, preferred_element_type=F32)


def mm_tn(left, right):
    return lax.dot_general(left, right, TN, preferred_element_type=F32)


def params_of(**more):
    return pltpu.CompilerParams(vmem_limit_bytes=VMEM_LIMIT, **more)


def whole(shape):
    zeros = (0,) * len(shape)
    return pl.BlockSpec(shape, lambda *grid_and_ids: zeros)


class Dims:
    def __init__(self, ns, nd, tokens, width, ff):
        self.ns, self.nd = ns, nd
        self.hi, self.lo = HI, nd // HI
        self.nx = ns // 2
        self.tokens, self.width = tokens, width
        self.seq = ns * tokens
        self.hw = width // ns
        self.ffw = ff // ns
        self.heads = self.hw // HEAD


def piece_copies(dims, kind, ids, pieces, target, sems):
    s, z, y = ids[0], ids[1], ids[2]
    copies = []
    for jz in range(dims.hi):
        for jy in range(dims.lo):
            piece = pieces[jz * dims.lo + jy]
            owner = (z ^ jz) * dims.lo + (y ^ jy)
            if kind == "row":
                rows = piece.shape[0]
                at = pl.multiple_of(owner * rows, rows)
                copies.append(
                    pltpu.make_async_copy(piece, target.at[pl.ds(at, rows)], sems.at[len(copies)])
                )
            else:
                rows = piece.shape[1]
                for js in range(dims.ns):
                    at = pl.multiple_of(((s ^ js) * dims.nd + owner) * rows, rows)
                    copies.append(
                        pltpu.make_async_copy(
                            piece.at[js], target.at[pl.ds(at, rows)], sems.at[len(copies)]
                        )
                    )
    return copies


def token_call(dims, name, ids, body, lhs, weights, extras, outs, tile, flops, scratch=()):
    count = dims.seq // tile
    n_lhs, n_out = len(lhs), len(outs)
    sizes = [len(w[1]) for w in weights]
    sem_counts = [
        len(w[1]) * (dims.ns if w[0] == "col" else 1) for w in weights
    ]

    def kernel(ids_ref, *refs):
        at = 0
        lhs_refs = refs[:n_lhs]
        at = n_lhs
        piece_refs = []
        for size in sizes:
            piece_refs.append(refs[at : at + size])
            at += size
        extra_refs = refs[at : at + len(extras)]
        at += len(extras)
        out_refs = refs[at : at + n_out]
        at += n_out
        weight_refs = refs[at : at + len(weights)]
        at += len(weights)
        sem_refs = refs[at : at + len(weights)]
        at += len(weights)
        scratch_refs = refs[at:]
        step = pl.program_id(0)

        if weights:

            @pl.when(step == 0)
            def _():
                copies = []
                for w, group, target, sems in zip(weights, piece_refs, weight_refs, sem_refs):
                    copies += piece_copies(dims, w[0], ids_ref, group, target, sems)
                for copy in copies:
                    copy.start()
                for copy in copies:
                    copy.wait()

        body(step, count, lhs_refs, weight_refs, extra_refs, out_refs, scratch_refs)

    in_specs = [pl.BlockSpec((tile, a.shape[1]), lambda i, ids_ref: (i, 0)) for a in lhs]
    for size in sizes:
        in_specs += [pl.BlockSpec(memory_space=pl.ANY)] * size
    in_specs += [whole(a.shape) for a in extras]
    bytes_moved = sum(a.size * a.dtype.itemsize for a in lhs) + sum(
        math.prod(o[0].shape) * o[0].dtype.itemsize for o in outs
    )
    return pl.pallas_call(
        kernel,
        out_shape=[o[0] for o in outs],
        grid_spec=pltpu.PrefetchScalarGridSpec(
            num_scalar_prefetch=1,
            grid=(count,),
            in_specs=in_specs,
            out_specs=[o[1] for o in outs],
            scratch_shapes=[pltpu.VMEM(w[2], BF) for w in weights]
            + [pltpu.SemaphoreType.DMA((n,)) for n in sem_counts]
            + list(scratch),
        ),
        compiler_params=params_of(),
        cost_estimate=pl.CostEstimate(flops=flops, bytes_accessed=bytes_moved, transcendentals=0),
        name=name,
    )(ids, *lhs, *[p for w in weights for p in w[1]], *extras)


def tiled_out(rows, cols, tile, dtype=BF):
    return (
        jax.ShapeDtypeStruct((rows, cols), dtype),
        pl.BlockSpec((tile, cols), lambda i, ids_ref: (i, 0)),
    )


def norm_pair(dims, pair, first, second, affine, carried):
    tile = 256
    per = dims.tokens // tile
    base = pair * 2 * per

    def kernel(*refs):
        a_ref, b_ref, affine_ref = refs[:3]
        attn_ref, ffn_ref, hat_ref, rows_ref = refs[-4:]
        block = pl.program_id(0)

        @pl.when(block == 0)
        def _():
            rows_ref[...] = a_ref[...]

        @pl.when(block == 1)
        def _():
            rows_ref[...] = b_ref[...]

        rows = rows_ref[...].astype(F32)
        center = jnp.mean(rows, axis=-1, keepdims=True)
        spread = rows - center
        hat = spread * lax.rsqrt(jnp.mean(spread * spread, axis=-1, keepdims=True) + epsilon)
        attn_ref[...] = (hat * affine_ref[0:1, :] + affine_ref[1:2, :]).astype(BF)
        ffn_ref[...] = (hat * affine_ref[2:3, :] + affine_ref[3:4, :]).astype(BF)
        hat_ref[...] = hat.astype(BF)

    out_spec = pl.BlockSpec((tile, dims.width), lambda b, t: (base + b * per + t, 0))
    shape = jax.ShapeDtypeStruct((dims.seq, dims.width), BF)
    return pl.pallas_call(
        kernel,
        out_shape=[shape] * 3,
        grid=(2, per),
        in_specs=[
            pl.BlockSpec((tile, dims.width), lambda b, t: (jnp.where(b == 0, t, per - 1), 0)),
            pl.BlockSpec((tile, dims.width), lambda b, t: (jnp.where(b == 0, 0, t), 0)),
            pl.BlockSpec((8, dims.width), lambda b, t: (0, 0)),
        ]
        + [pl.BlockSpec(memory_space=pl.ANY)] * len(carried),
        out_specs=[out_spec] * 3,
        scratch_shapes=[pltpu.VMEM((tile, dims.width), BF)],
        input_output_aliases={3 + i: i for i in range(len(carried))},
        compiler_params=params_of(),
        cost_estimate=pl.CostEstimate(
            flops=20 * 2 * dims.tokens * dims.width,
            bytes_accessed=2 * dims.tokens * dims.width * 8,
            transcendentals=0,
        ),
        name="norm_pair",
    )(first, second, affine, *carried)


def up_body(step, count, lhs, weights, extras, outs, scratch):
    pre = mm(lhs[0][...], weights[0][...]) + extras[0][0:1, :]
    total = 0.5 + 0.5 * lax.erf(pre * math.sqrt(0.5))
    density = jnp.exp(-0.5 * pre * pre) * (1.0 / math.sqrt(2.0 * math.pi))
    outs[0][...] = (pre * total).astype(BF)
    outs[1][...] = (total + pre * density).astype(BF)


def turn(values, cosine, sine, sign):
    lane = lax.broadcasted_iota(jnp.int32, (1, values.shape[1]), 1) % HEAD
    width = values.shape[1]
    half = ROT // 2
    other = jnp.where(
        lane < half, pltpu.roll(values, width - half, 1), pltpu.roll(values, half, 1)
    )
    return values * cosine + sign * (other * sine)


def spread_lanes(table, width):
    times = width // table.shape[1]
    return table if times == 1 else jnp.concatenate([table] * times, axis=1)


def qkv_body(dims, step, count, lhs, weights, extras, outs, scratch):
    hw = dims.hw
    joined = mm(lhs[0][...], weights[0][...]) + extras[0][0:1, :]
    cosine = spread_lanes(lhs[1][...], hw)
    sine = spread_lanes(lhs[2][...], hw)
    queries = turn(joined[:, :hw], cosine, sine, 1.0)
    keys = turn(joined[:, hw : 2 * hw], cosine, sine, 1.0)
    values = joined[:, 2 * hw :]
    outs[0][...] = queries.astype(BF) * (1.0 / math.sqrt(HEAD))
    outs[1][...] = keys.astype(BF)
    outs[2][...] = values.astype(BF)
    outs[3][...] = keys.T.astype(BF)
    outs[4][...] = values.T.astype(BF)


def mix_grad_body(step, count, lhs, weights, extras, outs, scratch):
    outs[0][...] = mm_nt(lhs[0][...], weights[0][...]).astype(BF)


def attention(dims, ids, queries, keys, values, keys_t, values_t, grad_mix, cos_table, sin_table):
    tile = 256
    hw, seq, heads = dims.hw, dims.seq, dims.heads
    per = dims.tokens // tile
    count = seq // tile
    scale = 1.0 / math.sqrt(HEAD)

    def place(ids_ref, block):
        return ((block // per) ^ ids_ref[0]) * per + block % per

    def kernel(
        ids_ref, q_ref, k_ref, v_ref, kt_ref, vt_ref, g_ref, cos_ref, sin_ref,
        mix_ref, gq_ref, gk_ref, gv_ref, sum_ref,
        score_ref, prob_ref, gk_acc, gv_acc,
    ):
        block = pl.program_id(0)

        @pl.when(block == 0)
        def _():
            gk_acc[...] = jnp.zeros_like(gk_acc)
            gv_acc[...] = jnp.zeros_like(gv_acc)
            sum_ref[...] = jnp.zeros_like(sum_ref)

        lane = lax.broadcasted_iota(jnp.int32, (1, hw), 1)
        own = [lane // HEAD == h for h in range(heads)]
        queries_here = q_ref[...]
        grads_here = g_ref[...]
        q_heads = [jnp.where(own[h], queries_here, jnp.zeros_like(queries_here)) for h in range(heads)]
        q_pos = block * tile + lax.broadcasted_iota(jnp.int32, (1, tile), 1)
        begin = jnp.zeros((1, tile), jnp.int32)
        low = 0
        for doc in range(1, DOCS):
            edge = ids_ref[doc]
            begin = jnp.where(q_pos >= edge, jnp.maximum(begin, edge), begin)
            low = jnp.where(edge <= block * tile, jnp.maximum(low, edge), low)
        low = low // tile

        def rows_of(key_block):
            return pl.ds(pl.multiple_of(place(ids_ref, key_block) * tile, tile), tile)

        def slot(key_block):
            return pl.ds(pl.multiple_of((key_block - low) * tile, tile), tile)

        def score_pass(key_block, highs):
            rows = k_ref[rows_of(key_block), :]
            key_pos = key_block * tile + lax.broadcasted_iota(jnp.int32, (tile, tile), 0)
            allowed = (key_pos >= begin) & (key_pos <= q_pos)
            result = []
            for h in range(heads):
                scores = jnp.where(allowed, mm_nt(rows, q_heads[h]), masked_score)
                score_ref[h, slot(key_block), :] = scores
                result.append(jnp.maximum(highs[h], jnp.max(scores, axis=0, keepdims=True)))
            return tuple(result)

        highs = lax.fori_loop(
            low, block + 1, score_pass,
            tuple(jnp.full((1, tile), masked_score, F32) for _ in range(heads)),
        )

        def prob_pass(key_block, carry):
            result = []
            rows = rows_of(key_block)
            for h in range(heads):
                total, mixed = carry[2 * h], carry[2 * h + 1]
                probs = jnp.exp(score_ref[h, slot(key_block), :] - highs[h])
                total = total + jnp.sum(probs, axis=0, keepdims=True)
                probs = probs.astype(BF)
                prob_ref[h, slot(key_block), :] = probs
                mixed = mixed + mm(vt_ref[h * HEAD : (h + 1) * HEAD, rows], probs)
                result += [total, mixed]
            return tuple(result)

        start = []
        for h in range(heads):
            start += [jnp.zeros((1, tile), F32), jnp.zeros((HEAD, tile), F32)]
        summed = lax.fori_loop(low, block + 1, prob_pass, tuple(start))

        grads_t = grads_here.astype(F32).T
        mixed_parts, scaled_parts, deltas = [], [], []
        for h in range(heads):
            inverse = 1.0 / summed[2 * h]
            mixed = summed[2 * h + 1] * inverse
            grads = grads_t[h * HEAD : (h + 1) * HEAD, :] * inverse
            deltas.append(jnp.sum(mixed * grads, axis=0, keepdims=True))
            mixed_parts.append(mixed)
            scaled_parts.append(grads)
        mix_ref[...] = jnp.concatenate(mixed_parts, axis=0).T.astype(BF)
        scaled = jnp.concatenate(scaled_parts, axis=0).T.astype(BF)
        g_heads = [jnp.where(own[h], scaled, jnp.zeros_like(scaled)) for h in range(heads)]

        def grad_pass(key_block, grads_q):
            rows = rows_of(key_block)
            value_rows = v_ref[rows, :]
            result = []
            grad_k = gk_acc[rows, :]
            grad_v = gv_acc[rows, :]
            for h in range(heads):
                probs = prob_ref[h, slot(key_block), :]
                grad_probs = mm_nt(value_rows, g_heads[h])
                grad_scores = (probs.astype(F32) * (grad_probs - deltas[h])).astype(BF)
                grad_v = grad_v + mm(probs, g_heads[h])
                grad_k = grad_k + mm(grad_scores, q_heads[h])
                result.append(
                    grads_q[h] + mm(kt_ref[h * HEAD : (h + 1) * HEAD, rows], grad_scores)
                )
            gk_acc[rows, :] = grad_k
            gv_acc[rows, :] = grad_v
            return tuple(result)

        grads_q = lax.fori_loop(
            low, block + 1, grad_pass, tuple(jnp.zeros((HEAD, tile), F32) for _ in range(heads))
        )
        here = rows_of(block)
        rot = (jnp.concatenate(grads_q, axis=0) * scale).T
        grad_q = turn(
            rot, spread_lanes(cos_ref[here, :], hw), spread_lanes(sin_ref[here, :], hw), -1.0
        ).astype(BF)
        gq_ref[...] = grad_q
        sum_ref[0:1, :] += jnp.sum(grad_q.astype(F32), axis=0, keepdims=True)

        @pl.when(block == count - 1)
        def _():
            def finish(t, carry):
                rows = pl.ds(pl.multiple_of(t * tile, tile), tile)
                grad_k = turn(
                    gk_acc[rows, :],
                    spread_lanes(cos_ref[rows, :], hw),
                    spread_lanes(sin_ref[rows, :], hw),
                    -1.0,
                ).astype(BF)
                grad_v = gv_acc[rows, :].astype(BF)
                gk_ref[rows, :] = grad_k
                gv_ref[rows, :] = grad_v
                sum_ref[1:2, :] += jnp.sum(grad_k.astype(F32), axis=0, keepdims=True)
                sum_ref[2:3, :] += jnp.sum(grad_v.astype(F32), axis=0, keepdims=True)
                return carry

            lax.fori_loop(0, count, finish, 0)

    tiled = pl.BlockSpec((tile, hw), lambda i, ids_ref: (place(ids_ref, i), 0))
    shape = jax.ShapeDtypeStruct((seq, hw), BF)
    return pl.pallas_call(
        kernel,
        out_shape=[shape] * 4 + [jax.ShapeDtypeStruct((8, hw), F32)],
        grid_spec=pltpu.PrefetchScalarGridSpec(
            num_scalar_prefetch=1,
            grid=(count,),
            in_specs=[
                tiled,
                whole((seq, hw)),
                whole((seq, hw)),
                whole((hw, seq)),
                whole((hw, seq)),
                tiled,
                whole(cos_table.shape),
                whole(sin_table.shape),
            ],
            out_specs=[tiled, tiled, whole((seq, hw)), whole((seq, hw)), whole((8, hw))],
            scratch_shapes=[
                pltpu.VMEM((heads, seq, tile), F32),
                pltpu.VMEM((heads, seq, tile), BF),
                pltpu.VMEM((seq, hw), F32),
                pltpu.VMEM((seq, hw), F32),
            ],
        ),
        compiler_params=params_of(),
        cost_estimate=pl.CostEstimate(
            flops=12 * seq * seq * hw, bytes_accessed=10 * seq * hw * 2, transcendentals=0
        ),
        name="attention",
    )(ids, queries, keys, values, keys_t, values_t, grad_mix, cos_table, sin_table)


def split_specs(dims, tile):
    per = dims.tokens // tile
    shape = jax.ShapeDtypeStruct((dims.nx, dims.tokens, dims.width), BF)

    def spec(odd):
        def index(i, ids_ref):
            block, t = i // per, i % per
            mine = block % 2 == odd
            row = jnp.where(mine, t, per - 1 if odd == 0 else 0)
            return (block // 2, row, 0)

        return pl.BlockSpec((None, tile, dims.width), index)

    return [(shape, spec(1)), (shape, spec(0))], per


def put_split(step, per, outs, value):
    odd = (step // per) % 2

    @pl.when(odd == 1)
    def _():
        outs[0][...] = value

    @pl.when(odd == 0)
    def _():
        outs[1][...] = value


def out_body(per, step, count, lhs, weights, extras, outs, scratch):
    value = mm(lhs[0][...], weights[0][...]) + mm(lhs[1][...], weights[1][...])
    put_split(step, per, outs, value.astype(BF))


def up_grad_body(step, count, lhs, weights, extras, outs, scratch):
    grads = (mm_nt(lhs[0][...], weights[0][...]) * lhs[1][...].astype(F32)).astype(BF)
    outs[0][...] = grads

    @pl.when(step == 0)
    def _():
        outs[1][...] = jnp.zeros_like(outs[1])

    outs[1][0:1, :] += jnp.sum(grads.astype(F32), axis=0, keepdims=True)


def in_grad_body(per, hw, step, count, lhs, weights, extras, outs, scratch):
    up_grad, gq, gk, gv, hat_ref = lhs
    qkv_ref, up_ref = weights
    affine = extras[0]
    attn = (
        mm_nt(gq[...], qkv_ref[:, :hw])
        + mm_nt(gk[...], qkv_ref[:, hw : 2 * hw])
        + mm_nt(gv[...], qkv_ref[:, 2 * hw :])
    )
    ffn = mm_nt(up_grad[...], up_ref[...])
    hat = hat_ref[...].astype(F32)

    @pl.when(step == 0)
    def _():
        outs[2][...] = jnp.zeros_like(outs[2])

    for row, value in enumerate((attn * hat, attn, ffn * hat, ffn)):
        outs[2][row : row + 1, :] += jnp.sum(value, axis=0, keepdims=True)
    put_split(step, per, outs, (attn * affine[0:1, :] + ffn * affine[2:3, :]).astype(BF))


def weight_grad(dims, name, kind, ids, left, rights):
    tile = 512
    m = left.shape[1]
    widths = [r.shape[1] for r in rights]
    n = sum(widths)
    count = dims.seq // tile
    hi, lo, ns, nd = dims.hi, dims.lo, dims.ns, dims.nd
    if kind == "row":
        rows = m // nd
        shape = (hi, rows, n)
    else:
        rows = m // (nd * ns)
        shape = (hi, ns, rows, n)

    def kernel(ids_ref, left_ref, *refs):
        right_refs = refs[: len(rights)]
        out_refs = refs[len(rights) : len(rights) + lo]
        total = refs[-1]
        step = pl.program_id(0)
        at = 0
        for width, right_ref in zip(widths, right_refs):
            part = mm_tn(left_ref[...], right_ref[...])
            cols = slice(at, at + width)

            @pl.when(step == 0)
            def _():
                total[:, cols] = part

            @pl.when(step > 0)
            def _():
                total[:, cols] += part

            at += width

        @pl.when(step == count - 1)
        def _():
            s, z, y = ids_ref[0], ids_ref[1], ids_ref[2]
            for jy in range(lo):
                for jz in range(hi):
                    owner = (z ^ jz) * lo + (y ^ jy)
                    if kind == "row":
                        at = pl.multiple_of(owner * rows, rows)
                        out_refs[jy][jz] = total[pl.ds(at, rows), :].astype(BF)
                    else:
                        for js in range(ns):
                            at = pl.multiple_of(((s ^ js) * nd + owner) * rows, rows)
                            out_refs[jy][jz, js] = total[pl.ds(at, rows), :].astype(BF)

    return pl.pallas_call(
        kernel,
        out_shape=[jax.ShapeDtypeStruct(shape, BF)] * lo,
        grid_spec=pltpu.PrefetchScalarGridSpec(
            num_scalar_prefetch=1,
            grid=(count,),
            in_specs=[pl.BlockSpec((tile, m), lambda i, ids_ref: (i, 0))]
            + [pl.BlockSpec((tile, w), lambda i, ids_ref: (i, 0)) for w in widths],
            out_specs=[whole(shape)] * lo,
            scratch_shapes=[pltpu.VMEM((m, n), F32)],
        ),
        compiler_params=params_of(),
        cost_estimate=pl.CostEstimate(
            flops=2 * dims.seq * m * n,
            bytes_accessed=2 * (dims.seq * (m + n) + m * n),
            transcendentals=0,
        ),
        name=name,
    )(ids, left, *rights)


def cut_columns(dims, ids, qkv, up):
    ns, hw, ffw = dims.ns, dims.hw, dims.ffw
    rows = qkv.shape[0]

    def kernel(ids_ref, qkv_ref, up_ref, *outs):
        for js in range(ns):
            other = ids_ref[0] ^ js
            for part in range(3):
                at = pl.multiple_of(part * dims.width + other * hw, hw)
                outs[js][:, part * hw : (part + 1) * hw] = qkv_ref[:, pl.ds(at, hw)]
            at = pl.multiple_of(other * ffw, ffw)
            outs[js][:, 3 * hw :] = up_ref[:, pl.ds(at, ffw)]

    shape = (rows, 3 * hw + ffw)
    return pl.pallas_call(
        kernel,
        out_shape=[jax.ShapeDtypeStruct(shape, BF)] * ns,
        grid_spec=pltpu.PrefetchScalarGridSpec(
            num_scalar_prefetch=1,
            grid=(1,),
            in_specs=[whole(qkv.shape), whole(up.shape)],
            out_specs=[whole(shape)] * ns,
        ),
        compiler_params=params_of(),
        name="cut_columns",
    )(ids, qkv, up)


def join_columns(dims, ids, pieces, parts, width):
    ns = dims.ns
    rows, n = pieces[0].shape
    w = n // parts
    total = n * ns

    def kernel(ids_ref, *refs):
        out = refs[-1]
        for js in range(ns):
            other = ids_ref[0] ^ js
            for part in range(parts):
                at = pl.multiple_of(part * width + other * w, w)
                out[:, pl.ds(at, w)] = refs[js][:, part * w : (part + 1) * w].astype(F32)

    return pl.pallas_call(
        kernel,
        out_shape=jax.ShapeDtypeStruct((rows, total), F32),
        grid_spec=pltpu.PrefetchScalarGridSpec(
            num_scalar_prefetch=1,
            grid=(1,),
            in_specs=[whole((rows, n))] * ns,
            out_specs=whole((rows, total)),
        ),
        compiler_params=params_of(),
        name="join_columns",
    )(ids, *pieces)


def permute_plan(
    hidden_states,
    segment_ids,
    positions,
    out_grad,
    qkv_weight,
    qkv_bias,
    dense_weight,
    dense_bias,
    up_weight,
    up_bias,
    down_weight,
    down_bias,
    attn_gain,
    attn_shift,
    ffn_gain,
    ffn_shift,
):
    ns, nd = lax.axis_size("seq"), lax.axis_size("dp")
    tokens, width = hidden_states.shape[1:]
    dims = Dims(ns, nd, tokens, width, up_weight.shape[1])
    hi, lo, nx = dims.hi, dims.lo, dims.nx
    hw, ffw, seq = dims.hw, dims.ffw, dims.seq
    s, d = lax.axis_index("seq"), lax.axis_index("dp")
    z, y = d // lo, d % lo
    ids = jnp.stack([s, z, y, s]).astype(jnp.int32)

    def by_seq(value, mask):
        return xor_swap(value, "seq", ns, mask)

    def by_dp(value, mask):
        return xor_swap(value, "dp", nd, mask)

    hidden, grad_out = hidden_states[0], out_grad[0]

    fields = (qkv_bias, dense_bias, up_bias, down_bias, attn_gain, attn_shift, ffn_gain, ffn_shift)
    mine = jnp.concatenate(fields)
    index = s * nd + d
    small = jnp.where(jnp.arange(ns * nd)[:, None] == index, mine[None, :], jnp.zeros((), BF))
    mask = 1
    while mask < ns:
        small = small + by_seq(small, mask)
        mask *= 2
    mask = 1
    while mask < nd:
        small = small + by_dp(small, mask)
        mask *= 2
    full, at = [], 0
    for field in fields:
        n = field.shape[0]
        full.append(small[:, at : at + n].reshape(-1).astype(F32))
        at += n
    b_qkv, b_dense, b_up, b_down, g_attn, s_attn, g_ffn, s_ffn = full
    affine = jnp.concatenate(
        [jnp.stack([g_attn, s_attn, g_ffn, s_ffn]), jnp.zeros((4, width), F32)], axis=0
    )
    bias_qkv = lax.dynamic_index_in_dim(
        b_qkv.reshape(3, ns, hw), s, 1, keepdims=False
    ).reshape(1, 3 * hw)
    bias_up = lax.dynamic_slice_in_dim(b_up, s * ffw, ffw).reshape(1, ffw)

    meta = jnp.stack([segment_ids[0], positions[0]])
    metas = [meta] + [by_seq(meta, js) for js in range(1, ns)]
    meta_all = jnp.concatenate(metas, axis=1)
    starts = [jnp.sum((meta_all[0] < v).astype(jnp.int32)) for v in range(1, DOCS)]
    doc_ids = jnp.stack([s.astype(jnp.int32)] + starts)
    half = ROT // 2
    freqs = rotary_base ** (-2.0 * jnp.arange(half, dtype=F32) / ROT)
    angles = meta_all[1].astype(F32)[None, :] * freqs[:, None]
    table = 2 * HEAD
    pick = np.zeros((half, table), np.float32)
    signed = np.zeros((half, table), np.float32)
    rest = np.ones((1, table), np.float32)
    for lane in range(table):
        if lane % HEAD < ROT:
            pick[lane % HEAD % half, lane] = 1.0
            signed[lane % HEAD % half, lane] = -1.0 if lane % HEAD < half else 1.0
            rest[0, lane] = 0.0
    exact = lax.Precision.HIGHEST
    cos_table = lax.dot_general(jnp.cos(angles), jnp.asarray(pick), TN, precision=exact) + rest
    sin_table = lax.dot_general(jnp.sin(angles), jnp.asarray(signed), TN, precision=exact)

    def gather_tokens(value):
        found = [value, by_seq(value, 1)]
        for m in range(1, nx):
            across = by_seq(value, 2 * m)
            found += [across, by_seq(across, 1)]
        return found

    blocks = gather_tokens(hidden)

    cuts = cut_columns(dims, ids, qkv_weight, up_weight)
    got = [cuts[0]] + [by_seq(cuts[js], js) for js in range(1, ns)]
    stacked = jnp.stack(got)

    def gather_dp(shard):
        pieces = []
        for jz in range(hi):
            here = shard if jz == 0 else by_dp(shard, jz * lo)
            pieces += [here] + [by_dp(here, jy) for jy in range(1, lo)]
        return pieces

    up_pieces = gather_dp(stacked[:, :, 3 * hw :])
    qkv_pieces = gather_dp(stacked[:, :, : 3 * hw])
    dense_pieces = gather_dp(dense_weight)
    down_pieces = gather_dp(down_weight)
    qkv_w = ("col", qkv_pieces, (width, 3 * hw))
    up_w = ("col", up_pieces, (width, ffw))
    dense_w = ("row", dense_pieces, (hw, width))
    down_w = ("row", down_pieces, (ffw, width))

    carried = ()
    for m in range(nx):
        carried = norm_pair(dims, m, blocks[2 * m], blocks[2 * m + 1], affine, carried)
    attn_low, ffn_low, hat_low = carried

    tile = 256
    act, slope = token_call(
        dims, "up", ids, up_body, [ffn_low], [up_w], [bias_up],
        [tiled_out(seq, ffw, tile)] * 2, tile, 2 * seq * width * ffw * 2,
    )
    flip = (
        jax.ShapeDtypeStruct((hw, seq), BF),
        pl.BlockSpec((hw, tile), lambda i, ids_ref: (0, i)),
    )
    queries, keys, values, keys_t, values_t = token_call(
        dims, "qkv", ids, functools.partial(qkv_body, dims), [attn_low, cos_table, sin_table],
        [qkv_w], [bias_qkv], [tiled_out(seq, hw, tile)] * 3 + [flip] * 2, tile,
        2 * seq * width * 3 * hw,
    )
    grads_all = jnp.concatenate(gather_tokens(grad_out), axis=0)
    grad_mix = token_call(
        dims, "mix_grad", ids, mix_grad_body, [grads_all], [dense_w], [],
        [tiled_out(seq, hw, tile)], tile, 2 * seq * width * hw,
    )[0]
    mixed, gq, gk, gv, qkv_sums = attention(
        dims, doc_ids, queries, keys, values, keys_t, values_t, grad_mix, cos_table, sin_table
    )

    def reduce_tokens(others, own):
        got = by_seq(others, 1)
        total = own[0].astype(F32) + got[0].astype(F32)
        for m in range(1, nx):
            total = total + by_seq(own[m] + got[m], 2 * m).astype(F32)
        return total

    def reduce_dp(parts):
        got = [by_dp(parts[jy], jy) for jy in range(1, lo)]

        def slab(jz):
            value = parts[0][jz].astype(F32)
            for g in got:
                value = value + g[jz].astype(F32)
            return value

        total = slab(0)
        for jz in range(1, hi):
            total = total + by_dp(slab(jz).astype(BF), jz * lo).astype(F32)
        return total

    def columns_home(total, parts):
        low = total.astype(BF)
        pieces = [low[0]] + [by_seq(low[js], js) for js in range(1, ns)]
        return join_columns(dims, ids, pieces, parts, width)

    down_parts = weight_grad(dims, "down_grad", "row", ids, act, [grads_all])
    grad_down = reduce_dp(down_parts)
    dense_parts = weight_grad(dims, "dense_grad", "row", ids, mixed, [grads_all])
    grad_dense = reduce_dp(dense_parts)
    qkv_parts = weight_grad(dims, "qkv_grad", "col", ids, attn_low, [gq, gk, gv])
    grad_qkv = columns_home(reduce_dp(qkv_parts), 3)

    sums_shape = lambda n: (jax.ShapeDtypeStruct((8, n), F32), whole((8, n)))
    grad_up_low, up_sums = token_call(
        dims, "up_grad", ids, up_grad_body, [grads_all, slope], [down_w], [],
        [tiled_out(seq, ffw, tile), sums_shape(ffw)], tile, 2 * seq * width * ffw,
    )
    up_parts = weight_grad(dims, "up_w_grad", "col", ids, ffn_low, [grad_up_low])
    grad_up = columns_home(reduce_dp(up_parts), 1)

    outs, per = split_specs(dims, tile)
    others, own = token_call(
        dims, "out", ids, functools.partial(out_body, per), [mixed, act], [dense_w, down_w], [],
        outs, tile, 2 * seq * width * (hw + ffw),
    )
    out_total = reduce_tokens(others, own)
    output = (hidden.astype(F32) + out_total + (b_dense + b_down)[None, :]).astype(BF)

    others, own, gain_sums = token_call(
        dims, "in_grad", ids, functools.partial(in_grad_body, per, hw),
        [grad_up_low, gq, gk, gv, hat_low], [qkv_w, up_w], [affine],
        outs + [sums_shape(width)], tile, 2 * seq * width * (3 * hw + ffw),
    )
    gx = reduce_tokens(others, own)
    rows = hidden.astype(F32)
    spread = rows - jnp.mean(rows, axis=-1, keepdims=True)
    inv_std = lax.rsqrt(jnp.mean(spread * spread, axis=-1, keepdims=True) + epsilon)
    hat = spread * inv_std
    back = inv_std * (
        gx
        - jnp.mean(gx, axis=-1, keepdims=True)
        - hat * jnp.mean(gx * hat, axis=-1, keepdims=True)
    )
    grad_out_f = grad_out.astype(F32)
    input_grad = (grad_out_f + back).astype(BF)

    def placed(value, parts, w):
        base = jnp.zeros((parts, ns, w), F32)
        return lax.dynamic_update_slice_in_dim(base, value.reshape(parts, 1, w), s, 1).reshape(-1)

    out_sum = jnp.sum(grad_out_f, axis=0)
    vectors = (
        placed(qkv_sums[:3], 3, hw),
        out_sum,
        placed(up_sums[0], 1, ffw),
        gain_sums[0],
        gain_sums[1],
        gain_sums[2],
        gain_sums[3],
    )
    packed = jnp.concatenate(vectors).reshape(-1, 128)
    mask = 1
    while mask < ns:
        packed = packed + by_seq(packed, mask)
        mask *= 2
    mask = 1
    while mask < nd:
        packed = packed + by_dp(packed, mask)
        mask *= 2
    flat = packed.reshape(-1)
    small_out, at = [], 0
    for vector in vectors:
        n = vector.shape[0]
        share = n // (ns * nd)
        small_out.append(lax.dynamic_slice_in_dim(flat, at + index * share, share))
        at += n
    gb_qkv, gb_out, gb_up, gg_attn, gs_attn, gg_ffn, gs_ffn = small_out
    return (
        output[None],
        input_grad[None],
        grad_qkv,
        gb_qkv,
        grad_dense,
        gb_out,
        grad_up,
        gb_up,
        grad_down,
        gb_out,
        gg_attn,
        gs_attn,
        gg_ffn,
        gs_ffn,
    )


class Bag(dict):
    __getattr__ = dict.__getitem__


class Net:
    def __init__(self, send, recv):
        self.send_sems, self.recv_sems, self.copies, self.count = send, recv, [], 0

    def make(self, source, target, **peer):
        at = self.count
        self.count += 1
        copy = pltpu.make_async_remote_copy(
            src_ref=source,
            dst_ref=target,
            send_sem=self.send_sems.at[at],
            recv_sem=self.recv_sems.at[at],
            device_id=peer,
            device_id_type=pl.DeviceIdType.MESH,
        )
        self.copies.append(copy)
        return copy

    def send(self, source, target, **peer):
        copy = self.make(source, target, **peer)
        copy.start()
        return copy

    def release(self, copies):
        for copy in copies:
            copy.wait_send()
        self.copies = [c for c in self.copies if all(c is not copy for copy in copies)]

    def finish(self):
        for copy in self.copies:
            copy.wait_send()


class Local:
    def __init__(self, sems):
        self.sems, self.copies, self.done = sems, [], 0

    def make(self, source, target):
        copy = pltpu.make_async_copy(source, target, self.sems.at[self.done + len(self.copies)])
        self.copies.append(copy)
        return copy

    def copy(self, source, target):
        copy = self.make(source, target)
        copy.start()
        return copy

    def load(self, source, target):
        copy = pltpu.make_async_copy(source, target, self.sems.at[self.done + len(self.copies)])
        copy.start()
        self.done += 1
        return copy

    def finish(self):
        for copy in self.copies:
            copy.wait()


def greet(peers):
    barrier = pltpu.get_barrier_semaphore()
    for peer in peers:
        pl.semaphore_signal(
            barrier, inc=1, device_id=peer, device_id_type=pl.DeviceIdType.MESH
        )
    pl.semaphore_wait(barrier, len(peers))


def neighbours(dims, s, d):
    return (
        [{"seq": s ^ js} for js in range(1, dims.ns)]
        + [{"dp": d ^ (jz * dims.lo)} for jz in range(1, dims.hi)]
        + [{"dp": d ^ jy} for jy in range(1, dims.lo)]
    )


def table_constants():
    half = ROT // 2
    table = 2 * HEAD
    constants = np.zeros((24, table), np.float32)
    for lane in range(table):
        if lane % HEAD < ROT:
            constants[lane % HEAD % half, lane] = 1.0
            constants[half + lane % HEAD % half, lane] = -1.0 if lane % HEAD < half else 1.0
        else:
            constants[2 * half, lane] = 1.0
    return constants


def rotary_tables(rows, const_ref, width):
    half = ROT // 2
    exact = lax.Precision.HIGHEST
    cosine = lax.dot_general(
        rows[0:half, :], const_ref[0:half, :], TN, precision=exact, preferred_element_type=F32
    ) + const_ref[2 * half : 2 * half + 1, :]
    sine = lax.dot_general(
        rows[half : 2 * half, :], const_ref[half : 2 * half, :], TN, precision=exact,
        preferred_element_type=F32,
    )
    return spread_lanes(cosine, width), spread_lanes(sine, width)


def gather_kernel(dims, hidden, grad_out, meta, small, qkv, up, dense):
    ns, nd, hi, lo, nx = dims.ns, dims.nd, dims.hi, dims.lo, dims.nx
    tokens, width, hw, ffw, seq = dims.tokens, dims.width, dims.hw, dims.ffw, dims.seq
    share, dense_share = qkv.shape[0], dense.shape[0]
    n_net, n_local = 128, 64

    def kernel(
        hid, gout, meta_ref, small_ref, qkv_ref, up_ref, dense_ref, const_ref,
        attn_out, ffn_out, hat_out, g_out, act_out, slope_out, q_out, k_out, v_out, kt_out,
        vt_out, mix_out, qkv_out, up_out, dense_out, meta_out, affine_out,
        h_buf, g_buf, attn_buf, ffn_buf, hat_buf, act_buf, slope_buf, q_buf, k_buf, v_buf,
        kt_buf, vt_buf, mix_buf, w_qkv, w_up, w_dense, meta_buf, affine, vectors, bias_rows,
        send_sems, recv_sems, local_sems,
    ):
        s, d = lax.axis_index("seq"), lax.axis_index("dp")
        z, y = d // lo, d % lo
        net, local = Net(send_sems, recv_sems), Local(local_sems)
        h_own = local.load(hid, h_buf.at[0:tokens])
        greet(neighbours(dims, s, d))

        def block(ref, j):
            return ref.at[j * tokens : (j + 1) * tokens]

        def along_z(weight):
            return [net.send(weight(d), weight(d), dp=d ^ (jz * lo)) for jz in range(1, hi)]

        def along_y(weight, jz):
            at = (z ^ jz) * lo + y
            return [net.send(weight(at), weight(at), dp=d ^ jy) for jy in range(1, lo)]

        def forward_y(arrivals, weight):
            sent = []
            for jz, done in enumerate(arrivals, 1):
                done.wait_recv()
                sent += along_y(weight, jz)
            return sent

        def to_columns(js, name):
            other = s ^ js
            if name == "up":
                at = pl.multiple_of(other * ffw, ffw)
                pairs = [(up_ref.at[:, pl.ds(at, ffw)], w_up.at[s, d])]
            else:
                pairs = []
                for part in range(3):
                    at = pl.multiple_of(part * width + other * hw, hw)
                    pairs.append(
                        (
                            qkv_ref.at[:, pl.ds(at, hw)],
                            w_qkv.at[s, d, :, part * hw : (part + 1) * hw],
                        )
                    )
            if js == 0:
                return [local.load(a, b) for a, b in pairs]
            return [net.send(a, b, seq=other) for a, b in pairs]

        tiny = [net.send(small_ref, vectors.at[s, d], seq=s ^ js) for js in range(1, ns)]
        vectors[s, d] = small_ref[...]
        cuts = Bag()
        for name in ("up", "qkv"):
            cuts[name] = [to_columns(js, name) for js in range(ns)]
        metas = [net.send(meta_ref, meta_buf.at[js], seq=s ^ js) for js in range(1, ns)]
        meta_buf[0] = meta_ref[...]
        h_core = net.send(hid, block(h_buf, 1), seq=s ^ 1)
        h_cross = [net.send(hid, block(h_buf, 2 * m), seq=s ^ (2 * m)) for m in range(1, nx)]
        g_core = net.send(gout, block(g_buf, 1), seq=s ^ 1)
        g_cross = [net.send(gout, block(g_buf, 2 * m), seq=s ^ (2 * m)) for m in range(1, nx)]
        g_own = local.load(gout, block(g_buf, 0))
        dense_own = local.load(dense_ref, w_dense.at[d])

        first, second = slice(0, ns // 2), slice(ns // 2, ns)
        part_qkv = [lambda at: w_qkv.at[first, at], lambda at: w_qkv.at[second, at]]
        part_up = [lambda at: w_up.at[first, at], lambda at: w_up.at[second, at]]
        part_dense = lambda at: w_dense.at[at]
        part_tiny = lambda at: vectors.at[:, at]

        for done in tiny:
            done.wait_recv()
        z_tiny = along_z(part_tiny)
        y_tiny = along_y(part_tiny, 0)

        def spread_weight(name, halves):
            for done in cuts[name][0]:
                done.wait()
            for group in cuts[name][1:]:
                for done in group:
                    done.wait_recv()
            return [along_z(half) for half in halves], [along_y(half, 0) for half in halves]

        z_up, y_up = spread_weight("up", part_up)
        y_tiny += forward_y(z_tiny, part_tiny)
        z_qkv, y_qkv = spread_weight("qkv", part_qkv)
        dense_own.wait()
        z_dense, y_dense = along_z(part_dense), along_y(part_dense, 0)

        for done in y_tiny:
            done.wait_recv()
        n = width // (ns * nd)
        per_row = 128 // n
        for row in range(width // 128):
            total = None
            for q in range(per_row):
                owner = row * per_row + q
                tile = vectors[owner // nd, owner % nd]
                tile = pltpu.roll(tile, q * n, 1) if q else tile
                total = tile if total is None else total + tile
            lanes = slice(row * 128, (row + 1) * 128)
            affine[0:4, lanes] = total[4:8, :]
            affine[4:5, lanes] = total[1:2, :] + total[3:4, :]
        lane = lax.broadcasted_iota(jnp.int32, (1, 128), 1)
        n = 3 * n
        bias_rows[...] = jnp.zeros_like(bias_rows)
        for owner in range(ns * nd):
            start, row = owner * n % 128, owner * n // 128
            tile = vectors[owner // nd, owner % nd]
            tile = (pltpu.roll(tile, start, 1) if start else tile)[0:1, :]
            bias_rows[row : row + 1, :] += jnp.where(lane >= start, tile, 0.0)
            if start + n > 128:
                bias_rows[row + 1 : row + 2, :] += jnp.where(lane < start, tile, 0.0)
        local.copy(affine, affine_out)
        tile = 256

        def norm(first, last):
            def body(t, carry):
                rows = pl.ds(pl.multiple_of(t * tile, tile), tile)
                x = h_buf[rows, :].astype(F32)
                spread = x - jnp.mean(x, axis=-1, keepdims=True)
                hat = spread * lax.rsqrt(
                    jnp.mean(spread * spread, axis=-1, keepdims=True) + epsilon
                )
                attn_buf[rows, :] = (hat * affine[0:1, :] + affine[1:2, :]).astype(BF)
                ffn_buf[rows, :] = (hat * affine[2:3, :] + affine[3:4, :]).astype(BF)
                hat_buf[rows, :] = hat.astype(BF)
                return carry

            per = tokens // tile
            lax.fori_loop(first * per, last * per, body, 0)
            here = slice(first * tokens, last * tokens)
            for source, target in ((attn_buf, attn_out), (ffn_buf, ffn_out), (hat_buf, hat_out)):
                local.copy(source.at[here], target.at[here])

        h_own.wait()
        h_core.wait_recv()
        norm(0, 2)
        y_up.append(forward_y(z_up[0], part_up[0]))
        y_up.append(forward_y(z_up[1], part_up[1]))
        h_far = []
        for m, done in enumerate(h_cross, 1):
            done.wait_recv()
            h_far.append(
                net.send(block(h_buf, 2 * m), block(h_buf, 2 * m + 1), seq=s ^ 1)
            )
        for done in h_far:
            done.wait_recv()
        norm(2, ns)
        y_qkv.append(forward_y(z_qkv[0], part_qkv[0]))

        for group in y_up:
            for done in group:
                done.wait_recv()
        bias_up = jnp.concatenate(
            [
                vectors[(s * (ffw // 128) + c) // nd, (s * (ffw // 128) + c) % nd, 2:3, :]
                for c in range(ffw // 128)
            ],
            axis=1,
        )

        def up_rows(first, last):
            def body(t, carry):
                rows = pl.ds(pl.multiple_of(t * tile, tile), tile)
                pre = mm(ffn_buf[rows, :], w_up[...].reshape(width, ffw)) + bias_up
                total = 0.5 + 0.5 * lax.erf(pre * math.sqrt(0.5))
                density = jnp.exp(-0.5 * pre * pre) * (1.0 / math.sqrt(2.0 * math.pi))
                act_buf[rows, :] = (pre * total).astype(BF)
                slope_buf[rows, :] = (total + pre * density).astype(BF)
                return carry

            per = tokens // tile
            lax.fori_loop(first * per, last * per, body, 0)
            here = slice(first * tokens, last * tokens)
            for source, target in ((act_buf, act_out), (slope_buf, slope_out)):
                local.copy(source.at[here], target.at[here])

        up_rows(0, ns // 2)
        y_qkv.append(forward_y(z_qkv[1], part_qkv[1]))
        up_rows(ns // 2, ns)
        local.copy(w_up, up_out)
        y_dense += forward_y(z_dense, part_dense)

        g_far = []
        for m, done in enumerate(g_cross, 1):
            done.wait_recv()
            g_far.append(
                net.send(block(g_buf, 2 * m), block(g_buf, 2 * m + 1), seq=s ^ 1)
            )
        for group in y_qkv:
            for done in group:
                done.wait_recv()
        for done in metas:
            done.wait_recv()
        parts = hw // 128
        bias_qkv = jnp.concatenate(
            [
                bias_rows[pl.ds(part * (width // 128) + s * parts + k, 1), :]
                for part in range(3)
                for k in range(parts)
            ],
            axis=1,
        )

        def qkv_block(j, carry):
            rows = pl.ds(pl.multiple_of(j * tokens, tokens), tokens)
            cosine, sine = rotary_tables(meta_buf[j], const_ref, hw)
            joined = mm(attn_buf[rows, :], w_qkv[...].reshape(width, 3 * hw)) + bias_qkv
            queries = turn(joined[:, :hw], cosine, sine, 1.0)
            keys = turn(joined[:, hw : 2 * hw], cosine, sine, 1.0)
            values = joined[:, 2 * hw :]
            q_buf[rows, :] = queries.astype(BF) * (1.0 / math.sqrt(HEAD))
            k_buf[rows, :] = keys.astype(BF)
            v_buf[rows, :] = values.astype(BF)
            kt_buf[:, rows] = keys.T.astype(BF)
            vt_buf[:, rows] = values.T.astype(BF)
            return carry

        lax.fori_loop(0, ns, qkv_block, 0)
        for source, target in (
            (q_buf, q_out), (k_buf, k_out), (v_buf, v_out), (kt_buf, kt_out), (vt_buf, vt_out),
            (w_qkv, qkv_out), (meta_buf, meta_out),
        ):
            local.copy(source, target)

        for done in y_dense + [g_core]:
            done.wait_recv()
        g_own.wait()

        def mix_block(j, carry):
            rows = pl.ds(pl.multiple_of(j * tokens, tokens), tokens)
            mix_buf[rows, :] = mm_nt(g_buf[rows, :], w_dense[...].reshape(hw, width)).astype(BF)
            return carry

        for done in g_far:
            done.wait_recv()
        lax.fori_loop(0, ns, mix_block, 0)
        for source, target in ((mix_buf, mix_out), (g_buf, g_out), (w_dense, dense_out)):
            local.copy(source, target)
        local.finish()
        net.finish()

    sds = jax.ShapeDtypeStruct
    any_spec = pl.BlockSpec(memory_space=pl.ANY)
    vmem_spec = pl.BlockSpec(memory_space=pltpu.VMEM)
    const = jnp.asarray(table_constants())
    out_shapes = (
        [sds((seq, width), BF)] * 4
        + [sds((seq, ffw), BF)] * 2
        + [sds((seq, hw), BF)] * 3
        + [sds((hw, seq), BF)] * 2
        + [sds((seq, hw), BF)]
        + [
            sds((ns, nd, share, 3 * hw), BF),
            sds((ns, nd, share, ffw), BF),
            sds((nd, dense_share, width), BF),
            sds((ns,) + meta.shape, F32),
            sds((8, width), F32),
        ]
    )
    scratch = [
        pltpu.VMEM(x.shape, x.dtype)
        for x in [sds((seq, width), BF)] * 5 + out_shapes[4:]
    ] + [
        pltpu.VMEM((ns, nd) + small.shape, F32),
        pltpu.VMEM((3 * width // 128 + 8, 128), F32),
        pltpu.SemaphoreType.DMA((n_net,)),
        pltpu.SemaphoreType.DMA((n_net,)),
        pltpu.SemaphoreType.DMA((n_local,)),
    ]
    return pl.pallas_call(
        kernel,
        out_shape=out_shapes,
        in_specs=[any_spec] * 2 + [vmem_spec] * 2 + [any_spec] * 3 + [vmem_spec],
        out_specs=[any_spec] * len(out_shapes),
        scratch_shapes=scratch,
        compiler_params=pltpu.CompilerParams(
            vmem_limit_bytes=VMEM_LIMIT, collective_id=1, has_side_effects=True
        ),
        name="gather",
    )(hidden, grad_out, meta, small, qkv, up, dense, const)


class Spread:
    def __init__(self, dims, net, where, groups, rows, total, base, cols, steps, bufs):
        self.steps = steps
        self.dims, self.net, self.where, self.groups, self.rows = dims, net, where, groups, rows
        self.total, self.base, self.cols = total, base, cols
        self.send_y, self.recv_y, self.send_z, self.recv_z = bufs

    def part(self, group, owner):
        unit = group * self.steps[0] + owner * self.steps[1]
        at = pl.multiple_of(self.base + unit * self.rows, self.rows)
        return self.total[pl.ds(at, self.rows), self.cols]

    def start(self):
        s, d, z, y = self.where
        dims = self.dims
        self.along_y = []
        for jy in range(1, dims.lo):
            for zz in range(dims.hi):
                for g in range(self.groups):
                    self.send_y[jy - 1, zz, g] = self.part(g, zz * dims.lo + (y ^ jy)).astype(BF)
            self.along_y.append(
                self.net.send(self.send_y.at[jy - 1], self.recv_y.at[jy - 1], dp=d ^ jy)
            )

    def summed(self, zz, g):
        s, d, z, y = self.where
        value = self.part(g, zz * self.dims.lo + y)
        for jy in range(1, self.dims.lo):
            value = value + self.recv_y[jy - 1, zz, g].astype(F32)
        return value

    def middle(self):
        s, d, z, y = self.where
        for copy in self.along_y:
            copy.wait_recv()
        self.along_z = []
        for jz in range(1, self.dims.hi):
            for g in range(self.groups):
                self.send_z[jz - 1, g] = self.summed(z ^ jz, g).astype(BF)
            self.along_z.append(
                self.net.send(
                    self.send_z.at[jz - 1], self.recv_z.at[jz - 1], dp=d ^ (jz * self.dims.lo)
                )
            )

    def own(self, g):
        s, d, z, y = self.where
        return self.summed(z, g)

    def arrive(self):
        for copy in self.along_z:
            copy.wait_recv()

    def final(self, g):
        value = self.own(g)
        for jz in range(1, self.dims.hi):
            value = value + self.recv_z[jz - 1, g].astype(F32)
        return value


class Stream:
    def __init__(self, slots, sems):
        self.slots, self.sems = slots, sems

    def copies(self, t, slot):
        found = []
        for k, array in enumerate(self.arrays):
            rows = pl.ds(pl.multiple_of(self.index(t) * self.size, self.size), self.size)
            found.append(
                pltpu.make_async_copy(
                    array.at[rows], self.slots.at[k, slot, 0 : self.size], self.sems.at[k, slot]
                )
            )
        return found

    def ask(self, arrays, size, index=lambda t: t):
        self.arrays, self.size, self.index = arrays, size, index
        for copy in self.copies(0, 0):
            copy.start()

    def run(self, count, body):
        def step(t, carry):
            slot = t % 2

            @pl.when(t + 1 < count)
            def _():
                for copy in self.copies(t + 1, 1 - slot):
                    copy.start()

            for copy in self.copies(t, slot):
                copy.wait()
            body(t, *[self.slots.at[k, slot, 0 : self.size] for k in range(len(self.arrays))])
            return carry

        lax.fori_loop(0, count, step, 0)


def main_kernel(dims, arrays, down):
    ns, nd, hi, lo, nx = dims.ns, dims.nd, dims.hi, dims.lo, dims.nx
    tokens, width, hw, ffw, seq = dims.tokens, dims.width, dims.hw, dims.ffw, dims.seq
    heads = dims.heads
    tile = 256
    per = tokens // tile
    blocks = seq // tile
    window = seq // 2 // tile
    wide = heads * tile
    r_col, r_dense, r_down = width // (ns * nd), hw // nd, ffw // nd
    half_d, half_f = width // 2, ffw // 2
    pieces = r_down // r_col
    plans = Bag(
        down0=(pieces, r_col, half_d, True), down1=(pieces, r_col, half_d, True),
        up0=(ns, r_col, half_f, False), up1=(ns, r_col, half_f, False),
        q=(ns, r_col, hw, False), k=(ns, r_col, hw, False), v=(ns, r_col, hw, False),
        dense=(1, r_dense, width, True),
    )
    columns = [n for n in plans if not plans[n][3]]
    rows_kind = [n for n in plans if plans[n][3]]
    shared = Bag(up0="down0", up1="down1")
    n_net, n_local = 128, 48
    in_names = (
        "queries", "keys", "values", "keys_t", "values_t", "grad_mix", "attn", "ffn", "hat",
        "act", "slope", "grads", "w_qkv", "w_up", "w_dense",
    )
    sds = jax.ShapeDtypeStruct
    cut = (ns, tokens, hw)
    outs = Bag(
        home_out=sds(cut, BF), home_in=sds(cut, BF),
        far_out=sds((nx - 1,) + cut, BF), far_in=sds((nx - 1,) + cut, BF),
        grad_up_low=sds((seq, ffw), BF),
        own_sums=sds((8, 128), F32), swap_sums=sds((ns - 1, 8, 128), F32),
    )
    for name in rows_kind:
        groups, rows, n, _ = plans[name]
        outs["own_" + name] = sds((groups, rows, n), F32)
        outs["z_" + name] = sds((hi - 1, groups, rows, n), BF)
    for name in columns:
        groups, rows, n, _ = plans[name]
        outs["own_" + name] = sds((rows, n), F32)
        outs["swap_" + name] = sds((ns - 1, rows, n), BF)
    scratch = Bag(
        w_qkv=sds((width, 3 * hw), BF), w_up=sds((width, ffw), BF),
        w_dense=sds((hw, width), BF), w_down=sds((nd, r_down, width), BF),
        acc=sds((ffw, width), F32), acc_k=sds((seq, hw), F32), acc_v=sds((seq, hw), F32),
        pool=sds((4, seq, hw), BF),
        keys_t=sds((hw, seq), BF), values_t=sds((hw, seq), BF),
        scores=sds(((window + 1) * tile, wide), F32),
        probs=sds(((window + 1) * tile, wide), BF),
        mixed=sds((seq, hw), BF), gq=sds((seq, hw), BF), gk=sds((seq, hw), BF),
        gv=sds((seq, hw), BF),
        got_out=sds((nx, seq, hw), BF), got_in=sds((nx, seq, hw), BF),
        out_parts=sds((2 * nx, seq, hw), BF),
        stream=sds((2, 2, tokens, width), BF),
        qkv_sum=sds((8, hw), F32), up_sum=sds((8, ffw), F32), gain_sum=sds((8, width), F32),
        sum_rows=sds((3 * width // 128 + 8, 128), F32),
        tiles=sds((ns, hi, lo, 8, 128), F32),
        tiles_y=sds((lo - 1, ns, hi, 8, 128), F32), tiles_z=sds((ns, hi, 8, 128), F32),
        tiles_zr=sds((hi - 1, ns, 8, 128), F32), tiles_s=sds((ns, 8, 128), F32),
    )
    for name, (groups, rows, n, landed) in plans.items():
        if name not in shared:
            scratch["sy_" + name] = sds((lo - 1, hi, groups, rows, n), BF)
            scratch["sz_" + name] = sds((hi - 1, groups, rows, n), BF)
        scratch["ry_" + name] = sds((lo - 1, hi, groups, rows, n), BF)
        if not landed:
            scratch["rz_" + name] = sds((hi - 1, groups, rows, n), BF)
            scratch["sw_" + name] = sds((ns - 1, rows, n), BF)
        scratch["ob_" + name] = sds((groups, rows, n) if landed else (rows, n), F32)

    def kernel(*all_refs):
        refs = list(all_refs)
        take = lambda names: Bag((name, refs.pop(0)) for name in names)
        hbm = take(in_names)
        down_ref, meta_ref, affine, const_ref = [refs.pop(0) for _ in range(4)]
        out = take(outs)
        vm = take(scratch)
        send_sems, recv_sems, local_sems, stream_sems = refs
        stream = Stream(vm.stream, stream_sems)
        stream.ask([hbm.act, hbm.grads], tokens)
        s, d = lax.axis_index("seq"), lax.axis_index("dp")
        z, y = d // lo, d % lo
        where = (s, d, z, y)
        net, local = Net(send_sems, recv_sems), Local(local_sems)
        loads = Bag()
        for at, name in enumerate(("queries", "keys", "values", "grad_mix")):
            loads[name] = local.load(hbm[name], vm.pool.at[at])
        for name in ("keys_t", "values_t", "w_dense", "w_qkv", "w_up"):
            loads[name] = local.load(hbm[name], vm[name])
        q_ref, k_ref, v_ref, g_ref = [vm.pool.at[at] for at in range(4)]
        greet(neighbours(dims, s, d))

        part_down = lambda at: vm.w_down.at[at]
        down_own = local.load(down_ref, part_down(d))
        z_down = [
            net.send(down_ref, part_down(d), dp=d ^ (jz * lo)) for jz in range(1, hi)
        ]
        y_down = [net.send(down_ref, part_down(d), dp=d ^ jy) for jy in range(1, lo)]

        totals = Bag(
            down0=("acc", 0, slice(0, half_d)), down1=("acc", 0, slice(half_d, width)),
            up0=("acc", 0, slice(0, half_f)), up1=("acc", 0, slice(half_f, ffw)),
            q=("scores", 0, slice(0, hw)), k=("scores", 0, slice(hw, 2 * hw)),
            v=("scores", 0, slice(2 * hw, 3 * hw)), dense=("scores", width, slice(0, width)),
        )
        sets = Bag()
        for name, (groups, rows, n, landed) in plans.items():
            total, base, cols = totals[name]
            source = shared.get(name, name)
            steps = (1, groups) if landed else (nd, 1)
            bufs = (
                vm["sy_" + source], vm["ry_" + name], vm["sz_" + source],
                out["z_" + name] if landed else vm["rz_" + name],
            )
            sets[name] = Spread(
                dims, net, where, groups, rows, vm[total], base, cols, steps, bufs
            )

        def rows_of_step(t, size):
            return pl.ds(pl.multiple_of(t * size, size), size)

        def finish_rows(name):
            for g in range(sets[name].groups):
                vm["ob_" + name][g] = sets[name].own(g)
            local.copy(vm["ob_" + name], out["own_" + name])

        chunk = 256

        def add_products(t, left, right):
            for m in range(0, ffw, chunk):
                vm.acc[m : m + chunk, :] += mm_tn(left[:, m : m + chunk], right[...])

        vm.acc[...] = jnp.zeros_like(vm.acc)
        stream.run(ns, add_products)
        stream.ask([hbm.grads, hbm.slope], tile)
        sets.down0.start()

        lane = lax.broadcasted_iota(jnp.int32, (1, hw), 1)
        segments = jnp.concatenate([meta_ref[j, 16:24, :] for j in range(ns)], axis=1)
        edges = [
            jnp.sum((segments[0:1, :] < float(v)).astype(F32), axis=1, keepdims=True).astype(
                jnp.int32
            )
            for v in range(1, DOCS)
        ]

        def by_head(value):
            zero = jnp.zeros_like(value)
            return jnp.concatenate(
                [jnp.where(lane // HEAD == h, value, zero) for h in range(heads)], axis=0
            )

        def rows_at(block):
            at = ((block // per) ^ s) * per + block % per
            return pl.ds(pl.multiple_of(at * tile, tile), tile)

        for name in ("queries", "keys", "values", "grad_mix", "keys_t", "values_t"):
            loads[name].wait()
        vm.acc_k[...] = jnp.zeros_like(vm.acc_k)
        vm.acc_v[...] = jnp.zeros_like(vm.acc_v)
        vm.qkv_sum[...] = jnp.zeros_like(vm.qkv_sum)
        cols = [slice(h * tile, (h + 1) * tile) for h in range(heads)]
        lanes_of = [slice(h * HEAD, (h + 1) * HEAD) for h in range(heads)]
        scale = 1.0 / math.sqrt(HEAD)

        def attend(block, carry_in):
            here = rows_at(block)
            q_stack = by_head(q_ref[here, :])
            q_pos = block * tile + lax.broadcasted_iota(jnp.int32, (1, wide), 1) % tile
            begin = jnp.zeros((1, wide), jnp.int32)
            for edge in edges:
                begin = jnp.where(q_pos >= edge, jnp.maximum(begin, edge), begin)
            low = jnp.maximum(block - window, 0)
            key_row = lax.broadcasted_iota(jnp.int32, (tile, wide), 0)

            def slot(key_block):
                return pl.ds(pl.multiple_of((key_block - low) * tile, tile), tile)

            def score_pass(key_block, high):
                allowed = key_row >= begin - key_block * tile
                scores = jnp.where(
                    allowed, mm_nt(k_ref[rows_at(key_block), :], q_stack), masked_score
                )
                vm.scores[slot(key_block), :] = scores
                return jnp.maximum(high, jnp.max(scores, axis=0, keepdims=True))

            high = lax.fori_loop(low, block, score_pass, jnp.full((1, wide), masked_score, F32))
            allowed = (key_row >= begin - block * tile) & (key_row <= q_pos - block * tile)
            scores = jnp.where(allowed, mm_nt(k_ref[here, :], q_stack), masked_score)
            vm.scores[slot(block), :] = scores
            high = jnp.maximum(high, jnp.max(scores, axis=0, keepdims=True))

            def prob_pass(key_block, carry):
                total, mixed = carry
                rows = rows_at(key_block)
                probs = jnp.exp(vm.scores[slot(key_block), :] - high)
                total = total + jnp.sum(probs, axis=0, keepdims=True)
                probs = probs.astype(BF)
                vm.probs[slot(key_block), :] = probs
                mixed = tuple(
                    mixed[h] + mm(vm.values_t[lanes_of[h], rows], probs[:, cols[h]])
                    for h in range(heads)
                )
                return total, mixed

            zeros = tuple(jnp.zeros((HEAD, tile), F32) for _ in range(heads))
            total, mixed = lax.fori_loop(
                low, block + 1, prob_pass, (jnp.zeros((1, wide), F32), zeros)
            )
            inverse = 1.0 / total
            grads_t = g_ref[here, :].astype(F32).T
            mixed = [mixed[h] * inverse[:, cols[h]] for h in range(heads)]
            scaled = [grads_t[lanes_of[h], :] * inverse[:, cols[h]] for h in range(heads)]
            delta = jnp.concatenate(
                [jnp.sum(mixed[h] * scaled[h], axis=0, keepdims=True) for h in range(heads)],
                axis=1,
            )
            vm.mixed[here, :] = jnp.concatenate(mixed, axis=0).T.astype(BF)
            g_stack = by_head(jnp.concatenate(scaled, axis=0).T.astype(BF))

            def grad_pass(key_block, grads_q):
                rows = rows_at(key_block)
                probs = vm.probs[slot(key_block), :]
                grad_probs = mm_nt(v_ref[rows, :], g_stack)
                grad_scores = (probs.astype(F32) * (grad_probs - delta)).astype(BF)
                vm.acc_v[rows, :] += mm(probs, g_stack)
                vm.acc_k[rows, :] += mm(grad_scores, q_stack)
                return tuple(
                    grads_q[h] + mm(vm.keys_t[lanes_of[h], rows], grad_scores[:, cols[h]])
                    for h in range(heads)
                )

            grads_q = lax.fori_loop(low, block + 1, grad_pass, zeros)
            finish_grad("gq", 0, here, (jnp.concatenate(grads_q, axis=0) * scale).T)
            return carry_in

        def finish_grad(name, row, rows, value):
            if row < 2:
                start = rows.start
                cosine, sine = rotary_tables(
                    meta_ref[start // tokens, :, pl.ds(pl.multiple_of(start % tokens, tile), tile)],
                    const_ref, hw,
                )
                value = turn(value, cosine, sine, -1.0)
            value = value.astype(BF)
            vm[name][rows, :] = value
            vm.qkv_sum[row : row + 1, :] += jnp.sum(value.astype(F32), axis=0, keepdims=True)

        def attend_blocks(first, last):
            none = s // 64
            lax.fori_loop(first + none, last + none, attend, 0)

        def forward_down():
            sent = []
            for jz, done in enumerate(z_down, 1):
                done.wait_recv()
                at = (z ^ jz) * lo + y
                sent += [net.send(part_down(at), part_down(at), dp=d ^ jy) for jy in range(1, lo)]
            return sent

        parity, across = s % 2, s // 2

        def put(parts, j, start, value):
            size = value.shape[0]
            slot = (1 - j % 2) * nx + j // 2
            for c in range(ns):
                at = pl.ds(pl.multiple_of(c * tokens + start, size), size)
                parts[slot, at, :] = value[:, c * hw : (c + 1) * hw]

        def add_got(keep, got, m):
            keep[m] = (keep[m].astype(F32) + got[m].astype(F32)).astype(BF)

        def as_cut(ref):
            return ref.reshape(ns, tokens, hw)

        give_out, keep_out = vm.out_parts.at[0:nx], vm.out_parts.at[nx : 2 * nx]
        core_out = [
            net.make(give_out.at[chip ^ across], vm.got_out.at[chip ^ across], seq=s ^ 1)
            for chip in range(nx)
        ]
        far_out = net.make(as_cut(keep_out.at[1]), out.far_out.at[0], seq=s ^ 2)
        home_out = local.make(as_cut(keep_out.at[0]), out.home_out)

        def ask_out(first):
            stream.ask([hbm.act], tokens, lambda t: (t + first) ^ s)

        def out_blocks(first, last):
            def body(t, act_tile):
                j = (t + first) ^ s
                rows = pl.ds(pl.multiple_of(j * tokens, tokens), tokens)
                value = mm(vm.mixed[rows, :], vm.w_dense[...]) + mm(act_tile[...], w_down())
                put(vm.out_parts, j, 0, value.astype(BF))

            stream.run(last - first, body)

        def cross_out(chip):
            core_out[chip].wait_recv()
            add_got(keep_out, vm.got_out, chip ^ across)

            @pl.when(across == chip)
            def _():
                home_out.start()

            @pl.when(across != chip)
            def _():
                far_out.start()

        attend_blocks(0, blocks // 2)
        y_down += forward_down()
        sets.down1.start()
        attend_blocks(blocks // 2, blocks - 1)
        sets.down0.middle()
        for done in y_down:
            done.wait_recv()
        down_own.wait()
        vm.up_sum[...] = jnp.zeros_like(vm.up_sum)
        w_down = lambda: vm.w_down[...].reshape(ffw, width)

        gu_tile = vm.stream.at[0, 0, tile : 2 * tile]
        gu_copy = lambda t: pltpu.make_async_copy(
            gu_tile, out.grad_up_low.at[rows_of_step(t, tile)], local_sems.at[n_local - 1]
        )

        def up_tile(t, g_tile, slope_tile):
            grads = (mm_nt(g_tile[...], w_down()) * slope_tile[...].astype(F32)).astype(BF)
            vm.up_sum[0:1, :] += jnp.sum(grads.astype(F32), axis=0, keepdims=True)

            @pl.when(t > 0)
            def _():
                gu_copy(t - 1).wait()

            gu_tile[...] = grads
            gu_copy(t).start()

        stream.run(blocks, up_tile)
        gu_copy(blocks - 1).wait()
        hbm["gu"] = out.grad_up_low
        stream.ask([hbm.ffn, hbm.gu], tokens)
        sets.down1.middle()
        finish_rows("down0")
        finish_rows("down1")
        vm.acc[...] = jnp.zeros_like(vm.acc)
        stream.run(ns, add_products)
        ask_out(0)
        net.release(sets.down0.along_y + sets.down1.along_y)
        sets.up0.start()
        sets.up1.start()
        loads.w_dense.wait()
        out_blocks(0, ns - 1)
        ask_out(ns - 1)
        core_out[0].start()

        @pl.when(parity == 1)
        def _():
            core_out[1].start()

        attend_blocks(blocks - 1, blocks)
        cross_out(0)

        @pl.when(parity == 0)
        def _():
            cross_out(1)

        net.release(sets.down0.along_z + sets.down1.along_z)
        sets.up0.middle()
        out_blocks(ns - 1, ns)
        stream.ask([hbm.attn], tokens)

        @pl.when(parity == 0)
        def _():
            core_out[1].start()

        sets.up1.middle()

        def finish_kv(t, carry):
            rows = pl.ds(pl.multiple_of(t * tile, tile), tile)
            finish_grad("gk", 1, rows, vm.acc_k[rows, :])
            finish_grad("gv", 2, rows, vm.acc_v[rows, :])
            return carry

        lax.fori_loop(0, blocks, finish_kv, 0)

        @pl.when(parity == 1)
        def _():
            cross_out(1)

        def qkv_tile(t, left):
            rows = rows_of_step(t, tokens)
            right = jnp.concatenate([vm[n][rows, :] for n in ("gq", "gk", "gv")], axis=1)
            for m in range(0, width, chunk):
                vm.scores[m : m + chunk, 0 : 3 * hw] += mm_tn(left[:, m : m + chunk], right)

        vm.scores[...] = jnp.zeros_like(vm.scores)
        stream.run(ns, qkv_tile)

        def ask_in(m):
            stream.ask([hbm.gu, hbm.hat], tile, lambda t: t + 2 * m * per)

        ask_in(1)
        for name in ("q", "k", "v"):
            sets[name].start()

        loads.w_qkv.wait()
        loads.w_up.wait()
        vm.gain_sum[...] = jnp.zeros_like(vm.gain_sum)
        give_in, keep_in = vm.pool.at[0:nx], vm.pool.at[nx : 2 * nx]
        core_in = [net.make(give_in.at[m], vm.got_in.at[m], seq=s ^ 1) for m in range(nx)]
        far_in = net.make(as_cut(keep_in.at[1]), out.far_in.at[0], seq=s ^ 2)
        home_in = local.make(as_cut(keep_in.at[0]), out.home_in)

        def in_blocks(m):
            first = 2 * m * per

            def body(step, gu_tile, hat_tile):
                t = step + first
                rows = pl.ds(pl.multiple_of(t * tile, tile), tile)
                joined = jnp.concatenate([vm[n][rows, :] for n in ("gq", "gk", "gv")], axis=1)
                attn = mm_nt(joined, vm.w_qkv[...])
                ffn = mm_nt(gu_tile[...], vm.w_up[...])
                hat = hat_tile[...].astype(F32)
                for row, value in ((1, attn), (3, ffn), (0, attn * hat), (2, ffn * hat)):
                    vm.gain_sum[row : row + 1, :] += jnp.sum(value, axis=0, keepdims=True)
                value = attn * affine[0:1, :] + ffn * affine[2:3, :]
                put(vm.pool, t // per, (t % per) * tile, value.astype(BF))

            stream.run(2 * per, body)
            core_in[m].start()

        in_blocks(1)
        stream.ask([hbm.grads], tokens)
        sets.q.middle()

        def dense_tile(t, g_tile):
            left = vm.mixed[rows_of_step(t, tokens), :]
            vm.scores[width : width + hw, :] += mm_tn(left, g_tile[...])

            @pl.when(t == 0)
            def _():
                vm.gain_sum[4:5, :] = jnp.sum(g_tile[...].astype(F32), axis=0, keepdims=True)

        stream.run(ns, dense_tile)
        ask_in(0)
        sets.dense.start()
        core_in[1].wait_recv()
        add_got(keep_in, vm.got_in, 1)
        far_in.start()
        sets.k.middle()
        in_blocks(0)
        sets.v.middle()

        rows = vm.sum_rows
        rows[...] = jnp.zeros_like(rows)
        parts = hw // 128
        for part in range(3):
            for k in range(parts):
                rows[pl.ds(part * (width // 128) + s * parts + k, 1), :] = vm.qkv_sum[
                    part : part + 1, k * 128 : (k + 1) * 128
                ]

        out_sum = vm.gain_sum[4:5, :]
        lane_row = lax.broadcasted_iota(jnp.int32, (1, 128), 1)
        n = width // (ns * nd)
        per_row = 128 // n
        split = lambda owner: (owner // nd, owner % nd // lo, owner % lo)
        for row in range(width // 128):
            at = slice(row * 128, (row + 1) * 128)
            stack = jnp.concatenate(
                [jnp.zeros((1, 128), F32), out_sum[:, at], jnp.zeros((1, 128), F32)]
                + [vm.gain_sum[k : k + 1, at] for k in range(4)]
                + [jnp.zeros((1, 128), F32)],
                axis=0,
            )
            for q in range(per_row):
                a, b, c = split(row * per_row + q)
                vm.tiles[a, b, c] = pltpu.roll(stack, 128 - q * n, 1) if q else stack
        n = 3 * n
        for owner in range(ns * nd):
            start, row = owner * n % 128, owner * n // 128
            value = rows[row : row + 1, :]
            if start + n > 128:
                value = jnp.where(lane_row >= start, value, rows[row + 1 : row + 2, :])
            a, b, c = split(owner)
            vm.tiles[a, b, c, 0:1, :] = pltpu.roll(value, 128 - start, 1) if start else value
        for c in range(ffw // 128):
            vm.tiles[s, c // lo, c % lo, 2:3, :] = vm.up_sum[0:1, c * 128 : (c + 1) * 128]
        tiles_y = [
            net.send(vm.tiles.at[:, :, y ^ jy], vm.tiles_y.at[jy - 1], dp=d ^ jy)
            for jy in range(1, lo)
        ]

        def column_home(name):
            sets[name].arrive()
            vm["ob_" + name][...] = sets[name].final(s)
            local.copy(vm["ob_" + name], out["own_" + name])
            sent = []
            for js in range(1, ns):
                vm["sw_" + name][js - 1] = sets[name].final(s ^ js).astype(BF)
                sent.append(
                    net.send(
                        vm["sw_" + name].at[js - 1], out["swap_" + name].at[js - 1], seq=s ^ js
                    )
                )
            return sent

        core_in[0].wait_recv()
        add_got(keep_in, vm.got_in, 0)
        home_in.start()
        sent = column_home("up0")
        sets.dense.middle()
        finish_rows("dense")
        for done in tiles_y:
            done.wait_recv()
        total = vm.tiles[:, :, y]
        for jy in range(1, lo):
            total = total + vm.tiles_y[jy - 1]
        vm.tiles_z[...] = total
        tiles_z = [
            net.send(vm.tiles_z.at[:, z ^ jz], vm.tiles_zr.at[jz - 1], dp=d ^ (jz * lo))
            for jz in range(1, hi)
        ]
        for name in ("up1", "q", "k", "v"):
            sent += column_home(name)
        for done in tiles_z:
            done.wait_recv()
        total = vm.tiles_z[:, z]
        for jz in range(1, hi):
            total = total + vm.tiles_zr[jz - 1]
        vm.tiles_s[...] = total
        sent += [
            net.send(vm.tiles_s.at[s ^ js], out.swap_sums.at[js - 1], seq=s ^ js)
            for js in range(1, ns)
        ]
        local.copy(vm.tiles_s.at[s], out.own_sums)
        for name in rows_kind:
            sets[name].arrive()
        far_out.wait_recv()
        far_in.wait_recv()
        for done in sent:
            done.wait_recv()
        local.finish()
        net.finish()

    any_spec = pl.BlockSpec(memory_space=pl.ANY)
    vmem_spec = pl.BlockSpec(memory_space=pltpu.VMEM)
    results = pl.pallas_call(
        kernel,
        out_shape=list(outs.values()),
        in_specs=[any_spec] * (len(in_names) + 1) + [vmem_spec] * 3,
        out_specs=[any_spec] * len(outs),
        scratch_shapes=[pltpu.VMEM(x.shape, x.dtype) for x in scratch.values()]
        + [
            pltpu.SemaphoreType.DMA((n_net,)), pltpu.SemaphoreType.DMA((n_net,)),
            pltpu.SemaphoreType.DMA((n_local,)), pltpu.SemaphoreType.DMA((2, 2)),
        ],
        compiler_params=pltpu.CompilerParams(
            vmem_limit_bytes=MAIN_LIMIT, collective_id=2, has_side_effects=True
        ),
        name="main",
    )(
        *[arrays[n] for n in in_names], down, arrays.meta,
        arrays.affine, jnp.asarray(table_constants()),
    )
    return dict(zip(outs, results))


def finish_kernel(dims, s, hidden, grad_out, affine, parts):
    ns, nd, hi, nx = dims.ns, dims.nd, dims.hi, dims.nx
    tokens, width, hw, ffw = dims.tokens, dims.width, dims.hw, dims.ffw
    r_col, r_dense, r_down = width // (ns * nd), hw // nd, ffw // nd
    tile = 128
    names = [n for n in parts if n != "grad_up_low"]
    token_names = [n for n in names if n.startswith(("home", "far"))]
    vector_rows = (0, 1, 2, 1, 3, 4, 5, 6)
    sds = jax.ShapeDtypeStruct

    def kernel(s_ref, hid, gout, affine_ref, *refs):
        part = dict(zip(names, refs[: len(names)]))
        out_ref, in_ref, qkv_out, dense_out, up_out, down_out, *vectors = refs[len(names) :]
        step = pl.program_id(0)
        here = s_ref[0]

        def whole_sum(name):
            columns = []
            for c in range(ns):
                value = part["home_" + name][c].astype(F32)
                for m in range(nx - 1):
                    value = value + part["far_" + name][m, c].astype(F32)
                columns.append(value)
            return jnp.concatenate(columns, axis=1)

        x = hid[...].astype(F32)
        out_ref[...] = (x + whole_sum("out") + affine_ref[4:5, :]).astype(BF)
        gx = whole_sum("in")
        spread = x - jnp.mean(x, axis=-1, keepdims=True)
        inv_std = lax.rsqrt(jnp.mean(spread * spread, axis=-1, keepdims=True) + epsilon)
        hat = spread * inv_std
        back = inv_std * (
            gx
            - jnp.mean(gx, axis=-1, keepdims=True)
            - hat * jnp.mean(gx * hat, axis=-1, keepdims=True)
        )
        in_ref[...] = (gout[...].astype(F32) + back).astype(BF)

        def rows_sum(name, target, cols):
            groups, rows, n = part["own_" + name].shape
            for g in range(groups):
                value = part["own_" + name][g]
                for jz in range(hi - 1):
                    value = value + part["z_" + name][jz, g].astype(F32)
                target[g * rows : (g + 1) * rows, cols] = value

        @pl.when(step == 0)
        def _():
            rows_sum("down0", down_out, slice(0, width // 2))
            rows_sum("down1", down_out, slice(width // 2, width))
            rows_sum("dense", dense_out, slice(0, width))

        def place(target, name, base):
            w = part["own_" + name].shape[1]
            block = width // 1 if target is qkv_out else ffw
            for js in range(ns):
                owner = here ^ js
                at = base(owner)
                value = (
                    part["own_" + name][...]
                    if js == 0
                    else part["swap_" + name][js - 1].astype(F32)
                )
                target[:, pl.ds(pl.multiple_of(at, 128), w)] = value

        @pl.when(step == 1)
        def _():
            for k, name in enumerate(("q", "k", "v")):
                place(qkv_out, name, lambda owner, k=k: k * width + owner * hw)

        @pl.when(step == 2)
        def _():
            for k, name in enumerate(("up0", "up1")):
                place(up_out, name, lambda owner, k=k: owner * ffw + k * (ffw // 2))
            total = part["own_sums"][...]
            for js in range(ns - 1):
                total = total + part["swap_sums"][js]
            for k, target in zip(vector_rows, vectors):
                target[...] = total[k : k + 1, : target.shape[1]]

    def spec(name):
        shape = parts[name].shape
        if name in token_names:
            lead = shape[:-2]
            zeros = (0,) * len(lead)
            return pl.BlockSpec(lead + (tile, hw), lambda t, s_ref: zeros + (t, 0))
        return whole(shape)

    token_spec = pl.BlockSpec((tile, width), lambda t, s_ref: (t, 0))
    finals = [
        (r_col, 3 * width), (r_dense, width), (r_col, ffw * ns), (r_down, width)
    ] + [(1, (3 if k == 0 else 4 if k == 2 else 1) * r_col) for k in vector_rows]
    return pl.pallas_call(
        kernel,
        out_shape=[sds((tokens, width), BF)] * 2 + [sds(f, F32) for f in finals],
        grid_spec=pltpu.PrefetchScalarGridSpec(
            num_scalar_prefetch=1,
            grid=(tokens // tile,),
            in_specs=[token_spec, token_spec, whole(affine.shape)] + [spec(n) for n in names],
            out_specs=[token_spec, token_spec] + [whole(f) for f in finals],
        ),
        compiler_params=params_of(),
        name="finish",
    )(s, hidden, grad_out, affine, *[parts[n] for n in names])


def fused_plan(
    hidden_states,
    segment_ids,
    positions,
    out_grad,
    qkv_weight,
    qkv_bias,
    dense_weight,
    dense_bias,
    up_weight,
    up_bias,
    down_weight,
    down_bias,
    attn_gain,
    attn_shift,
    ffn_gain,
    ffn_shift,
):
    ns, nd = lax.axis_size("seq"), lax.axis_size("dp")
    tokens, width = hidden_states.shape[1:]
    dims = Dims(ns, nd, tokens, width, up_weight.shape[1])
    s = lax.axis_index("seq").astype(jnp.int32).reshape(1)
    hidden, grad_out = hidden_states[0], out_grad[0]
    fields = (
        qkv_bias, dense_bias, up_bias, down_bias, attn_gain, attn_shift, ffn_gain, ffn_shift
    )
    small = jnp.stack([jnp.pad(f, (0, 128 - f.shape[0])) for f in fields]).astype(F32)
    half = ROT // 2
    freqs = rotary_base ** (-2.0 * jnp.arange(half, dtype=F32) / ROT)
    angles = positions[0].astype(F32)[None, :] * freqs[:, None]
    meta = jnp.concatenate(
        [
            jnp.cos(angles),
            jnp.sin(angles),
            jnp.broadcast_to(segment_ids[0].astype(F32)[None, :], (half, tokens)),
        ],
        axis=0,
    )
    names = (
        "attn", "ffn", "hat", "grads", "act", "slope", "queries", "keys", "values", "keys_t",
        "values_t", "grad_mix", "w_qkv", "w_up", "w_dense", "meta", "affine",
    )
    arrays = Bag(
        zip(
            names,
            gather_kernel(
                dims, hidden, grad_out, meta, small, qkv_weight, up_weight, dense_weight
            ),
        )
    )
    arrays["w_qkv"] = arrays.w_qkv.reshape(width, -1)
    arrays["w_up"] = arrays.w_up.reshape(width, -1)
    arrays["w_dense"] = arrays.w_dense.reshape(-1, width)
    parts = main_kernel(dims, arrays, down_weight)
    output, input_grad, grad_qkv, grad_dense, grad_up, grad_down, *vectors = finish_kernel(
        dims, s, hidden, grad_out, arrays.affine, parts
    )
    vectors = [v.reshape(-1) for v in vectors]
    return (
        output[None],
        input_grad[None],
        grad_qkv,
        vectors[0],
        grad_dense,
        vectors[1],
        grad_up,
        vectors[2],
        grad_down,
        *vectors[3:],
    )


def per_device(*args):
    tokens, width = args[0].shape[1:]
    ns, nd = lax.axis_size("seq"), lax.axis_size("dp")
    fits = ns == 4 and ns * tokens * width <= 2048 * 1024 and width // (ns * nd) % 16 == 0
    return fused_plan(*args) if fits else permute_plan(*args)


def solution(mesh):
    token = P("dp", "seq", None)
    matrix = P(("seq", "dp"), None)
    vector = P(("seq", "dp"))
    weights = (matrix, vector) * 4 + (vector,) * 4
    return jax.shard_map(
        per_device,
        mesh=mesh,
        in_specs=(token, P("dp", "seq"), P("dp", "seq"), token) + weights,
        out_specs=(token, token) + weights,
        check_vma=False,
    )
```

```python
import functools
import math

import jax
import jax.numpy as jnp
import numpy as np
from jax import lax
from jax.experimental import pallas as pl
from jax.experimental.pallas import tpu as pltpu
from jax.sharding import PartitionSpec as P

HEAD = 64
ROT = 16
DOCS = 4
HI = 4

epsilon = 1e-05
masked_score = -1e30
rotary_base = 10000.0

BF = jnp.bfloat16
F32 = jnp.float32
NT = (((1,), (1,)), ((), ()))
TN = (((0,), (0,)), ((), ()))


VMEM_LIMIT = 60 * 1024 * 1024
MAIN_LIMIT = 61 * 1024 * 1024


def xor_swap(value, axis, count, mask):
    return lax.ppermute(value, axis, [(i, i ^ mask) for i in range(count)])


def mm(left, right):
    return jnp.dot(left, right, preferred_element_type=F32)


def mm_nt(left, right):
    return lax.dot_general(left, right, NT, preferred_element_type=F32)


def mm_tn(left, right):
    return lax.dot_general(left, right, TN, preferred_element_type=F32)


def params_of(**more):
    return pltpu.CompilerParams(vmem_limit_bytes=VMEM_LIMIT, **more)


def whole(shape):
    zeros = (0,) * len(shape)
    return pl.BlockSpec(shape, lambda *grid_and_ids: zeros)


class Dims:
    def __init__(self, ns, nd, tokens, width, ff):
        self.ns, self.nd = ns, nd
        self.hi, self.lo = HI, nd // HI
        self.nx = ns // 2
        self.tokens, self.width = tokens, width
        self.seq = ns * tokens
        self.hw = width // ns
        self.ffw = ff // ns
        self.heads = self.hw // HEAD


def piece_copies(dims, kind, ids, pieces, target, sems):
    s, z, y = ids[0], ids[1], ids[2]
    copies = []
    for jz in range(dims.hi):
        for jy in range(dims.lo):
            piece = pieces[jz * dims.lo + jy]
            owner = (z ^ jz) * dims.lo + (y ^ jy)
            if kind == "row":
                rows = piece.shape[0]
                at = pl.multiple_of(owner * rows, rows)
                copies.append(
                    pltpu.make_async_copy(piece, target.at[pl.ds(at, rows)], sems.at[len(copies)])
                )
            else:
                rows = piece.shape[1]
                for js in range(dims.ns):
                    at = pl.multiple_of(((s ^ js) * dims.nd + owner) * rows, rows)
                    copies.append(
                        pltpu.make_async_copy(
                            piece.at[js], target.at[pl.ds(at, rows)], sems.at[len(copies)]
                        )
                    )
    return copies


def token_call(dims, name, ids, body, lhs, weights, extras, outs, tile, flops, scratch=()):
    count = dims.seq // tile
    n_lhs, n_out = len(lhs), len(outs)
    sizes = [len(w[1]) for w in weights]
    sem_counts = [
        len(w[1]) * (dims.ns if w[0] == "col" else 1) for w in weights
    ]

    def kernel(ids_ref, *refs):
        at = 0
        lhs_refs = refs[:n_lhs]
        at = n_lhs
        piece_refs = []
        for size in sizes:
            piece_refs.append(refs[at : at + size])
            at += size
        extra_refs = refs[at : at + len(extras)]
        at += len(extras)
        out_refs = refs[at : at + n_out]
        at += n_out
        weight_refs = refs[at : at + len(weights)]
        at += len(weights)
        sem_refs = refs[at : at + len(weights)]
        at += len(weights)
        scratch_refs = refs[at:]
        step = pl.program_id(0)

        if weights:

            @pl.when(step == 0)
            def _():
                copies = []
                for w, group, target, sems in zip(weights, piece_refs, weight_refs, sem_refs):
                    copies += piece_copies(dims, w[0], ids_ref, group, target, sems)
                for copy in copies:
                    copy.start()
                for copy in copies:
                    copy.wait()

        body(step, count, lhs_refs, weight_refs, extra_refs, out_refs, scratch_refs)

    in_specs = [pl.BlockSpec((tile, a.shape[1]), lambda i, ids_ref: (i, 0)) for a in lhs]
    for size in sizes:
        in_specs += [pl.BlockSpec(memory_space=pl.ANY)] * size
    in_specs += [whole(a.shape) for a in extras]
    bytes_moved = sum(a.size * a.dtype.itemsize for a in lhs) + sum(
        math.prod(o[0].shape) * o[0].dtype.itemsize for o in outs
    )
    return pl.pallas_call(
        kernel,
        out_shape=[o[0] for o in outs],
        grid_spec=pltpu.PrefetchScalarGridSpec(
            num_scalar_prefetch=1,
            grid=(count,),
            in_specs=in_specs,
            out_specs=[o[1] for o in outs],
            scratch_shapes=[pltpu.VMEM(w[2], BF) for w in weights]
            + [pltpu.SemaphoreType.DMA((n,)) for n in sem_counts]
            + list(scratch),
        ),
        compiler_params=params_of(),
        cost_estimate=pl.CostEstimate(flops=flops, bytes_accessed=bytes_moved, transcendentals=0),
        name=name,
    )(ids, *lhs, *[p for w in weights for p in w[1]], *extras)


def tiled_out(rows, cols, tile, dtype=BF):
    return (
        jax.ShapeDtypeStruct((rows, cols), dtype),
        pl.BlockSpec((tile, cols), lambda i, ids_ref: (i, 0)),
    )


def norm_pair(dims, pair, first, second, affine, carried):
    tile = 256
    per = dims.tokens // tile
    base = pair * 2 * per

    def kernel(*refs):
        a_ref, b_ref, affine_ref = refs[:3]
        attn_ref, ffn_ref, hat_ref, rows_ref = refs[-4:]
        block = pl.program_id(0)

        @pl.when(block == 0)
        def _():
            rows_ref[...] = a_ref[...]

        @pl.when(block == 1)
        def _():
            rows_ref[...] = b_ref[...]

        rows = rows_ref[...].astype(F32)
        center = jnp.mean(rows, axis=-1, keepdims=True)
        spread = rows - center
        hat = spread * lax.rsqrt(jnp.mean(spread * spread, axis=-1, keepdims=True) + epsilon)
        attn_ref[...] = (hat * affine_ref[0:1, :] + affine_ref[1:2, :]).astype(BF)
        ffn_ref[...] = (hat * affine_ref[2:3, :] + affine_ref[3:4, :]).astype(BF)
        hat_ref[...] = hat.astype(BF)

    out_spec = pl.BlockSpec((tile, dims.width), lambda b, t: (base + b * per + t, 0))
    shape = jax.ShapeDtypeStruct((dims.seq, dims.width), BF)
    return pl.pallas_call(
        kernel,
        out_shape=[shape] * 3,
        grid=(2, per),
        in_specs=[
            pl.BlockSpec((tile, dims.width), lambda b, t: (jnp.where(b == 0, t, per - 1), 0)),
            pl.BlockSpec((tile, dims.width), lambda b, t: (jnp.where(b == 0, 0, t), 0)),
            pl.BlockSpec((8, dims.width), lambda b, t: (0, 0)),
        ]
        + [pl.BlockSpec(memory_space=pl.ANY)] * len(carried),
        out_specs=[out_spec] * 3,
        scratch_shapes=[pltpu.VMEM((tile, dims.width), BF)],
        input_output_aliases={3 + i: i for i in range(len(carried))},
        compiler_params=params_of(),
        cost_estimate=pl.CostEstimate(
            flops=20 * 2 * dims.tokens * dims.width,
            bytes_accessed=2 * dims.tokens * dims.width * 8,
            transcendentals=0,
        ),
        name="norm_pair",
    )(first, second, affine, *carried)


def up_body(step, count, lhs, weights, extras, outs, scratch):
    pre = mm(lhs[0][...], weights[0][...]) + extras[0][0:1, :]
    total = 0.5 + 0.5 * lax.erf(pre * math.sqrt(0.5))
    density = jnp.exp(-0.5 * pre * pre) * (1.0 / math.sqrt(2.0 * math.pi))
    outs[0][...] = (pre * total).astype(BF)
    outs[1][...] = (total + pre * density).astype(BF)


def turn(values, cosine, sine, sign):
    lane = lax.broadcasted_iota(jnp.int32, (1, values.shape[1]), 1) % HEAD
    width = values.shape[1]
    half = ROT // 2
    other = jnp.where(
        lane < half, pltpu.roll(values, width - half, 1), pltpu.roll(values, half, 1)
    )
    return values * cosine + sign * (other * sine)


def spread_lanes(table, width):
    times = width // table.shape[1]
    return table if times == 1 else jnp.concatenate([table] * times, axis=1)


def qkv_body(dims, step, count, lhs, weights, extras, outs, scratch):
    hw = dims.hw
    joined = mm(lhs[0][...], weights[0][...]) + extras[0][0:1, :]
    cosine = spread_lanes(lhs[1][...], hw)
    sine = spread_lanes(lhs[2][...], hw)
    queries = turn(joined[:, :hw], cosine, sine, 1.0)
    keys = turn(joined[:, hw : 2 * hw], cosine, sine, 1.0)
    values = joined[:, 2 * hw :]
    outs[0][...] = queries.astype(BF) * (1.0 / math.sqrt(HEAD))
    outs[1][...] = keys.astype(BF)
    outs[2][...] = values.astype(BF)
    outs[3][...] = keys.T.astype(BF)
    outs[4][...] = values.T.astype(BF)


def mix_grad_body(step, count, lhs, weights, extras, outs, scratch):
    outs[0][...] = mm_nt(lhs[0][...], weights[0][...]).astype(BF)


def attention(dims, ids, queries, keys, values, keys_t, values_t, grad_mix, cos_table, sin_table):
    tile = 256
    hw, seq, heads = dims.hw, dims.seq, dims.heads
    per = dims.tokens // tile
    count = seq // tile
    scale = 1.0 / math.sqrt(HEAD)

    def place(ids_ref, block):
        return ((block // per) ^ ids_ref[0]) * per + block % per

    def kernel(
        ids_ref, q_ref, k_ref, v_ref, kt_ref, vt_ref, g_ref, cos_ref, sin_ref,
        mix_ref, gq_ref, gk_ref, gv_ref, sum_ref,
        score_ref, prob_ref, gk_acc, gv_acc,
    ):
        block = pl.program_id(0)

        @pl.when(block == 0)
        def _():
            gk_acc[...] = jnp.zeros_like(gk_acc)
            gv_acc[...] = jnp.zeros_like(gv_acc)
            sum_ref[...] = jnp.zeros_like(sum_ref)

        lane = lax.broadcasted_iota(jnp.int32, (1, hw), 1)
        own = [lane // HEAD == h for h in range(heads)]
        queries_here = q_ref[...]
        grads_here = g_ref[...]
        q_heads = [jnp.where(own[h], queries_here, jnp.zeros_like(queries_here)) for h in range(heads)]
        q_pos = block * tile + lax.broadcasted_iota(jnp.int32, (1, tile), 1)
        begin = jnp.zeros((1, tile), jnp.int32)
        low = 0
        for doc in range(1, DOCS):
            edge = ids_ref[doc]
            begin = jnp.where(q_pos >= edge, jnp.maximum(begin, edge), begin)
            low = jnp.where(edge <= block * tile, jnp.maximum(low, edge), low)
        low = low // tile

        def rows_of(key_block):
            return pl.ds(pl.multiple_of(place(ids_ref, key_block) * tile, tile), tile)

        def slot(key_block):
            return pl.ds(pl.multiple_of((key_block - low) * tile, tile), tile)

        def score_pass(key_block, highs):
            rows = k_ref[rows_of(key_block), :]
            key_pos = key_block * tile + lax.broadcasted_iota(jnp.int32, (tile, tile), 0)
            allowed = (key_pos >= begin) & (key_pos <= q_pos)
            result = []
            for h in range(heads):
                scores = jnp.where(allowed, mm_nt(rows, q_heads[h]), masked_score)
                score_ref[h, slot(key_block), :] = scores
                result.append(jnp.maximum(highs[h], jnp.max(scores, axis=0, keepdims=True)))
            return tuple(result)

        highs = lax.fori_loop(
            low, block + 1, score_pass,
            tuple(jnp.full((1, tile), masked_score, F32) for _ in range(heads)),
        )

        def prob_pass(key_block, carry):
            result = []
            rows = rows_of(key_block)
            for h in range(heads):
                total, mixed = carry[2 * h], carry[2 * h + 1]
                probs = jnp.exp(score_ref[h, slot(key_block), :] - highs[h])
                total = total + jnp.sum(probs, axis=0, keepdims=True)
                probs = probs.astype(BF)
                prob_ref[h, slot(key_block), :] = probs
                mixed = mixed + mm(vt_ref[h * HEAD : (h + 1) * HEAD, rows], probs)
                result += [total, mixed]
            return tuple(result)

        start = []
        for h in range(heads):
            start += [jnp.zeros((1, tile), F32), jnp.zeros((HEAD, tile), F32)]
        summed = lax.fori_loop(low, block + 1, prob_pass, tuple(start))

        grads_t = grads_here.astype(F32).T
        mixed_parts, scaled_parts, deltas = [], [], []
        for h in range(heads):
            inverse = 1.0 / summed[2 * h]
            mixed = summed[2 * h + 1] * inverse
            grads = grads_t[h * HEAD : (h + 1) * HEAD, :] * inverse
            deltas.append(jnp.sum(mixed * grads, axis=0, keepdims=True))
            mixed_parts.append(mixed)
            scaled_parts.append(grads)
        mix_ref[...] = jnp.concatenate(mixed_parts, axis=0).T.astype(BF)
        scaled = jnp.concatenate(scaled_parts, axis=0).T.astype(BF)
        g_heads = [jnp.where(own[h], scaled, jnp.zeros_like(scaled)) for h in range(heads)]

        def grad_pass(key_block, grads_q):
            rows = rows_of(key_block)
            value_rows = v_ref[rows, :]
            result = []
            grad_k = gk_acc[rows, :]
            grad_v = gv_acc[rows, :]
            for h in range(heads):
                probs = prob_ref[h, slot(key_block), :]
                grad_probs = mm_nt(value_rows, g_heads[h])
                grad_scores = (probs.astype(F32) * (grad_probs - deltas[h])).astype(BF)
                grad_v = grad_v + mm(probs, g_heads[h])
                grad_k = grad_k + mm(grad_scores, q_heads[h])
                result.append(
                    grads_q[h] + mm(kt_ref[h * HEAD : (h + 1) * HEAD, rows], grad_scores)
                )
            gk_acc[rows, :] = grad_k
            gv_acc[rows, :] = grad_v
            return tuple(result)

        grads_q = lax.fori_loop(
            low, block + 1, grad_pass, tuple(jnp.zeros((HEAD, tile), F32) for _ in range(heads))
        )
        here = rows_of(block)
        rot = (jnp.concatenate(grads_q, axis=0) * scale).T
        grad_q = turn(
            rot, spread_lanes(cos_ref[here, :], hw), spread_lanes(sin_ref[here, :], hw), -1.0
        ).astype(BF)
        gq_ref[...] = grad_q
        sum_ref[0:1, :] += jnp.sum(grad_q.astype(F32), axis=0, keepdims=True)

        @pl.when(block == count - 1)
        def _():
            def finish(t, carry):
                rows = pl.ds(pl.multiple_of(t * tile, tile), tile)
                grad_k = turn(
                    gk_acc[rows, :],
                    spread_lanes(cos_ref[rows, :], hw),
                    spread_lanes(sin_ref[rows, :], hw),
                    -1.0,
                ).astype(BF)
                grad_v = gv_acc[rows, :].astype(BF)
                gk_ref[rows, :] = grad_k
                gv_ref[rows, :] = grad_v
                sum_ref[1:2, :] += jnp.sum(grad_k.astype(F32), axis=0, keepdims=True)
                sum_ref[2:3, :] += jnp.sum(grad_v.astype(F32), axis=0, keepdims=True)
                return carry

            lax.fori_loop(0, count, finish, 0)

    tiled = pl.BlockSpec((tile, hw), lambda i, ids_ref: (place(ids_ref, i), 0))
    shape = jax.ShapeDtypeStruct((seq, hw), BF)
    return pl.pallas_call(
        kernel,
        out_shape=[shape] * 4 + [jax.ShapeDtypeStruct((8, hw), F32)],
        grid_spec=pltpu.PrefetchScalarGridSpec(
            num_scalar_prefetch=1,
            grid=(count,),
            in_specs=[
                tiled,
                whole((seq, hw)),
                whole((seq, hw)),
                whole((hw, seq)),
                whole((hw, seq)),
                tiled,
                whole(cos_table.shape),
                whole(sin_table.shape),
            ],
            out_specs=[tiled, tiled, whole((seq, hw)), whole((seq, hw)), whole((8, hw))],
            scratch_shapes=[
                pltpu.VMEM((heads, seq, tile), F32),
                pltpu.VMEM((heads, seq, tile), BF),
                pltpu.VMEM((seq, hw), F32),
                pltpu.VMEM((seq, hw), F32),
            ],
        ),
        compiler_params=params_of(),
        cost_estimate=pl.CostEstimate(
            flops=12 * seq * seq * hw, bytes_accessed=10 * seq * hw * 2, transcendentals=0
        ),
        name="attention",
    )(ids, queries, keys, values, keys_t, values_t, grad_mix, cos_table, sin_table)


def split_specs(dims, tile):
    per = dims.tokens // tile
    shape = jax.ShapeDtypeStruct((dims.nx, dims.tokens, dims.width), BF)

    def spec(odd):
        def index(i, ids_ref):
            block, t = i // per, i % per
            mine = block % 2 == odd
            row = jnp.where(mine, t, per - 1 if odd == 0 else 0)
            return (block // 2, row, 0)

        return pl.BlockSpec((None, tile, dims.width), index)

    return [(shape, spec(1)), (shape, spec(0))], per


def put_split(step, per, outs, value):
    odd = (step // per) % 2

    @pl.when(odd == 1)
    def _():
        outs[0][...] = value

    @pl.when(odd == 0)
    def _():
        outs[1][...] = value


def out_body(per, step, count, lhs, weights, extras, outs, scratch):
    value = mm(lhs[0][...], weights[0][...]) + mm(lhs[1][...], weights[1][...])
    put_split(step, per, outs, value.astype(BF))


def up_grad_body(step, count, lhs, weights, extras, outs, scratch):
    grads = (mm_nt(lhs[0][...], weights[0][...]) * lhs[1][...].astype(F32)).astype(BF)
    outs[0][...] = grads

    @pl.when(step == 0)
    def _():
        outs[1][...] = jnp.zeros_like(outs[1])

    outs[1][0:1, :] += jnp.sum(grads.astype(F32), axis=0, keepdims=True)


def in_grad_body(per, hw, step, count, lhs, weights, extras, outs, scratch):
    up_grad, gq, gk, gv, hat_ref = lhs
    qkv_ref, up_ref = weights
    affine = extras[0]
    attn = (
        mm_nt(gq[...], qkv_ref[:, :hw])
        + mm_nt(gk[...], qkv_ref[:, hw : 2 * hw])
        + mm_nt(gv[...], qkv_ref[:, 2 * hw :])
    )
    ffn = mm_nt(up_grad[...], up_ref[...])
    hat = hat_ref[...].astype(F32)

    @pl.when(step == 0)
    def _():
        outs[2][...] = jnp.zeros_like(outs[2])

    for row, value in enumerate((attn * hat, attn, ffn * hat, ffn)):
        outs[2][row : row + 1, :] += jnp.sum(value, axis=0, keepdims=True)
    put_split(step, per, outs, (attn * affine[0:1, :] + ffn * affine[2:3, :]).astype(BF))


def weight_grad(dims, name, kind, ids, left, rights):
    tile = 512
    m = left.shape[1]
    widths = [r.shape[1] for r in rights]
    n = sum(widths)
    count = dims.seq // tile
    hi, lo, ns, nd = dims.hi, dims.lo, dims.ns, dims.nd
    if kind == "row":
        rows = m // nd
        shape = (hi, rows, n)
    else:
        rows = m // (nd * ns)
        shape = (hi, ns, rows, n)

    def kernel(ids_ref, left_ref, *refs):
        right_refs = refs[: len(rights)]
        out_refs = refs[len(rights) : len(rights) + lo]
        total = refs[-1]
        step = pl.program_id(0)
        at = 0
        for width, right_ref in zip(widths, right_refs):
            part = mm_tn(left_ref[...], right_ref[...])
            cols = slice(at, at + width)

            @pl.when(step == 0)
            def _():
                total[:, cols] = part

            @pl.when(step > 0)
            def _():
                total[:, cols] += part

            at += width

        @pl.when(step == count - 1)
        def _():
            s, z, y = ids_ref[0], ids_ref[1], ids_ref[2]
            for jy in range(lo):
                for jz in range(hi):
                    owner = (z ^ jz) * lo + (y ^ jy)
                    if kind == "row":
                        at = pl.multiple_of(owner * rows, rows)
                        out_refs[jy][jz] = total[pl.ds(at, rows), :].astype(BF)
                    else:
                        for js in range(ns):
                            at = pl.multiple_of(((s ^ js) * nd + owner) * rows, rows)
                            out_refs[jy][jz, js] = total[pl.ds(at, rows), :].astype(BF)

    return pl.pallas_call(
        kernel,
        out_shape=[jax.ShapeDtypeStruct(shape, BF)] * lo,
        grid_spec=pltpu.PrefetchScalarGridSpec(
            num_scalar_prefetch=1,
            grid=(count,),
            in_specs=[pl.BlockSpec((tile, m), lambda i, ids_ref: (i, 0))]
            + [pl.BlockSpec((tile, w), lambda i, ids_ref: (i, 0)) for w in widths],
            out_specs=[whole(shape)] * lo,
            scratch_shapes=[pltpu.VMEM((m, n), F32)],
        ),
        compiler_params=params_of(),
        cost_estimate=pl.CostEstimate(
            flops=2 * dims.seq * m * n,
            bytes_accessed=2 * (dims.seq * (m + n) + m * n),
            transcendentals=0,
        ),
        name=name,
    )(ids, left, *rights)


def cut_columns(dims, ids, qkv, up):
    ns, hw, ffw = dims.ns, dims.hw, dims.ffw
    rows = qkv.shape[0]

    def kernel(ids_ref, qkv_ref, up_ref, *outs):
        for js in range(ns):
            other = ids_ref[0] ^ js
            for part in range(3):
                at = pl.multiple_of(part * dims.width + other * hw, hw)
                outs[js][:, part * hw : (part + 1) * hw] = qkv_ref[:, pl.ds(at, hw)]
            at = pl.multiple_of(other * ffw, ffw)
            outs[js][:, 3 * hw :] = up_ref[:, pl.ds(at, ffw)]

    shape = (rows, 3 * hw + ffw)
    return pl.pallas_call(
        kernel,
        out_shape=[jax.ShapeDtypeStruct(shape, BF)] * ns,
        grid_spec=pltpu.PrefetchScalarGridSpec(
            num_scalar_prefetch=1,
            grid=(1,),
            in_specs=[whole(qkv.shape), whole(up.shape)],
            out_specs=[whole(shape)] * ns,
        ),
        compiler_params=params_of(),
        name="cut_columns",
    )(ids, qkv, up)


def join_columns(dims, ids, pieces, parts, width):
    ns = dims.ns
    rows, n = pieces[0].shape
    w = n // parts
    total = n * ns

    def kernel(ids_ref, *refs):
        out = refs[-1]
        for js in range(ns):
            other = ids_ref[0] ^ js
            for part in range(parts):
                at = pl.multiple_of(part * width + other * w, w)
                out[:, pl.ds(at, w)] = refs[js][:, part * w : (part + 1) * w].astype(F32)

    return pl.pallas_call(
        kernel,
        out_shape=jax.ShapeDtypeStruct((rows, total), F32),
        grid_spec=pltpu.PrefetchScalarGridSpec(
            num_scalar_prefetch=1,
            grid=(1,),
            in_specs=[whole((rows, n))] * ns,
            out_specs=whole((rows, total)),
        ),
        compiler_params=params_of(),
        name="join_columns",
    )(ids, *pieces)


def permute_plan(
    hidden_states,
    segment_ids,
    positions,
    out_grad,
    qkv_weight,
    qkv_bias,
    dense_weight,
    dense_bias,
    up_weight,
    up_bias,
    down_weight,
    down_bias,
    attn_gain,
    attn_shift,
    ffn_gain,
    ffn_shift,
):
    ns, nd = lax.axis_size("seq"), lax.axis_size("dp")
    tokens, width = hidden_states.shape[1:]
    dims = Dims(ns, nd, tokens, width, up_weight.shape[1])
    hi, lo, nx = dims.hi, dims.lo, dims.nx
    hw, ffw, seq = dims.hw, dims.ffw, dims.seq
    s, d = lax.axis_index("seq"), lax.axis_index("dp")
    z, y = d // lo, d % lo
    ids = jnp.stack([s, z, y, s]).astype(jnp.int32)

    def by_seq(value, mask):
        return xor_swap(value, "seq", ns, mask)

    def by_dp(value, mask):
        return xor_swap(value, "dp", nd, mask)

    hidden, grad_out = hidden_states[0], out_grad[0]

    fields = (qkv_bias, dense_bias, up_bias, down_bias, attn_gain, attn_shift, ffn_gain, ffn_shift)
    mine = jnp.concatenate(fields)
    index = s * nd + d
    small = jnp.where(jnp.arange(ns * nd)[:, None] == index, mine[None, :], jnp.zeros((), BF))
    mask = 1
    while mask < ns:
        small = small + by_seq(small, mask)
        mask *= 2
    mask = 1
    while mask < nd:
        small = small + by_dp(small, mask)
        mask *= 2
    full, at = [], 0
    for field in fields:
        n = field.shape[0]
        full.append(small[:, at : at + n].reshape(-1).astype(F32))
        at += n
    b_qkv, b_dense, b_up, b_down, g_attn, s_attn, g_ffn, s_ffn = full
    affine = jnp.concatenate(
        [jnp.stack([g_attn, s_attn, g_ffn, s_ffn]), jnp.zeros((4, width), F32)], axis=0
    )
    bias_qkv = lax.dynamic_index_in_dim(
        b_qkv.reshape(3, ns, hw), s, 1, keepdims=False
    ).reshape(1, 3 * hw)
    bias_up = lax.dynamic_slice_in_dim(b_up, s * ffw, ffw).reshape(1, ffw)

    meta = jnp.stack([segment_ids[0], positions[0]])
    metas = [meta] + [by_seq(meta, js) for js in range(1, ns)]
    meta_all = jnp.concatenate(metas, axis=1)
    starts = [jnp.sum((meta_all[0] < v).astype(jnp.int32)) for v in range(1, DOCS)]
    doc_ids = jnp.stack([s.astype(jnp.int32)] + starts)
    half = ROT // 2
    freqs = rotary_base ** (-2.0 * jnp.arange(half, dtype=F32) / ROT)
    angles = meta_all[1].astype(F32)[None, :] * freqs[:, None]
    table = 2 * HEAD
    pick = np.zeros((half, table), np.float32)
    signed = np.zeros((half, table), np.float32)
    rest = np.ones((1, table), np.float32)
    for lane in range(table):
        if lane % HEAD < ROT:
            pick[lane % HEAD % half, lane] = 1.0
            signed[lane % HEAD % half, lane] = -1.0 if lane % HEAD < half else 1.0
            rest[0, lane] = 0.0
    exact = lax.Precision.HIGHEST
    cos_table = lax.dot_general(jnp.cos(angles), jnp.asarray(pick), TN, precision=exact) + rest
    sin_table = lax.dot_general(jnp.sin(angles), jnp.asarray(signed), TN, precision=exact)

    def gather_tokens(value):
        found = [value, by_seq(value, 1)]
        for m in range(1, nx):
            across = by_seq(value, 2 * m)
            found += [across, by_seq(across, 1)]
        return found

    blocks = gather_tokens(hidden)

    cuts = cut_columns(dims, ids, qkv_weight, up_weight)
    got = [cuts[0]] + [by_seq(cuts[js], js) for js in range(1, ns)]
    stacked = jnp.stack(got)

    def gather_dp(shard):
        pieces = []
        for jz in range(hi):
            here = shard if jz == 0 else by_dp(shard, jz * lo)
            pieces += [here] + [by_dp(here, jy) for jy in range(1, lo)]
        return pieces

    up_pieces = gather_dp(stacked[:, :, 3 * hw :])
    qkv_pieces = gather_dp(stacked[:, :, : 3 * hw])
    dense_pieces = gather_dp(dense_weight)
    down_pieces = gather_dp(down_weight)
    qkv_w = ("col", qkv_pieces, (width, 3 * hw))
    up_w = ("col", up_pieces, (width, ffw))
    dense_w = ("row", dense_pieces, (hw, width))
    down_w = ("row", down_pieces, (ffw, width))

    carried = ()
    for m in range(nx):
        carried = norm_pair(dims, m, blocks[2 * m], blocks[2 * m + 1], affine, carried)
    attn_low, ffn_low, hat_low = carried

    tile = 256
    act, slope = token_call(
        dims, "up", ids, up_body, [ffn_low], [up_w], [bias_up],
        [tiled_out(seq, ffw, tile)] * 2, tile, 2 * seq * width * ffw * 2,
    )
    flip = (
        jax.ShapeDtypeStruct((hw, seq), BF),
        pl.BlockSpec((hw, tile), lambda i, ids_ref: (0, i)),
    )
    queries, keys, values, keys_t, values_t = token_call(
        dims, "qkv", ids, functools.partial(qkv_body, dims), [attn_low, cos_table, sin_table],
        [qkv_w], [bias_qkv], [tiled_out(seq, hw, tile)] * 3 + [flip] * 2, tile,
        2 * seq * width * 3 * hw,
    )
    grads_all = jnp.concatenate(gather_tokens(grad_out), axis=0)
    grad_mix = token_call(
        dims, "mix_grad", ids, mix_grad_body, [grads_all], [dense_w], [],
        [tiled_out(seq, hw, tile)], tile, 2 * seq * width * hw,
    )[0]
    mixed, gq, gk, gv, qkv_sums = attention(
        dims, doc_ids, queries, keys, values, keys_t, values_t, grad_mix, cos_table, sin_table
    )

    def reduce_tokens(others, own):
        got = by_seq(others, 1)
        total = own[0].astype(F32) + got[0].astype(F32)
        for m in range(1, nx):
            total = total + by_seq(own[m] + got[m], 2 * m).astype(F32)
        return total

    def reduce_dp(parts):
        got = [by_dp(parts[jy], jy) for jy in range(1, lo)]

        def slab(jz):
            value = parts[0][jz].astype(F32)
            for g in got:
                value = value + g[jz].astype(F32)
            return value

        total = slab(0)
        for jz in range(1, hi):
            total = total + by_dp(slab(jz).astype(BF), jz * lo).astype(F32)
        return total

    def columns_home(total, parts):
        low = total.astype(BF)
        pieces = [low[0]] + [by_seq(low[js], js) for js in range(1, ns)]
        return join_columns(dims, ids, pieces, parts, width)

    down_parts = weight_grad(dims, "down_grad", "row", ids, act, [grads_all])
    grad_down = reduce_dp(down_parts)
    dense_parts = weight_grad(dims, "dense_grad", "row", ids, mixed, [grads_all])
    grad_dense = reduce_dp(dense_parts)
    qkv_parts = weight_grad(dims, "qkv_grad", "col", ids, attn_low, [gq, gk, gv])
    grad_qkv = columns_home(reduce_dp(qkv_parts), 3)

    sums_shape = lambda n: (jax.ShapeDtypeStruct((8, n), F32), whole((8, n)))
    grad_up_low, up_sums = token_call(
        dims, "up_grad", ids, up_grad_body, [grads_all, slope], [down_w], [],
        [tiled_out(seq, ffw, tile), sums_shape(ffw)], tile, 2 * seq * width * ffw,
    )
    up_parts = weight_grad(dims, "up_w_grad", "col", ids, ffn_low, [grad_up_low])
    grad_up = columns_home(reduce_dp(up_parts), 1)

    outs, per = split_specs(dims, tile)
    others, own = token_call(
        dims, "out", ids, functools.partial(out_body, per), [mixed, act], [dense_w, down_w], [],
        outs, tile, 2 * seq * width * (hw + ffw),
    )
    out_total = reduce_tokens(others, own)
    output = (hidden.astype(F32) + out_total + (b_dense + b_down)[None, :]).astype(BF)

    others, own, gain_sums = token_call(
        dims, "in_grad", ids, functools.partial(in_grad_body, per, hw),
        [grad_up_low, gq, gk, gv, hat_low], [qkv_w, up_w], [affine],
        outs + [sums_shape(width)], tile, 2 * seq * width * (3 * hw + ffw),
    )
    gx = reduce_tokens(others, own)
    rows = hidden.astype(F32)
    spread = rows - jnp.mean(rows, axis=-1, keepdims=True)
    inv_std = lax.rsqrt(jnp.mean(spread * spread, axis=-1, keepdims=True) + epsilon)
    hat = spread * inv_std
    back = inv_std * (
        gx
        - jnp.mean(gx, axis=-1, keepdims=True)
        - hat * jnp.mean(gx * hat, axis=-1, keepdims=True)
    )
    grad_out_f = grad_out.astype(F32)
    input_grad = (grad_out_f + back).astype(BF)

    def placed(value, parts, w):
        base = jnp.zeros((parts, ns, w), F32)
        return lax.dynamic_update_slice_in_dim(base, value.reshape(parts, 1, w), s, 1).reshape(-1)

    out_sum = jnp.sum(grad_out_f, axis=0)
    vectors = (
        placed(qkv_sums[:3], 3, hw),
        out_sum,
        placed(up_sums[0], 1, ffw),
        gain_sums[0],
        gain_sums[1],
        gain_sums[2],
        gain_sums[3],
    )
    packed = jnp.concatenate(vectors).reshape(-1, 128)
    mask = 1
    while mask < ns:
        packed = packed + by_seq(packed, mask)
        mask *= 2
    mask = 1
    while mask < nd:
        packed = packed + by_dp(packed, mask)
        mask *= 2
    flat = packed.reshape(-1)
    small_out, at = [], 0
    for vector in vectors:
        n = vector.shape[0]
        share = n // (ns * nd)
        small_out.append(lax.dynamic_slice_in_dim(flat, at + index * share, share))
        at += n
    gb_qkv, gb_out, gb_up, gg_attn, gs_attn, gg_ffn, gs_ffn = small_out
    return (
        output[None],
        input_grad[None],
        grad_qkv,
        gb_qkv,
        grad_dense,
        gb_out,
        grad_up,
        gb_up,
        grad_down,
        gb_out,
        gg_attn,
        gs_attn,
        gg_ffn,
        gs_ffn,
    )


class Bag(dict):
    __getattr__ = dict.__getitem__


class Net:
    def __init__(self, send, recv):
        self.send_sems, self.recv_sems, self.copies, self.count = send, recv, [], 0

    def make(self, source, target, **peer):
        at = self.count
        self.count += 1
        copy = pltpu.make_async_remote_copy(
            src_ref=source,
            dst_ref=target,
            send_sem=self.send_sems.at[at],
            recv_sem=self.recv_sems.at[at],
            device_id=peer,
            device_id_type=pl.DeviceIdType.MESH,
        )
        self.copies.append(copy)
        return copy

    def send(self, source, target, **peer):
        copy = self.make(source, target, **peer)
        copy.start()
        return copy

    def release(self, copies):
        for copy in copies:
            copy.wait_send()
        self.copies = [c for c in self.copies if all(c is not copy for copy in copies)]

    def finish(self):
        for copy in self.copies:
            copy.wait_send()


class Local:
    def __init__(self, sems):
        self.sems, self.copies, self.done = sems, [], 0

    def make(self, source, target):
        copy = pltpu.make_async_copy(source, target, self.sems.at[self.done + len(self.copies)])
        self.copies.append(copy)
        return copy

    def copy(self, source, target):
        copy = self.make(source, target)
        copy.start()
        return copy

    def load(self, source, target):
        copy = pltpu.make_async_copy(source, target, self.sems.at[self.done + len(self.copies)])
        copy.start()
        self.done += 1
        return copy

    def finish(self):
        for copy in self.copies:
            copy.wait()


def greet(peers):
    barrier = pltpu.get_barrier_semaphore()
    for peer in peers:
        pl.semaphore_signal(
            barrier, inc=1, device_id=peer, device_id_type=pl.DeviceIdType.MESH
        )
    pl.semaphore_wait(barrier, len(peers))


def neighbours(dims, s, d):
    return (
        [{"seq": s ^ js} for js in range(1, dims.ns)]
        + [{"dp": d ^ (jz * dims.lo)} for jz in range(1, dims.hi)]
        + [{"dp": d ^ jy} for jy in range(1, dims.lo)]
    )


def table_constants():
    half = ROT // 2
    table = 2 * HEAD
    constants = np.zeros((4 * half, table), np.float32)
    constants[3 * half :, :] = rotary_base ** (-2.0 * np.arange(half)[:, None] / ROT)
    for lane in range(table):
        if lane % HEAD < ROT:
            constants[lane % HEAD % half, lane] = 1.0
            constants[half + lane % HEAD % half, lane] = -1.0 if lane % HEAD < half else 1.0
        else:
            constants[2 * half, lane] = 1.0
    return constants


def rotary_tables(rows, const_ref, width):
    half = ROT // 2
    exact = lax.Precision.HIGHEST
    cosine = lax.dot_general(
        rows[0:half, :], const_ref[0:half, :], TN, precision=exact, preferred_element_type=F32
    ) + const_ref[2 * half : 2 * half + 1, :]
    sine = lax.dot_general(
        rows[half : 2 * half, :], const_ref[half : 2 * half, :], TN, precision=exact,
        preferred_element_type=F32,
    )
    return spread_lanes(cosine, width), spread_lanes(sine, width)


def gather_kernel(dims, hidden, grad_out, places, segments, fields, qkv, up, dense):
    ns, nd, hi, lo, nx = dims.ns, dims.nd, dims.hi, dims.lo, dims.nx
    tokens, width, hw, ffw, seq = dims.tokens, dims.width, dims.hw, dims.ffw, dims.seq
    share, dense_share = qkv.shape[0], dense.shape[0]
    n_net, n_local = 128, 64

    def kernel(
        hid, gout, places_ref, segments_ref, qkv_ref, up_ref, dense_ref, const_ref, f0, f1, f2, f3, f4, f5, f6, f7,
        attn_out, ffn_out, hat_out, g_out, act_out, slope_out, q_out, k_out, v_out, kt_out,
        vt_out, mix_out, qkv_out, up_out, dense_out, meta_out, affine_out,
        h_buf, g_buf, attn_buf, ffn_buf, hat_buf, act_buf, slope_buf, q_buf, k_buf, v_buf,
        kt_buf, vt_buf, mix_buf, w_qkv, w_up, w_dense, meta_buf, affine, vectors, bias_rows, small_ref, meta_ref,
        send_sems, recv_sems, local_sems,
    ):
        s, d = lax.axis_index("seq"), lax.axis_index("dp")
        z, y = d // lo, d % lo
        net, local = Net(send_sems, recv_sems), Local(local_sems)
        h_own = local.load(hid, h_buf.at[0:tokens])
        small_ref[...] = jnp.zeros_like(small_ref)
        for row, field in enumerate((f0, f1, f2, f3, f4, f5, f6, f7)):
            n = field.shape[0]
            small_ref[row : row + 1, 0:n] = field[...].astype(F32).reshape(1, n)
        half = ROT // 2
        angles = const_ref[3 * half : 4 * half, 0:1] * places_ref[...].astype(F32)
        meta_ref[0:half, :] = jnp.cos(angles)
        meta_ref[half : 2 * half, :] = jnp.sin(angles)
        meta_ref[2 * half :, :] = jnp.broadcast_to(segments_ref[...].astype(F32), (half, tokens))
        greet(neighbours(dims, s, d))

        def block(ref, j):
            return ref.at[j * tokens : (j + 1) * tokens]

        def along_z(weight):
            return [net.send(weight(d), weight(d), dp=d ^ (jz * lo)) for jz in range(1, hi)]

        def along_y(weight, jz):
            at = (z ^ jz) * lo + y
            return [net.send(weight(at), weight(at), dp=d ^ jy) for jy in range(1, lo)]

        def forward_y(arrivals, weight):
            sent = []
            for jz, done in enumerate(arrivals, 1):
                done.wait_recv()
                sent += along_y(weight, jz)
            return sent

        def to_columns(js, name):
            other = s ^ js
            if name == "up":
                at = pl.multiple_of(other * ffw, ffw)
                pairs = [(up_ref.at[:, pl.ds(at, ffw)], w_up.at[s, d])]
            else:
                pairs = []
                for part in range(3):
                    at = pl.multiple_of(part * width + other * hw, hw)
                    pairs.append(
                        (
                            qkv_ref.at[:, pl.ds(at, hw)],
                            w_qkv.at[s, d, :, part * hw : (part + 1) * hw],
                        )
                    )
            if js == 0:
                return [local.load(a, b) for a, b in pairs]
            return [net.send(a, b, seq=other) for a, b in pairs]

        tiny = [net.send(small_ref, vectors.at[s, d], seq=s ^ js) for js in range(1, ns)]
        vectors[s, d] = small_ref[...]
        cuts = Bag()
        for name in ("up", "qkv"):
            cuts[name] = [to_columns(js, name) for js in range(ns)]
        metas = [net.send(meta_ref, meta_buf.at[js], seq=s ^ js) for js in range(1, ns)]
        meta_buf[0] = meta_ref[...]
        h_core = net.send(hid, block(h_buf, 1), seq=s ^ 1)
        h_cross = [net.send(hid, block(h_buf, 2 * m), seq=s ^ (2 * m)) for m in range(1, nx)]
        g_core = net.send(gout, block(g_buf, 1), seq=s ^ 1)
        g_cross = [net.send(gout, block(g_buf, 2 * m), seq=s ^ (2 * m)) for m in range(1, nx)]
        g_own = local.load(gout, block(g_buf, 0))
        dense_own = local.load(dense_ref, w_dense.at[d])

        first, second = slice(0, ns // 2), slice(ns // 2, ns)
        part_qkv = [lambda at: w_qkv.at[first, at], lambda at: w_qkv.at[second, at]]
        part_up = [lambda at: w_up.at[first, at], lambda at: w_up.at[second, at]]
        part_dense = lambda at: w_dense.at[at]
        part_tiny = lambda at: vectors.at[:, at]

        for done in tiny:
            done.wait_recv()
        z_tiny = along_z(part_tiny)
        y_tiny = along_y(part_tiny, 0)

        def spread_weight(name, halves):
            for done in cuts[name][0]:
                done.wait()
            for group in cuts[name][1:]:
                for done in group:
                    done.wait_recv()
            return [along_z(half) for half in halves], [along_y(half, 0) for half in halves]

        z_up, y_up = spread_weight("up", part_up)
        y_tiny += forward_y(z_tiny, part_tiny)
        z_qkv, y_qkv = spread_weight("qkv", part_qkv)
        dense_own.wait()
        z_dense, y_dense = along_z(part_dense), along_y(part_dense, 0)

        for done in y_tiny:
            done.wait_recv()
        n = width // (ns * nd)
        per_row = 128 // n
        for row in range(width // 128):
            total = None
            for q in range(per_row):
                owner = row * per_row + q
                tile = vectors[owner // nd, owner % nd]
                tile = pltpu.roll(tile, q * n, 1) if q else tile
                total = tile if total is None else total + tile
            lanes = slice(row * 128, (row + 1) * 128)
            affine[0:4, lanes] = total[4:8, :]
            affine[4:5, lanes] = total[1:2, :] + total[3:4, :]
        lane = lax.broadcasted_iota(jnp.int32, (1, 128), 1)
        n = 3 * n
        bias_rows[...] = jnp.zeros_like(bias_rows)
        for owner in range(ns * nd):
            start, row = owner * n % 128, owner * n // 128
            tile = vectors[owner // nd, owner % nd]
            tile = (pltpu.roll(tile, start, 1) if start else tile)[0:1, :]
            bias_rows[row : row + 1, :] += jnp.where(lane >= start, tile, 0.0)
            if start + n > 128:
                bias_rows[row + 1 : row + 2, :] += jnp.where(lane < start, tile, 0.0)
        local.copy(affine, affine_out)
        tile = 256

        def norm(first, last):
            def body(t, carry):
                rows = pl.ds(pl.multiple_of(t * tile, tile), tile)
                x = h_buf[rows, :].astype(F32)
                spread = x - jnp.mean(x, axis=-1, keepdims=True)
                hat = spread * lax.rsqrt(
                    jnp.mean(spread * spread, axis=-1, keepdims=True) + epsilon
                )
                attn_buf[rows, :] = (hat * affine[0:1, :] + affine[1:2, :]).astype(BF)
                ffn_buf[rows, :] = (hat * affine[2:3, :] + affine[3:4, :]).astype(BF)
                hat_buf[rows, :] = hat.astype(BF)
                return carry

            per = tokens // tile
            lax.fori_loop(first * per, last * per, body, 0)
            here = slice(first * tokens, last * tokens)
            for source, target in ((attn_buf, attn_out), (ffn_buf, ffn_out), (hat_buf, hat_out)):
                local.copy(source.at[here], target.at[here])

        h_own.wait()
        h_core.wait_recv()
        norm(0, 2)
        y_up.append(forward_y(z_up[0], part_up[0]))
        y_up.append(forward_y(z_up[1], part_up[1]))
        h_far = []
        for m, done in enumerate(h_cross, 1):
            done.wait_recv()
            h_far.append(
                net.send(block(h_buf, 2 * m), block(h_buf, 2 * m + 1), seq=s ^ 1)
            )
        for done in h_far:
            done.wait_recv()
        norm(2, ns)
        y_qkv.append(forward_y(z_qkv[0], part_qkv[0]))

        for group in y_up:
            for done in group:
                done.wait_recv()
        bias_up = jnp.concatenate(
            [
                vectors[(s * (ffw // 128) + c) // nd, (s * (ffw // 128) + c) % nd, 2:3, :]
                for c in range(ffw // 128)
            ],
            axis=1,
        )

        def up_rows(first, last):
            def body(t, carry):
                rows = pl.ds(pl.multiple_of(t * tile, tile), tile)
                pre = mm(ffn_buf[rows, :], w_up[...].reshape(width, ffw)) + bias_up
                total = 0.5 + 0.5 * lax.erf(pre * math.sqrt(0.5))
                density = jnp.exp(-0.5 * pre * pre) * (1.0 / math.sqrt(2.0 * math.pi))
                act_buf[rows, :] = (pre * total).astype(BF)
                slope_buf[rows, :] = (total + pre * density).astype(BF)
                return carry

            per = tokens // tile
            lax.fori_loop(first * per, last * per, body, 0)
            here = slice(first * tokens, last * tokens)
            for source, target in ((act_buf, act_out), (slope_buf, slope_out)):
                local.copy(source.at[here], target.at[here])

        up_rows(0, ns // 2)
        y_qkv.append(forward_y(z_qkv[1], part_qkv[1]))
        up_rows(ns // 2, ns)
        local.copy(w_up, up_out)
        y_dense += forward_y(z_dense, part_dense)

        g_far = []
        for m, done in enumerate(g_cross, 1):
            done.wait_recv()
            g_far.append(
                net.send(block(g_buf, 2 * m), block(g_buf, 2 * m + 1), seq=s ^ 1)
            )
        for group in y_qkv:
            for done in group:
                done.wait_recv()
        for done in metas:
            done.wait_recv()
        parts = hw // 128
        bias_qkv = jnp.concatenate(
            [
                bias_rows[pl.ds(part * (width // 128) + s * parts + k, 1), :]
                for part in range(3)
                for k in range(parts)
            ],
            axis=1,
        )

        def qkv_block(j, carry):
            rows = pl.ds(pl.multiple_of(j * tokens, tokens), tokens)
            cosine, sine = rotary_tables(meta_buf[j], const_ref, hw)
            joined = mm(attn_buf[rows, :], w_qkv[...].reshape(width, 3 * hw)) + bias_qkv
            queries = turn(joined[:, :hw], cosine, sine, 1.0)
            keys = turn(joined[:, hw : 2 * hw], cosine, sine, 1.0)
            values = joined[:, 2 * hw :]
            q_buf[rows, :] = queries.astype(BF) * (1.0 / math.sqrt(HEAD))
            k_buf[rows, :] = keys.astype(BF)
            v_buf[rows, :] = values.astype(BF)
            kt_buf[:, rows] = keys.T.astype(BF)
            vt_buf[:, rows] = values.T.astype(BF)
            return carry

        lax.fori_loop(0, ns, qkv_block, 0)
        for source, target in (
            (q_buf, q_out), (k_buf, k_out), (v_buf, v_out), (kt_buf, kt_out), (vt_buf, vt_out),
            (w_qkv, qkv_out), (meta_buf, meta_out),
        ):
            local.copy(source, target)

        for done in y_dense + [g_core]:
            done.wait_recv()
        g_own.wait()

        def mix_block(j, carry):
            rows = pl.ds(pl.multiple_of(j * tokens, tokens), tokens)
            mix_buf[rows, :] = mm_nt(g_buf[rows, :], w_dense[...].reshape(hw, width)).astype(BF)
            return carry

        near, beyond = slice(0, 2 * tokens), slice(2 * tokens, seq)
        local.copy(w_dense, dense_out)
        local.copy(g_buf.at[near], g_out.at[near])
        lax.fori_loop(0, 2, mix_block, 0)
        local.copy(mix_buf.at[near], mix_out.at[near])
        for done in g_far:
            done.wait_recv()
        local.copy(g_buf.at[beyond], g_out.at[beyond])
        lax.fori_loop(2, ns, mix_block, 0)
        local.copy(mix_buf.at[beyond], mix_out.at[beyond])
        local.finish()
        net.finish()

    sds = jax.ShapeDtypeStruct
    any_spec = pl.BlockSpec(memory_space=pl.ANY)
    vmem_spec = pl.BlockSpec(memory_space=pltpu.VMEM)
    const = jnp.asarray(table_constants())
    out_shapes = (
        [sds((seq, width), BF)] * 4
        + [sds((seq, ffw), BF)] * 2
        + [sds((seq, hw), BF)] * 3
        + [sds((hw, seq), BF)] * 2
        + [sds((seq, hw), BF)]
        + [
            sds((ns, nd, share, 3 * hw), BF),
            sds((ns, nd, share, ffw), BF),
            sds((nd, dense_share, width), BF),
            sds((ns, 3 * ROT // 2, tokens), F32),
            sds((8, width), F32),
        ]
    )
    scratch = [
        pltpu.VMEM(x.shape, x.dtype)
        for x in [sds((seq, width), BF)] * 5 + out_shapes[4:]
    ] + [
        pltpu.VMEM((ns, nd, 8, 128), F32),
        pltpu.VMEM((3 * width // 128 + 8, 128), F32),
        pltpu.VMEM((8, 128), F32),
        pltpu.VMEM((3 * ROT // 2, tokens), F32),
        pltpu.SemaphoreType.DMA((n_net,)),
        pltpu.SemaphoreType.DMA((n_net,)),
        pltpu.SemaphoreType.DMA((n_local,)),
    ]
    return pl.pallas_call(
        kernel,
        out_shape=out_shapes,
        in_specs=[any_spec] * 2 + [vmem_spec] * 2 + [any_spec] * 3 + [vmem_spec] * 9,
        out_specs=[any_spec] * len(out_shapes),
        scratch_shapes=scratch,
        compiler_params=pltpu.CompilerParams(
            vmem_limit_bytes=VMEM_LIMIT, collective_id=1, has_side_effects=True
        ),
        name="gather",
    )(hidden, grad_out, places, segments, qkv, up, dense, const, *fields)


class Spread:
    def __init__(self, dims, net, where, groups, rows, total, base, cols, steps, bufs):
        self.steps = steps
        self.dims, self.net, self.where, self.groups, self.rows = dims, net, where, groups, rows
        self.total, self.base, self.cols = total, base, cols
        self.send_y, self.recv_y, self.send_z, self.recv_z = bufs

    def part(self, group, owner):
        unit = group * self.steps[0] + owner * self.steps[1]
        at = pl.multiple_of(self.base + unit * self.rows, self.rows)
        return self.total[pl.ds(at, self.rows), self.cols]

    def start(self):
        s, d, z, y = self.where
        dims = self.dims
        self.along_y = []
        for jy in range(1, dims.lo):
            for zz in range(dims.hi):
                for g in range(self.groups):
                    self.send_y[jy - 1, zz, g] = self.part(g, zz * dims.lo + (y ^ jy)).astype(BF)
            self.along_y.append(
                self.net.send(self.send_y.at[jy - 1], self.recv_y.at[jy - 1], dp=d ^ jy)
            )

    def summed(self, zz, g):
        s, d, z, y = self.where
        value = self.part(g, zz * self.dims.lo + y)
        for jy in range(1, self.dims.lo):
            value = value + self.recv_y[jy - 1, zz, g].astype(F32)
        return value

    def middle(self):
        s, d, z, y = self.where
        for copy in self.along_y:
            copy.wait_recv()
        self.along_z = []
        for jz in range(1, self.dims.hi):
            for g in range(self.groups):
                self.send_z[jz - 1, g] = self.summed(z ^ jz, g).astype(BF)
            self.along_z.append(
                self.net.send(
                    self.send_z.at[jz - 1], self.recv_z.at[jz - 1], dp=d ^ (jz * self.dims.lo)
                )
            )

    def own(self, g):
        s, d, z, y = self.where
        return self.summed(z, g)

    def arrive(self):
        for copy in self.along_z:
            copy.wait_recv()

    def final(self, g):
        value = self.own(g)
        for jz in range(1, self.dims.hi):
            value = value + self.recv_z[jz - 1, g].astype(F32)
        return value


class Stream:
    def __init__(self, slots, sems):
        self.slots, self.sems = slots, sems

    def copies(self, t, slot):
        found = []
        for k, array in enumerate(self.arrays):
            rows = pl.ds(pl.multiple_of(self.index(t) * self.size, self.size), self.size)
            found.append(
                pltpu.make_async_copy(
                    array.at[rows], self.slots.at[k, slot, 0 : self.size], self.sems.at[k, slot]
                )
            )
        return found

    def ask(self, arrays, size, index=lambda t: t):
        self.arrays, self.size, self.index = arrays, size, index
        for copy in self.copies(0, 0):
            copy.start()

    def run(self, count, body):
        def step(t, carry):
            slot = t % 2

            @pl.when(t + 1 < count)
            def _():
                for copy in self.copies(t + 1, 1 - slot):
                    copy.start()

            for copy in self.copies(t, slot):
                copy.wait()
            body(t, *[self.slots.at[k, slot, 0 : self.size] for k in range(len(self.arrays))])
            return carry

        lax.fori_loop(0, count, step, 0)


def main_kernel(dims, arrays, down):
    ns, nd, hi, lo, nx = dims.ns, dims.nd, dims.hi, dims.lo, dims.nx
    tokens, width, hw, ffw, seq = dims.tokens, dims.width, dims.hw, dims.ffw, dims.seq
    heads = dims.heads
    tile = 256
    per = tokens // tile
    blocks = seq // tile
    window = seq // 2 // tile
    wide = heads * tile
    r_col, r_dense, r_down = width // (ns * nd), hw // nd, ffw // nd
    half_d, half_f = width // 2, ffw // 2
    pieces = r_down // r_col
    plans = Bag(
        down0=(pieces, r_col, half_d, True), down1=(pieces, r_col, half_d, True),
        up0=(ns, r_col, half_f, False), up1=(ns, r_col, half_f, False),
        q=(ns, r_col, hw, False), k=(ns, r_col, hw, False), v=(ns, r_col, hw, False),
        dense=(1, r_dense, width, True),
    )
    columns = [n for n in plans if not plans[n][3]]
    rows_kind = [n for n in plans if plans[n][3]]
    shared = Bag(up0="down0", up1="down1")
    n_net, n_local = 128, 48
    in_names = (
        "queries", "keys", "values", "keys_t", "values_t", "grad_mix", "attn", "ffn", "hat",
        "act", "slope", "grads", "w_qkv", "w_up", "w_dense",
    )
    sds = jax.ShapeDtypeStruct
    cut = (ns, tokens, hw)
    outs = Bag(
        home_out=sds(cut, BF), home_in=sds(cut, BF),
        far_out=sds((nx - 1,) + cut, BF), far_in=sds((nx - 1,) + cut, BF),
        grad_up_low=sds((seq, ffw), BF),
        own_sums=sds((8, 128), F32), swap_sums=sds((ns - 1, 8, 128), F32),
    )
    for name in rows_kind:
        groups, rows, n, _ = plans[name]
        outs["own_" + name] = sds((groups, rows, n), F32)
        outs["z_" + name] = sds((hi - 1, groups, rows, n), BF)
    for name in columns:
        groups, rows, n, _ = plans[name]
        outs["own_" + name] = sds((rows, n), F32)
        outs["swap_" + name] = sds((ns - 1, rows, n), BF)
    scratch = Bag(
        w_qkv=sds((width, 3 * hw), BF), w_up=sds((width, ffw), BF),
        w_dense=sds((hw, width), BF), w_down=sds((nd, r_down, width), BF),
        acc=sds((ffw, width), F32), acc_k=sds((seq, hw), F32), acc_v=sds((seq, hw), F32),
        pool=sds((4, seq, hw), BF),
        keys_t=sds((hw, seq), BF), values_t=sds((hw, seq), BF),
        scores=sds(((window + 1) * tile, wide), F32),
        probs=sds(((window + 1) * tile, wide), BF),
        mixed=sds((seq, hw), BF), gq=sds((seq, hw), BF), gk=sds((seq, hw), BF),
        gv=sds((seq, hw), BF),
        got_out=sds((nx, seq, hw), BF), got_in=sds((nx, seq, hw), BF),
        out_parts=sds((2 * nx, seq, hw), BF),
        stream=sds((2, 2, tokens, width), BF),
        qkv_sum=sds((8, hw), F32), up_sum=sds((8, ffw), F32), gain_sum=sds((8, width), F32),
        sum_rows=sds((3 * width // 128 + 8, 128), F32),
        tiles=sds((ns, hi, lo, 8, 128), F32),
        tiles_y=sds((lo - 1, ns, hi, 8, 128), F32), tiles_z=sds((ns, hi, 8, 128), F32),
        tiles_zr=sds((hi - 1, ns, 8, 128), F32), tiles_s=sds((ns, 8, 128), F32),
    )
    for name, (groups, rows, n, landed) in plans.items():
        if name not in shared:
            scratch["sy_" + name] = sds((lo - 1, hi, groups, rows, n), BF)
            scratch["sz_" + name] = sds((hi - 1, groups, rows, n), BF)
        scratch["ry_" + name] = sds((lo - 1, hi, groups, rows, n), BF)
        if not landed:
            scratch["rz_" + name] = sds((hi - 1, groups, rows, n), BF)
            scratch["sw_" + name] = sds((ns - 1, rows, n), BF)
        scratch["ob_" + name] = sds((groups, rows, n) if landed else (rows, n), F32)

    def kernel(*all_refs):
        refs = list(all_refs)
        take = lambda names: Bag((name, refs.pop(0)) for name in names)
        hbm = take(in_names)
        down_ref, meta_ref, affine, const_ref = [refs.pop(0) for _ in range(4)]
        out = take(outs)
        vm = take(scratch)
        send_sems, recv_sems, local_sems, stream_sems = refs
        stream = Stream(vm.stream, stream_sems)
        stream.ask([hbm.act, hbm.grads], tokens)
        s, d = lax.axis_index("seq"), lax.axis_index("dp")
        z, y = d // lo, d % lo
        where = (s, d, z, y)
        net, local = Net(send_sems, recv_sems), Local(local_sems)
        loads = Bag()
        for at, name in enumerate(("queries", "keys", "values", "grad_mix")):
            loads[name] = local.load(hbm[name], vm.pool.at[at])
        for name in ("keys_t", "values_t", "w_dense", "w_qkv", "w_up"):
            loads[name] = local.load(hbm[name], vm[name])
        q_ref, k_ref, v_ref, g_ref = [vm.pool.at[at] for at in range(4)]
        greet(neighbours(dims, s, d))

        part_down = lambda at: vm.w_down.at[at]
        down_own = local.load(down_ref, part_down(d))
        z_down = [
            net.send(down_ref, part_down(d), dp=d ^ (jz * lo)) for jz in range(1, hi)
        ]
        y_down = [net.send(down_ref, part_down(d), dp=d ^ jy) for jy in range(1, lo)]

        totals = Bag(
            down0=("acc", 0, slice(0, half_d)), down1=("acc", 0, slice(half_d, width)),
            up0=("acc", 0, slice(0, half_f)), up1=("acc", 0, slice(half_f, ffw)),
            q=("scores", 0, slice(0, hw)), k=("scores", 0, slice(hw, 2 * hw)),
            v=("scores", 0, slice(2 * hw, 3 * hw)), dense=("scores", width, slice(0, width)),
        )
        sets = Bag()
        for name, (groups, rows, n, landed) in plans.items():
            total, base, cols = totals[name]
            source = shared.get(name, name)
            steps = (1, groups) if landed else (nd, 1)
            bufs = (
                vm["sy_" + source], vm["ry_" + name], vm["sz_" + source],
                out["z_" + name] if landed else vm["rz_" + name],
            )
            sets[name] = Spread(
                dims, net, where, groups, rows, vm[total], base, cols, steps, bufs
            )

        def rows_of_step(t, size):
            return pl.ds(pl.multiple_of(t * size, size), size)

        def finish_rows(name):
            for g in range(sets[name].groups):
                vm["ob_" + name][g] = sets[name].own(g)
            local.copy(vm["ob_" + name], out["own_" + name])

        chunk = 256

        def add_products(t, left, right):
            for m in range(0, ffw, chunk):
                vm.acc[m : m + chunk, :] += mm_tn(left[:, m : m + chunk], right[...])

        vm.acc[...] = jnp.zeros_like(vm.acc)
        stream.run(ns, add_products)
        stream.ask([hbm.grads, hbm.slope], tile)
        sets.down0.start()

        lane = lax.broadcasted_iota(jnp.int32, (1, hw), 1)
        segments = jnp.concatenate([meta_ref[j, 16:24, :] for j in range(ns)], axis=1)
        edges = [
            jnp.sum((segments[0:1, :] < float(v)).astype(F32), axis=1, keepdims=True).astype(
                jnp.int32
            )
            for v in range(1, DOCS)
        ]

        def by_head(value):
            zero = jnp.zeros_like(value)
            return jnp.concatenate(
                [jnp.where(lane // HEAD == h, value, zero) for h in range(heads)], axis=0
            )

        def rows_at(block):
            at = ((block // per) ^ s) * per + block % per
            return pl.ds(pl.multiple_of(at * tile, tile), tile)

        for name in ("queries", "keys", "values", "grad_mix", "keys_t", "values_t"):
            loads[name].wait()
        vm.acc_k[...] = jnp.zeros_like(vm.acc_k)
        vm.acc_v[...] = jnp.zeros_like(vm.acc_v)
        vm.qkv_sum[...] = jnp.zeros_like(vm.qkv_sum)
        cols = [slice(h * tile, (h + 1) * tile) for h in range(heads)]
        lanes_of = [slice(h * HEAD, (h + 1) * HEAD) for h in range(heads)]
        scale = 1.0 / math.sqrt(HEAD)

        def attend(block, carry_in):
            here = rows_at(block)
            q_stack = by_head(q_ref[here, :])
            q_pos = block * tile + lax.broadcasted_iota(jnp.int32, (1, wide), 1) % tile
            begin = jnp.zeros((1, wide), jnp.int32)
            for edge in edges:
                begin = jnp.where(q_pos >= edge, jnp.maximum(begin, edge), begin)
            low = jnp.maximum(block - window, 0)
            key_row = lax.broadcasted_iota(jnp.int32, (tile, wide), 0)

            def slot(key_block):
                return pl.ds(pl.multiple_of((key_block - low) * tile, tile), tile)

            def score_pass(key_block, high):
                allowed = key_row >= begin - key_block * tile
                scores = jnp.where(
                    allowed, mm_nt(k_ref[rows_at(key_block), :], q_stack), masked_score
                )
                vm.scores[slot(key_block), :] = scores
                return jnp.maximum(high, jnp.max(scores, axis=0, keepdims=True))

            high = lax.fori_loop(low, block, score_pass, jnp.full((1, wide), masked_score, F32))
            allowed = (key_row >= begin - block * tile) & (key_row <= q_pos - block * tile)
            scores = jnp.where(allowed, mm_nt(k_ref[here, :], q_stack), masked_score)
            vm.scores[slot(block), :] = scores
            high = jnp.maximum(high, jnp.max(scores, axis=0, keepdims=True))

            def prob_pass(key_block, carry):
                total, mixed = carry
                rows = rows_at(key_block)
                probs = jnp.exp(vm.scores[slot(key_block), :] - high)
                total = total + jnp.sum(probs, axis=0, keepdims=True)
                probs = probs.astype(BF)
                vm.probs[slot(key_block), :] = probs
                mixed = tuple(
                    mixed[h] + mm(vm.values_t[lanes_of[h], rows], probs[:, cols[h]])
                    for h in range(heads)
                )
                return total, mixed

            zeros = tuple(jnp.zeros((HEAD, tile), F32) for _ in range(heads))
            total, mixed = lax.fori_loop(
                low, block + 1, prob_pass, (jnp.zeros((1, wide), F32), zeros)
            )
            inverse = 1.0 / total
            grads_t = g_ref[here, :].astype(F32).T
            mixed = [mixed[h] * inverse[:, cols[h]] for h in range(heads)]
            scaled = [grads_t[lanes_of[h], :] * inverse[:, cols[h]] for h in range(heads)]
            delta = jnp.concatenate(
                [jnp.sum(mixed[h] * scaled[h], axis=0, keepdims=True) for h in range(heads)],
                axis=1,
            )
            vm.mixed[here, :] = jnp.concatenate(mixed, axis=0).T.astype(BF)
            g_stack = by_head(jnp.concatenate(scaled, axis=0).T.astype(BF))

            def grad_pass(key_block, grads_q):
                rows = rows_at(key_block)
                probs = vm.probs[slot(key_block), :]
                grad_probs = mm_nt(v_ref[rows, :], g_stack)
                grad_scores = (probs.astype(F32) * (grad_probs - delta)).astype(BF)
                vm.acc_v[rows, :] += mm(probs, g_stack)
                vm.acc_k[rows, :] += mm(grad_scores, q_stack)
                return tuple(
                    grads_q[h] + mm(vm.keys_t[lanes_of[h], rows], grad_scores[:, cols[h]])
                    for h in range(heads)
                )

            grads_q = lax.fori_loop(low, block + 1, grad_pass, zeros)
            finish_grad("gq", 0, here, (jnp.concatenate(grads_q, axis=0) * scale).T)
            return carry_in

        def finish_grad(name, row, rows, value):
            if row < 2:
                start = rows.start
                cosine, sine = rotary_tables(
                    meta_ref[start // tokens, :, pl.ds(pl.multiple_of(start % tokens, tile), tile)],
                    const_ref, hw,
                )
                value = turn(value, cosine, sine, -1.0)
            value = value.astype(BF)
            vm[name][rows, :] = value
            vm.qkv_sum[row : row + 1, :] += jnp.sum(value.astype(F32), axis=0, keepdims=True)

        def attend_blocks(first, last):
            none = s // 64
            lax.fori_loop(first + none, last + none, attend, 0)

        def forward_down():
            sent = []
            for jz, done in enumerate(z_down, 1):
                done.wait_recv()
                at = (z ^ jz) * lo + y
                sent += [net.send(part_down(at), part_down(at), dp=d ^ jy) for jy in range(1, lo)]
            return sent

        parity, across = s % 2, s // 2

        def put(parts, j, start, value):
            size = value.shape[0]
            slot = (1 - j % 2) * nx + j // 2
            for c in range(ns):
                at = pl.ds(pl.multiple_of(c * tokens + start, size), size)
                parts[slot, at, :] = value[:, c * hw : (c + 1) * hw]

        def add_got(keep, got, m):
            keep[m] = (keep[m].astype(F32) + got[m].astype(F32)).astype(BF)

        def as_cut(ref):
            return ref.reshape(ns, tokens, hw)

        give_out, keep_out = vm.out_parts.at[0:nx], vm.out_parts.at[nx : 2 * nx]
        core_out = [
            net.make(give_out.at[chip ^ across], vm.got_out.at[chip ^ across], seq=s ^ 1)
            for chip in range(nx)
        ]
        far_out = net.make(as_cut(keep_out.at[1]), out.far_out.at[0], seq=s ^ 2)
        home_out = local.make(as_cut(keep_out.at[0]), out.home_out)

        def ask_out(first):
            stream.ask([hbm.act], tokens, lambda t: (t + first) ^ s)

        def out_blocks(first, last):
            def body(t, act_tile):
                j = (t + first) ^ s
                rows = pl.ds(pl.multiple_of(j * tokens, tokens), tokens)
                value = mm(vm.mixed[rows, :], vm.w_dense[...]) + mm(act_tile[...], w_down())
                put(vm.out_parts, j, 0, value.astype(BF))

            stream.run(last - first, body)

        def cross_out(chip):
            core_out[chip].wait_recv()
            add_got(keep_out, vm.got_out, chip ^ across)

            @pl.when(across == chip)
            def _():
                home_out.start()

            @pl.when(across != chip)
            def _():
                far_out.start()

        attend_blocks(0, blocks // 2)
        y_down += forward_down()
        sets.down1.start()
        attend_blocks(blocks // 2, blocks - 1)
        sets.down0.middle()
        for done in y_down:
            done.wait_recv()
        down_own.wait()
        vm.up_sum[...] = jnp.zeros_like(vm.up_sum)
        w_down = lambda: vm.w_down[...].reshape(ffw, width)

        gu_tile = vm.stream.at[0, 0, tile : 2 * tile]
        gu_copy = lambda t: pltpu.make_async_copy(
            gu_tile, out.grad_up_low.at[rows_of_step(t, tile)], local_sems.at[n_local - 1]
        )

        def up_tile(t, g_tile, slope_tile):
            grads = (mm_nt(g_tile[...], w_down()) * slope_tile[...].astype(F32)).astype(BF)
            vm.up_sum[0:1, :] += jnp.sum(grads.astype(F32), axis=0, keepdims=True)

            @pl.when(t > 0)
            def _():
                gu_copy(t - 1).wait()

            gu_tile[...] = grads
            gu_copy(t).start()

        stream.run(blocks, up_tile)
        gu_copy(blocks - 1).wait()
        hbm["gu"] = out.grad_up_low
        stream.ask([hbm.ffn, hbm.gu], tokens)
        sets.down1.middle()
        finish_rows("down0")
        finish_rows("down1")
        vm.acc[...] = jnp.zeros_like(vm.acc)
        stream.run(ns, add_products)
        ask_out(0)
        net.release(sets.down0.along_y + sets.down1.along_y)
        sets.up0.start()
        sets.up1.start()
        loads.w_dense.wait()
        out_blocks(0, ns - 1)
        ask_out(ns - 1)
        core_out[0].start()

        @pl.when(parity == 1)
        def _():
            core_out[1].start()

        attend_blocks(blocks - 1, blocks)
        cross_out(0)

        @pl.when(parity == 0)
        def _():
            cross_out(1)

        net.release(sets.down0.along_z + sets.down1.along_z)
        sets.up0.middle()
        out_blocks(ns - 1, ns)
        stream.ask([hbm.attn], tokens)

        @pl.when(parity == 0)
        def _():
            core_out[1].start()

        sets.up1.middle()

        def finish_kv(t, carry):
            rows = pl.ds(pl.multiple_of(t * tile, tile), tile)
            finish_grad("gk", 1, rows, vm.acc_k[rows, :])
            finish_grad("gv", 2, rows, vm.acc_v[rows, :])
            return carry

        lax.fori_loop(0, blocks, finish_kv, 0)

        @pl.when(parity == 1)
        def _():
            cross_out(1)

        def qkv_tile(t, left):
            rows = rows_of_step(t, tokens)
            right = jnp.concatenate([vm[n][rows, :] for n in ("gq", "gk", "gv")], axis=1)
            for m in range(0, width, chunk):
                vm.scores[m : m + chunk, 0 : 3 * hw] += mm_tn(left[:, m : m + chunk], right)

        vm.scores[...] = jnp.zeros_like(vm.scores)
        stream.run(ns, qkv_tile)

        def ask_in(m):
            stream.ask([hbm.gu, hbm.hat], tile, lambda t: t + 2 * m * per)

        ask_in(1)
        for name in ("q", "k", "v"):
            sets[name].start()

        loads.w_qkv.wait()
        loads.w_up.wait()
        vm.gain_sum[...] = jnp.zeros_like(vm.gain_sum)
        give_in, keep_in = vm.pool.at[0:nx], vm.pool.at[nx : 2 * nx]
        core_in = [net.make(give_in.at[m], vm.got_in.at[m], seq=s ^ 1) for m in range(nx)]
        far_in = net.make(as_cut(keep_in.at[1]), out.far_in.at[0], seq=s ^ 2)
        home_in = local.make(as_cut(keep_in.at[0]), out.home_in)

        def in_blocks(m):
            first = 2 * m * per

            def body(step, gu_tile, hat_tile):
                t = step + first
                rows = pl.ds(pl.multiple_of(t * tile, tile), tile)
                joined = jnp.concatenate([vm[n][rows, :] for n in ("gq", "gk", "gv")], axis=1)
                attn = mm_nt(joined, vm.w_qkv[...])
                ffn = mm_nt(gu_tile[...], vm.w_up[...])
                hat = hat_tile[...].astype(F32)
                for row, value in ((1, attn), (3, ffn), (0, attn * hat), (2, ffn * hat)):
                    vm.gain_sum[row : row + 1, :] += jnp.sum(value, axis=0, keepdims=True)
                value = attn * affine[0:1, :] + ffn * affine[2:3, :]
                put(vm.pool, t // per, (t % per) * tile, value.astype(BF))

            stream.run(2 * per, body)
            core_in[m].start()

        in_blocks(1)
        stream.ask([hbm.grads], tokens)
        sets.q.middle()

        def dense_tile(t, g_tile):
            left = vm.mixed[rows_of_step(t, tokens), :]
            vm.scores[width : width + hw, :] += mm_tn(left, g_tile[...])

            @pl.when(t == 0)
            def _():
                vm.gain_sum[4:5, :] = jnp.sum(g_tile[...].astype(F32), axis=0, keepdims=True)

        stream.run(ns, dense_tile)
        ask_in(0)
        sets.dense.start()
        core_in[1].wait_recv()
        add_got(keep_in, vm.got_in, 1)
        far_in.start()
        sets.k.middle()
        in_blocks(0)
        sets.v.middle()

        rows = vm.sum_rows
        rows[...] = jnp.zeros_like(rows)
        parts = hw // 128
        for part in range(3):
            for k in range(parts):
                rows[pl.ds(part * (width // 128) + s * parts + k, 1), :] = vm.qkv_sum[
                    part : part + 1, k * 128 : (k + 1) * 128
                ]

        out_sum = vm.gain_sum[4:5, :]
        lane_row = lax.broadcasted_iota(jnp.int32, (1, 128), 1)
        n = width // (ns * nd)
        per_row = 128 // n
        split = lambda owner: (owner // nd, owner % nd // lo, owner % lo)
        for row in range(width // 128):
            at = slice(row * 128, (row + 1) * 128)
            stack = jnp.concatenate(
                [jnp.zeros((1, 128), F32), out_sum[:, at], jnp.zeros((1, 128), F32)]
                + [vm.gain_sum[k : k + 1, at] for k in range(4)]
                + [jnp.zeros((1, 128), F32)],
                axis=0,
            )
            for q in range(per_row):
                a, b, c = split(row * per_row + q)
                vm.tiles[a, b, c] = pltpu.roll(stack, 128 - q * n, 1) if q else stack
        n = 3 * n
        for owner in range(ns * nd):
            start, row = owner * n % 128, owner * n // 128
            value = rows[row : row + 1, :]
            if start + n > 128:
                value = jnp.where(lane_row >= start, value, rows[row + 1 : row + 2, :])
            a, b, c = split(owner)
            vm.tiles[a, b, c, 0:1, :] = pltpu.roll(value, 128 - start, 1) if start else value
        for c in range(ffw // 128):
            vm.tiles[s, c // lo, c % lo, 2:3, :] = vm.up_sum[0:1, c * 128 : (c + 1) * 128]
        tiles_y = [
            net.send(vm.tiles.at[:, :, y ^ jy], vm.tiles_y.at[jy - 1], dp=d ^ jy)
            for jy in range(1, lo)
        ]

        def column_home(name):
            sets[name].arrive()
            vm["ob_" + name][...] = sets[name].final(s)
            local.copy(vm["ob_" + name], out["own_" + name])
            sent = []
            for js in range(1, ns):
                vm["sw_" + name][js - 1] = sets[name].final(s ^ js).astype(BF)
                sent.append(
                    net.send(
                        vm["sw_" + name].at[js - 1], out["swap_" + name].at[js - 1], seq=s ^ js
                    )
                )
            return sent

        core_in[0].wait_recv()
        add_got(keep_in, vm.got_in, 0)
        home_in.start()
        sent = column_home("up0")
        sets.dense.middle()
        finish_rows("dense")
        for done in tiles_y:
            done.wait_recv()
        total = vm.tiles[:, :, y]
        for jy in range(1, lo):
            total = total + vm.tiles_y[jy - 1]
        vm.tiles_z[...] = total
        tiles_z = [
            net.send(vm.tiles_z.at[:, z ^ jz], vm.tiles_zr.at[jz - 1], dp=d ^ (jz * lo))
            for jz in range(1, hi)
        ]
        for name in ("up1", "q", "k", "v"):
            sent += column_home(name)
        for done in tiles_z:
            done.wait_recv()
        total = vm.tiles_z[:, z]
        for jz in range(1, hi):
            total = total + vm.tiles_zr[jz - 1]
        vm.tiles_s[...] = total
        sent += [
            net.send(vm.tiles_s.at[s ^ js], out.swap_sums.at[js - 1], seq=s ^ js)
            for js in range(1, ns)
        ]
        local.copy(vm.tiles_s.at[s], out.own_sums)
        for name in rows_kind:
            sets[name].arrive()
        far_out.wait_recv()
        far_in.wait_recv()
        for done in sent:
            done.wait_recv()
        local.finish()
        net.finish()

    any_spec = pl.BlockSpec(memory_space=pl.ANY)
    vmem_spec = pl.BlockSpec(memory_space=pltpu.VMEM)
    results = pl.pallas_call(
        kernel,
        out_shape=list(outs.values()),
        in_specs=[any_spec] * (len(in_names) + 1) + [vmem_spec] * 3,
        out_specs=[any_spec] * len(outs),
        scratch_shapes=[pltpu.VMEM(x.shape, x.dtype) for x in scratch.values()]
        + [
            pltpu.SemaphoreType.DMA((n_net,)), pltpu.SemaphoreType.DMA((n_net,)),
            pltpu.SemaphoreType.DMA((n_local,)), pltpu.SemaphoreType.DMA((2, 2)),
        ],
        compiler_params=pltpu.CompilerParams(
            vmem_limit_bytes=MAIN_LIMIT, collective_id=2, has_side_effects=True
        ),
        name="main",
    )(
        *[arrays[n] for n in in_names], down, arrays.meta,
        arrays.affine, jnp.asarray(table_constants()),
    )
    return dict(zip(outs, results))


def finish_kernel(dims, s, hidden, grad_out, affine, parts):
    ns, nd, hi, nx = dims.ns, dims.nd, dims.hi, dims.nx
    tokens, width, hw, ffw = dims.tokens, dims.width, dims.hw, dims.ffw
    r_col, r_dense, r_down = width // (ns * nd), hw // nd, ffw // nd
    tile = 256
    names = [n for n in parts if n != "grad_up_low"]
    token_names = [n for n in names if n.startswith(("home", "far"))]
    vector_rows = (0, 1, 2, 1, 3, 4, 5, 6)
    sds = jax.ShapeDtypeStruct

    def kernel(s_ref, hid, gout, affine_ref, *refs):
        part = dict(zip(names, refs[: len(names)]))
        out_ref, in_ref, qkv_out, dense_out, up_out, down_out, *vectors = refs[len(names) :]
        step = pl.program_id(0)
        here = s_ref[0]

        def whole_sum(name):
            columns = []
            for c in range(ns):
                value = part["home_" + name][c].astype(F32)
                for m in range(nx - 1):
                    value = value + part["far_" + name][m, c].astype(F32)
                columns.append(value)
            return jnp.concatenate(columns, axis=1)

        x = hid[...].astype(F32)
        out_ref[...] = (x + whole_sum("out") + affine_ref[4:5, :]).astype(BF)
        gx = whole_sum("in")
        spread = x - jnp.mean(x, axis=-1, keepdims=True)
        inv_std = lax.rsqrt(jnp.mean(spread * spread, axis=-1, keepdims=True) + epsilon)
        hat = spread * inv_std
        back = inv_std * (
            gx
            - jnp.mean(gx, axis=-1, keepdims=True)
            - hat * jnp.mean(gx * hat, axis=-1, keepdims=True)
        )
        in_ref[...] = (gout[...].astype(F32) + back).astype(BF)

        def rows_sum(name, target, cols):
            groups, rows, n = part["own_" + name].shape
            for g in range(groups):
                value = part["own_" + name][g]
                for jz in range(hi - 1):
                    value = value + part["z_" + name][jz, g].astype(F32)
                target[g * rows : (g + 1) * rows, cols] = value

        @pl.when(step == 0)
        def _():
            rows_sum("down0", down_out, slice(0, width // 2))
            rows_sum("down1", down_out, slice(width // 2, width))
            rows_sum("dense", dense_out, slice(0, width))

        def place(target, name, base):
            w = part["own_" + name].shape[1]
            block = width // 1 if target is qkv_out else ffw
            for js in range(ns):
                owner = here ^ js
                at = base(owner)
                value = (
                    part["own_" + name][...]
                    if js == 0
                    else part["swap_" + name][js - 1].astype(F32)
                )
                target[:, pl.ds(pl.multiple_of(at, 128), w)] = value

        @pl.when(step == 1)
        def _():
            for k, name in enumerate(("q", "k", "v")):
                place(qkv_out, name, lambda owner, k=k: k * width + owner * hw)

        @pl.when(step == 1)
        def _():
            for k, name in enumerate(("up0", "up1")):
                place(up_out, name, lambda owner, k=k: owner * ffw + k * (ffw // 2))
            total = part["own_sums"][...]
            for js in range(ns - 1):
                total = total + part["swap_sums"][js]
            for k, target in zip(vector_rows, vectors):
                target[...] = total[k : k + 1, : target.shape[1]]

    def spec(name):
        shape = parts[name].shape
        if name in token_names:
            lead = shape[:-2]
            zeros = (0,) * len(lead)
            return pl.BlockSpec(lead + (tile, hw), lambda t, s_ref: zeros + (t, 0))
        return whole(shape)

    token_spec = pl.BlockSpec((tile, width), lambda t, s_ref: (t, 0))
    finals = [
        (r_col, 3 * width), (r_dense, width), (r_col, ffw * ns), (r_down, width)
    ] + [(1, (3 if k == 0 else 4 if k == 2 else 1) * r_col) for k in vector_rows]
    return pl.pallas_call(
        kernel,
        out_shape=[sds((tokens, width), BF)] * 2 + [sds(f, F32) for f in finals],
        grid_spec=pltpu.PrefetchScalarGridSpec(
            num_scalar_prefetch=1,
            grid=(tokens // tile,),
            in_specs=[token_spec, token_spec, whole(affine.shape)] + [spec(n) for n in names],
            out_specs=[token_spec, token_spec] + [whole(f) for f in finals],
        ),
        compiler_params=params_of(),
        name="finish",
    )(s, hidden, grad_out, affine, *[parts[n] for n in names])


def fused_plan(
    hidden_states,
    segment_ids,
    positions,
    out_grad,
    qkv_weight,
    qkv_bias,
    dense_weight,
    dense_bias,
    up_weight,
    up_bias,
    down_weight,
    down_bias,
    attn_gain,
    attn_shift,
    ffn_gain,
    ffn_shift,
):
    ns, nd = lax.axis_size("seq"), lax.axis_size("dp")
    tokens, width = hidden_states.shape[1:]
    dims = Dims(ns, nd, tokens, width, up_weight.shape[1])
    s = lax.axis_index("seq").astype(jnp.int32).reshape(1)
    hidden, grad_out = hidden_states[0], out_grad[0]
    fields = (
        qkv_bias, dense_bias, up_bias, down_bias, attn_gain, attn_shift, ffn_gain, ffn_shift
    )
    names = (
        "attn", "ffn", "hat", "grads", "act", "slope", "queries", "keys", "values", "keys_t",
        "values_t", "grad_mix", "w_qkv", "w_up", "w_dense", "meta", "affine",
    )
    arrays = Bag(
        zip(
            names,
            gather_kernel(
                dims, hidden, grad_out, positions, segment_ids, fields, qkv_weight, up_weight,
                dense_weight,
            ),
        )
    )
    arrays["w_qkv"] = arrays.w_qkv.reshape(width, -1)
    arrays["w_up"] = arrays.w_up.reshape(width, -1)
    arrays["w_dense"] = arrays.w_dense.reshape(-1, width)
    parts = main_kernel(dims, arrays, down_weight)
    output, input_grad, grad_qkv, grad_dense, grad_up, grad_down, *vectors = finish_kernel(
        dims, s, hidden, grad_out, arrays.affine, parts
    )
    vectors = [v.reshape(-1) for v in vectors]
    return (
        output[None],
        input_grad[None],
        grad_qkv,
        vectors[0],
        grad_dense,
        vectors[1],
        grad_up,
        vectors[2],
        grad_down,
        *vectors[3:],
    )


def per_device(*args):
    tokens, width = args[0].shape[1:]
    ns, nd = lax.axis_size("seq"), lax.axis_size("dp")
    fits = ns == 4 and ns * tokens * width <= 2048 * 1024 and width // (ns * nd) % 16 == 0
    return fused_plan(*args) if fits else permute_plan(*args)


def solution(mesh):
    token = P("dp", "seq", None)
    matrix = P(("seq", "dp"), None)
    vector = P(("seq", "dp"))
    weights = (matrix, vector) * 4 + (vector,) * 4
    return jax.shard_map(
        per_device,
        mesh=mesh,
        in_specs=(token, P("dp", "seq"), P("dp", "seq"), token) + weights,
        out_specs=(token, token) + weights,
        check_vma=False,
    )
```
